16 devices in a mesh: dp: 2 (over y, z), wg: 8 (over x, core).
Axes of the slice: x: 4, y: 2, z: 1, core: 2. Of those that a mesh axis runs over, the one named last changes fastest.
The devices are a block of a 4x4x8 slice.
Arguments:
- hidden: bfloat16 [48, 128, 4096], P(('dp', 'wg')), parts along dimension 0
- seq_lens: int32 [48], P(('dp', 'wg')), parts along dimension 0
- route_idx: int32 [6144, 2], P(('dp', 'wg')), parts along dimension 0
- g_attn_in: bfloat16 [4096], P('wg')
- w_query: bfloat16 [4096, 4096], P('wg')
- w_key: bfloat16 [4096, 1024], P('wg')
- w_value: bfloat16 [4096, 1024], P('wg')
- w_attn_out: bfloat16 [4096, 4096], P('wg')
- g_attn_out: bfloat16 [4096], P('wg')
- g_moe_in: bfloat16 [4096], P('wg')
- w_router: bfloat16 [4096, 8], P('wg')
- w_gate: bfloat16 [8, 4096, 1024], P(None, 'wg')
- w_up: bfloat16 [8, 4096, 1024], P(None, 'wg')
- w_down: bfloat16 [8, 1024, 4096], P(None, 'wg')
- g_moe_out: bfloat16 [4096], P('wg')
Outputs:
- output 1: bfloat16 [48, 128, 4096], P(('dp', 'wg')), parts along dimension 0
- output 2: bfloat16 [48, 128, 8, 128], P(('dp', 'wg')), parts along dimension 0
- output 3: bfloat16 [48, 128, 8, 128], P(('dp', 'wg')), parts along dimension 0
There are 2 independent parts. The reference program is written for one: setup_inputs(seed, part) draws one part's arguments, and reference() takes and returns one part's arrays. A program takes and returns all parts, laid end to end along the dimension named above; an argument that names none is the same for every part.
All inputs are finite; a program needn't handle non-finite values.
Results may differ from the reference program's by a relative error of at most 0.02.
Values are sent between devices in bfloat16 or wider.
A program may use at most 768 MiB of HBM per device.

```python
import jax
import jax.numpy as jnp
from jax import lax

D_MODEL = 4096
HEADS = 32
KV_HEADS = 8
HEAD_DIM = 128
EXPERTS = 8
TOP_K = 2
FF_DIM = 1024
SEQ_LEN = 128
BATCH = 24
TOKENS_DEV = 384

SOFT_CAP = 30.0
NORM_EPS = 1e-5
ROPE_BASE = 10000.0
ATTN_SCALE = HEAD_DIM ** -0.5
GROUPS = HEADS // KV_HEADS
N_ROWS = BATCH * SEQ_LEN


def normal_weight(key_w, out_shape, w_scale):
    return (jax.random.normal(key_w, out_shape, jnp.float32) * w_scale).astype(jnp.bfloat16)


def setup_inputs(seed: int = 0, part: int = 0) -> dict:
    root_key = jax.random.key(seed)
    part_key = jax.random.fold_in(jax.random.key(seed + 1), part)
    w_keys = jax.random.split(root_key, 9)
    p_keys = jax.random.split(part_key, 7)
    in_scale = D_MODEL ** -0.5
    hidden = jax.random.normal(p_keys[0], (BATCH, SEQ_LEN, D_MODEL), jnp.float32).astype(jnp.bfloat16)
    seq_lens = jax.random.randint(p_keys[1], (BATCH,), SEQ_LEN // 4, SEQ_LEN + 1)
    len_picks = jax.random.permutation(p_keys[2], BATCH)
    seq_lens = seq_lens.at[len_picks[0]].set(SEQ_LEN).at[len_picks[1]].set(SEQ_LEN // 4).astype(jnp.int32)
    draw_a = jax.random.randint(p_keys[3], (N_ROWS,), 0, EXPERTS)
    draw_b = jax.random.randint(p_keys[4], (N_ROWS,), 0, EXPERTS)
    shift_amt = jax.random.randint(p_keys[5], (), 0, EXPERTS)
    local_pos = jnp.arange(N_ROWS) % TOKENS_DEV
    first_pick = jnp.where(local_pos < EXPERTS, (local_pos + shift_amt) % EXPERTS, jnp.minimum(draw_a, draw_b))
    second_pick = (first_pick + jax.random.randint(p_keys[6], (N_ROWS,), 1, EXPERTS)) % EXPERTS
    route_idx = jnp.stack([first_pick, second_pick], axis=1).astype(jnp.int32)
    gain_rows = (1.0 + 0.3 * jax.random.normal(w_keys[7], (4, D_MODEL), jnp.float32)).astype(jnp.bfloat16)
    return {
        'hidden': hidden,
        'seq_lens': seq_lens,
        'route_idx': route_idx,
        'g_attn_in': gain_rows[0],
        'w_query': normal_weight(w_keys[0], (D_MODEL, HEADS * HEAD_DIM), 3.0 * in_scale),
        'w_key': normal_weight(w_keys[1], (D_MODEL, KV_HEADS * HEAD_DIM), 3.0 * in_scale),
        'w_value': normal_weight(w_keys[2], (D_MODEL, KV_HEADS * HEAD_DIM), in_scale),
        'w_attn_out': normal_weight(w_keys[3], (HEADS * HEAD_DIM, D_MODEL), (HEADS * HEAD_DIM) ** -0.5),
        'g_attn_out': gain_rows[1],
        'g_moe_in': gain_rows[2],
        'w_router': normal_weight(w_keys[4], (D_MODEL, EXPERTS), in_scale),
        'w_gate': normal_weight(w_keys[5], (EXPERTS, D_MODEL, FF_DIM), in_scale),
        'w_up': normal_weight(w_keys[6], (EXPERTS, D_MODEL, FF_DIM), in_scale),
        'w_down': normal_weight(w_keys[8], (EXPERTS, FF_DIM, D_MODEL), FF_DIM ** -0.5),
        'g_moe_out': gain_rows[3],
    }


def rms_norm(values, gain_vec):
    values_f32 = values.astype(jnp.float32)
    inv_rms = lax.rsqrt(jnp.mean(values_f32 * values_f32, axis=-1, keepdims=True) + NORM_EPS)
    return values_f32 * inv_rms * gain_vec.astype(jnp.float32)


def apply_rope(values, cos_t, sin_t):
    half_dim = HEAD_DIM // 2
    values_f32 = values.astype(jnp.float32)
    first_half = values_f32[..., :half_dim]
    second_half = values_f32[..., half_dim:]
    return jnp.concatenate([first_half * cos_t - second_half * sin_t, second_half * cos_t + first_half * sin_t], axis=-1).astype(jnp.bfloat16)


def reference(hidden, seq_lens, route_idx, g_attn_in, w_query, w_key, w_value, w_attn_out, g_attn_out, g_moe_in, w_router, w_gate, w_up, w_down, g_moe_out):
    half_dim = HEAD_DIM // 2
    inv_freq = ROPE_BASE ** (-jnp.arange(half_dim, dtype=jnp.float32) * (2.0 / HEAD_DIM))
    angles = jnp.arange(SEQ_LEN, dtype=jnp.float32)[:, None] * inv_freq[None, :]
    cos_t = jnp.cos(angles)[:, None, :]
    sin_t = jnp.sin(angles)[:, None, :]
    positions = jnp.arange(SEQ_LEN)
    expert_ids = jnp.arange(EXPERTS)

    def layer_prompt(operands):
        tok_rows, length, choice = operands
        h_attn = rms_norm(tok_rows, g_attn_in).astype(jnp.bfloat16)
        q_proj = jnp.dot(h_attn, w_query, preferred_element_type=jnp.float32).astype(jnp.bfloat16)
        k_proj = jnp.dot(h_attn, w_key, preferred_element_type=jnp.float32).astype(jnp.bfloat16)
        v_proj = jnp.dot(h_attn, w_value, preferred_element_type=jnp.float32).astype(jnp.bfloat16)
        q_rope = apply_rope(q_proj.reshape(SEQ_LEN, HEADS, HEAD_DIM), cos_t, sin_t).reshape(SEQ_LEN, KV_HEADS, GROUPS, HEAD_DIM)
        k_rope = apply_rope(k_proj.reshape(SEQ_LEN, KV_HEADS, HEAD_DIM), cos_t, sin_t)
        v_heads = v_proj.reshape(SEQ_LEN, KV_HEADS, HEAD_DIM)
        scores = jnp.einsum('qkgd,skd->kgqs', q_rope.astype(jnp.float32), k_rope.astype(jnp.float32)) * ATTN_SCALE
        scores = SOFT_CAP * jnp.tanh(scores / SOFT_CAP)
        allowed = (positions[None, :] <= positions[:, None]) & (positions[None, :] < length)
        scores = jnp.where(allowed, scores, -1e30)
        attn_probs = jax.nn.softmax(scores, axis=-1).astype(jnp.bfloat16)
        context = jnp.einsum('kgqs,skd->qkgd', attn_probs.astype(jnp.float32), v_heads.astype(jnp.float32)).astype(jnp.bfloat16)
        attn_out = jnp.dot(context.reshape(SEQ_LEN, HEADS * HEAD_DIM), w_attn_out, preferred_element_type=jnp.float32)
        mid_rows = (tok_rows.astype(jnp.float32) + rms_norm(attn_out, g_attn_out)).astype(jnp.bfloat16)
        h_moe = rms_norm(mid_rows, g_moe_in).astype(jnp.bfloat16)
        router_probs = jax.nn.softmax(jnp.dot(h_moe, w_router, preferred_element_type=jnp.float32), axis=-1)
        gate_probs = jnp.take_along_axis(router_probs, choice, axis=1)
        combine = jnp.sum(gate_probs[:, :, None] * (choice[:, :, None] == expert_ids).astype(jnp.float32), axis=1)

        def expert_step(moe_acc, expert_ops):
            w_gate_e, w_up_e, w_down_e, weight_col = expert_ops
            gate_act = jnp.dot(h_moe, w_gate_e, preferred_element_type=jnp.float32)
            up_act = jnp.dot(h_moe, w_up_e, preferred_element_type=jnp.float32)
            inner_act = (jax.nn.gelu(gate_act) * up_act).astype(jnp.bfloat16)
            expert_out = jnp.dot(inner_act, w_down_e, preferred_element_type=jnp.float32)
            return moe_acc + weight_col[:, None] * expert_out, None

        moe_out = lax.scan(expert_step, jnp.zeros((SEQ_LEN, D_MODEL), jnp.float32), (w_gate, w_up, w_down, combine.T))[0]
        y_rows = (mid_rows.astype(jnp.float32) + rms_norm(moe_out, g_moe_out)).astype(jnp.bfloat16)
        return y_rows, k_rope, v_heads

    y_out, k_cache, v_cache = lax.map(layer_prompt, (hidden, seq_lens, route_idx.reshape(BATCH, SEQ_LEN, TOP_K)))
    return y_out, k_cache, v_cache
```

```python
import functools
import jax
import jax.numpy as jnp
from jax import lax
from jax.experimental import pallas as pl
from jax.experimental.pallas import tpu as pltpu
from jax.sharding import PartitionSpec as P

HEAD_DIM = 128
LANES = 128
SOFT_CAP = 30.0
NORM_EPS = 1e-5
ROPE_BASE = 10000.0
ATTN_SCALE = HEAD_DIM ** -0.5
MESH = pl.DeviceIdType.MESH
ANY = pl.BlockSpec(memory_space=pl.ANY)
VMEM_FULL = pl.BlockSpec(memory_space=pltpu.VMEM)
DIRS = (1, -1)


def dot_f32(left_op, right_op):
    return jnp.dot(left_op, right_op, preferred_element_type=jnp.float32)


def rms_norm(values, gain_vec):
    values_f32 = values.astype(jnp.float32)
    inv_rms = lax.rsqrt(jnp.mean(values_f32 * values_f32, axis=-1, keepdims=True) + NORM_EPS)
    return values_f32 * inv_rms * gain_vec.astype(jnp.float32)


def rope_tables(seq_len):
    half_dim = HEAD_DIM // 2
    inv_freq = ROPE_BASE ** (-jnp.arange(half_dim, dtype=jnp.float32) * (2.0 / HEAD_DIM))
    angles = jnp.arange(seq_len, dtype=jnp.float32)[:, None] * inv_freq[None, :]
    return jnp.cos(angles)[:, None, :], jnp.sin(angles)[:, None, :]


def apply_rope(values, cos_t, sin_t):
    half_dim = HEAD_DIM // 2
    values_f32 = values.astype(jnp.float32)
    first_half = values_f32[..., :half_dim]
    second_half = values_f32[..., half_dim:]
    return jnp.concatenate([first_half * cos_t - second_half * sin_t, second_half * cos_t + first_half * sin_t], axis=-1).astype(jnp.bfloat16)


def attend_prompt(operands):
    q_rows, k_rows, v_rows, length = operands
    positions = jnp.arange(q_rows.shape[0])
    scores = jnp.einsum('qkgd,skd->kgqs', q_rows, k_rows, preferred_element_type=jnp.float32) * ATTN_SCALE
    scores = SOFT_CAP * jnp.tanh(scores / SOFT_CAP)
    allowed = (positions[None, :] <= positions[:, None]) & (positions[None, :] < length)
    scores = jnp.where(allowed, scores, -1e30)
    attn_probs = jax.nn.softmax(scores, axis=-1).astype(jnp.bfloat16)
    return jnp.einsum('kgqs,skd->qkgd', attn_probs, v_rows, preferred_element_type=jnp.float32).astype(jnp.bfloat16)


def attend_rows(q_proj, k_proj, v_proj, seq_lens):
    n_prompts = seq_lens.shape[0]
    seq_len = q_proj.shape[0] // n_prompts
    n_heads = q_proj.shape[1] // HEAD_DIM
    n_kv = k_proj.shape[1] // HEAD_DIM
    cos_t, sin_t = rope_tables(seq_len)
    q_rope = apply_rope(q_proj.reshape(n_prompts, seq_len, n_heads, HEAD_DIM), cos_t, sin_t)
    k_rope = apply_rope(k_proj.reshape(n_prompts, seq_len, n_kv, HEAD_DIM), cos_t, sin_t)
    v_heads = v_proj.reshape(n_prompts, seq_len, n_kv, HEAD_DIM)
    q_groups = q_rope.reshape(n_prompts, seq_len, n_kv, n_heads // n_kv, HEAD_DIM)
    context = lax.map(attend_prompt, (q_groups, k_rope, v_heads, seq_lens))
    return context.reshape(n_prompts * seq_len, n_heads * HEAD_DIM), k_rope, v_heads


class Place:
    def __init__(self, n):
        self.n = n
        self.chips = n // 2
        self.me = lax.axis_index('wg')
        self.dp = lax.axis_index('dp')
        self.chip = self.me // 2
        self.core = self.me % 2
        self.parity = self.dp % 2
        self.twin = self.dp + 1 - 2 * self.parity

    def at(self, offset, rel):
        return ((self.chip + offset + self.chips) % self.chips) * 2 + (self.core + rel) % 2

    def chip_at(self, offset):
        return (self.chip + offset + self.chips) % self.chips


class Wires:
    def __init__(self, place, send_sems, recv_sems):
        self.place, self.send_sems, self.recv_sems = place, send_sems, recv_sems
        self.slots = {}
        self.open = []

    def copy(self, name, src, dst, wg=None, dp=None):
        slot = self.slots.setdefault(name, len(self.slots))
        return pltpu.make_async_remote_copy(
            src_ref=src, dst_ref=dst, send_sem=self.send_sems.at[slot], recv_sem=self.recv_sems.at[slot],
            device_id={'dp': self.place.dp if dp is None else dp, 'wg': self.place.me if wg is None else wg},
            device_id_type=MESH)

    def send(self, name, src, dst, wg=None, dp=None):
        desc = self.copy(name, src, dst, wg, dp)
        desc.start()
        self.open.append(desc)

    def recv(self, name, dst):
        self.copy(name, dst, dst).wait_recv()

    def finish(self):
        for desc in self.open:
            desc.wait_send()
        self.open = []


def enter(place, with_twin):
    barrier = pltpu.get_barrier_semaphore()
    peers = [(place.dp, place.at(off, rel)) for off in DIRS for rel in (0, 1)] + [(place.dp, place.at(0, 1))]
    if with_twin:
        peers.append((place.twin, place.me))
    for dp, wg in peers:
        pl.semaphore_signal(barrier, inc=1, device_id={'dp': dp, 'wg': wg}, device_id_type=MESH)
    pl.semaphore_wait(barrier, len(peers))


def reshard_kernel(n, gate, up, down, wgu, wd, relay_gu, relay_d, send_sems, recv_sems, loc_sems):
    place = Place(n)
    wires = Wires(place, send_sems, recv_sems)
    experts, rows, cols = gate.shape[0], gate.shape[1], gate.shape[2] // n
    drows, dcols = down.shape[1], down.shape[2] // n
    half, quarter = experts // 2, experts // 4
    mine, theirs = place.parity * half, half - place.parity * half
    me = place.me

    def piece(arr, e0, cnt, j):
        if arr == 'd':
            return down.at[pl.ds(e0, cnt), :, pl.ds(pl.multiple_of(j * dcols, LANES), dcols)]
        return (gate if arr == 'g' else up).at[pl.ds(e0, cnt), :, pl.ds(pl.multiple_of(j * cols, LANES), cols)]

    def land(arr, e0, cnt, src):
        if arr == 'd':
            return wd.at[pl.ds(e0, cnt), pl.ds(pl.multiple_of(src * drows, drows), drows), :]
        row = pl.ds(pl.multiple_of(src * rows, rows), rows)
        if arr == 'gu':
            return wgu.at[pl.ds(e0, cnt), row, :]
        return wgu.at[pl.ds(e0, cnt), row, pl.ds(0 if arr == 'g' else cols, cols)]

    def relay(arr, side, rel):
        if arr == 'd':
            return relay_d.at[side, rel]
        if arr == 'gu':
            return relay_gu.at[side, rel]
        return relay_gu.at[side, rel, :, :, pl.ds(0 if arr == 'g' else cols, cols)]

    enter(place, True)
    local = []
    for i, arr in enumerate('gud'):
        desc = pltpu.make_async_copy(piece(arr, 0, experts, me), land(arr, 0, experts, me), loc_sems.at[i])
        desc.start()
        local.append(desc)

    def direct(rel, arrs):
        for arr in arrs:
            for d in DIRS:
                to = place.at(d, rel)
                wires.send(('direct', d, rel, arr), piece(arr, mine, half, to), land(arr, mine, half, me), wg=to)

    def first_leg(rel, arrs):
        for arr in arrs:
            for side, d in enumerate(DIRS):
                e0 = mine + side * quarter
                wires.send(('leg1', d, rel, arr), piece(arr, e0, quarter, place.at(2 * d, rel)), relay(arr, side, rel),
                           wg=place.at(d, 0))

    def to_twin(name, arr, e0, cnt, src):
        region = land(arr, e0, cnt, src)
        wires.send(name, region, region, dp=place.twin)

    direct(0, 'gud')
    sib = place.at(0, 1)
    for arr in 'gud':
        wires.send(('sib', arr), piece(arr, 0, experts, sib), land(arr, 0, experts, me), wg=sib)
    first_leg(0, 'gud')
    first_leg(1, 'gud')
    direct(1, 'gud')

    def direct_in(rel, arrs):
        for arr in arrs:
            for d in DIRS:
                src = place.at(-d, rel)
                if arr == 'gu':
                    wires.recv(('direct', d, rel, 'g'), land('g', mine, half, src))
                    wires.recv(('direct', d, rel, 'u'), land('u', mine, half, src))
                else:
                    wires.recv(('direct', d, rel, arr), land(arr, mine, half, src))
                to_twin(('twin', d, rel, arr), arr, mine, half, src)

    def second_leg(rel):
        for arr in ('gu', 'd'):
            for side, d in enumerate(DIRS):
                if arr == 'gu':
                    wires.recv(('leg1', d, rel, 'g'), relay('g', side, rel))
                    wires.recv(('leg1', d, rel, 'u'), relay('u', side, rel))
                else:
                    wires.recv(('leg1', d, rel, arr), relay(arr, side, rel))
                wires.send(('leg2', d, rel, arr), relay(arr, side, rel), land(arr, mine + side * quarter, quarter, place.at(-d, 0)),
                           wg=place.at(d, rel))

    direct_in(0, ('gu', 'd'))
    second_leg(0)
    second_leg(1)
    direct_in(1, ('gu', 'd'))
    for rel in (0, 1):
        for arr in ('gu', 'd'):
            for side, d in enumerate(DIRS):
                src = place.at(2 * d, rel)
                e0 = mine + side * quarter
                wires.recv(('leg2', d, rel, arr), land(arr, e0, quarter, src))
                to_twin(('twin2', d, rel, arr), arr, e0, quarter, src)
    for arr in 'gud':
        wires.recv(('sib', arr), land(arr, 0, experts, sib))
    for rel in (0, 1):
        for arr in ('gu', 'd'):
            for side, d in enumerate(DIRS):
                wires.recv(('twin', d, rel, arr), land(arr, theirs, half, place.at(-d, rel)))
                wires.recv(('twin2', d, rel, arr), land(arr, theirs + side * quarter, quarter, place.at(2 * d, rel)))
    for desc in local:
        desc.wait()
    wires.finish()


def reshard(n, gate, up, down):
    experts, rows, ff = gate.shape
    drows, d_model = down.shape[1:]
    cols, dcols = ff // n, d_model // n
    bf16 = jnp.bfloat16
    outs = pl.pallas_call(
        functools.partial(reshard_kernel, n),
        name='reshard',
        out_shape=(
            jax.ShapeDtypeStruct((experts, rows * n, 2 * cols), bf16),
            jax.ShapeDtypeStruct((experts, drows * n, dcols), bf16),
            jax.ShapeDtypeStruct((2, 2, experts // 4, rows, 2 * cols), bf16),
            jax.ShapeDtypeStruct((2, 2, experts // 4, drows, dcols), bf16),
        ),
        in_specs=[ANY] * 3,
        out_specs=(ANY,) * 4,
        scratch_shapes=[pltpu.SemaphoreType.DMA((64,)), pltpu.SemaphoreType.DMA((64,)), pltpu.SemaphoreType.DMA((4,))],
        compiler_params=pltpu.CompilerParams(collective_id=0, has_side_effects=True),
        cost_estimate=pl.CostEstimate(flops=100_000_000_000, bytes_accessed=50_000_000, transcendentals=0),
    )(gate, up, down)
    return outs[0], outs[1]


class Gather:
    def __init__(self, wires, name, region, half_region):
        self.wires, self.place, self.name = wires, wires.place, name
        self.region, self.half_region = region, half_region

    def start(self, src):
        place, dst = self.place, self.region(self.place.me)
        for d in DIRS:
            self.wires.send((self.name, 'own', d), src, dst, wg=place.at(d, 0))
        self.wires.send((self.name, 'own', 0), src, dst, wg=place.at(0, 1))

    def near_in(self, side):
        d, place = DIRS[side], self.place
        owner = place.at(-d, 0)
        block, part = self.region(owner), self.half_region(owner, side)
        self.wires.recv((self.name, 'own', d), block)
        self.wires.send((self.name, 'far', d), part, part, wg=place.at(d, 0))
        self.wires.send((self.name, 'across', d), block, block, wg=place.at(0, 1))

    def far_in(self):
        place = self.place
        owner = place.at(2, 0)
        for side, d in enumerate(DIRS):
            part = self.half_region(owner, side)
            self.wires.recv((self.name, 'far', d), part)
            self.wires.send((self.name, 'across2', d), part, part, wg=place.at(0, 1))

    def sib_own(self):
        self.wires.recv((self.name, 'own', 0), self.region(self.place.at(0, 1)))

    def sib_near(self, side):
        self.wires.recv((self.name, 'across', DIRS[side]), self.region(self.place.at(-DIRS[side], 1)))

    def sib_far(self):
        for side, d in enumerate(DIRS):
            self.wires.recv((self.name, 'across2', d), self.half_region(self.place.at(2, 1), side))


def moe_kernel(n, experts, h2, route, wr, wgu, wd, m_out, hg, relay_m,
               vgu, vd, hbuf, u_all, gates, us, mbuf, send_sems, recv_sems, load_sems, w_sems, out_sems):
    place = Place(n)
    wires = Wires(place, send_sems, recv_sems)
    steps, seq, d_model = h2.shape
    chips, me = place.chips, place.me
    cols = vgu.shape[2] // 2
    dcols = vd.shape[2]
    offsets = (0, -1, 1, 2)

    enter(place, False)
    h_gathers = []
    for t in range(steps):
        gather = Gather(wires, ('h', t), lambda owner, t=t: hg.at[t, owner],
                        lambda owner, side, t=t: hg.at[t, owner, pl.ds(side * (seq // 2), seq // 2), :])
        gather.start(h2.at[t])
        h_gathers.append(gather)
    w_loads = []
    for e in range(experts):
        desc = pltpu.make_async_copy(wgu.at[e], vgu.at[e], w_sems.at[e])
        desc.start()
        w_loads.append(desc)
    d_load = pltpu.make_async_copy(wd, vd, w_sems.at[experts])
    d_load.start()

    def u_owner_chip(owner, q):
        return (owner // 2 + offsets[q] + chips) % chips

    u_gathers = {}

    def fetch(t, q, slot):
        if q == 0:
            first = pltpu.make_async_copy(h2.at[t], hbuf.at[slot, place.core], load_sems.at[slot, 0])
            sib = 1 - place.core
            second = pltpu.make_async_copy(hg.at[t, place.at(0, 1)], hbuf.at[slot, sib], load_sems.at[slot, 1])
            return [first, second]
        chip = place.chip_at(offsets[q])
        return [pltpu.make_async_copy(hg.at[t, pl.ds(2 * chip, 2)], hbuf.at[slot], load_sems.at[slot, 0])]

    def arrive(t, q):
        gather = h_gathers[t]
        if q == 0:
            gather.sib_own()
        elif q < 3:
            gather.near_in(q - 1)
            gather.sib_near(q - 1)
        else:
            gather.far_in()
            gather.sib_far()

    def up_part(t, q, slot):
        chip = place.chip_at(offsets[q])
        h = hbuf.at[slot]
        rows = 2 * seq
        r0 = route[t, pl.ds(2 * chip, 2), 0].reshape(rows, LANES).astype(jnp.float32)
        r1 = route[t, pl.ds(2 * chip, 2), 1].reshape(rows, LANES).astype(jnp.float32)
        logits = dot_f32(h[...].reshape(rows, d_model), wr[...])
        lane = lax.broadcasted_iota(jnp.int32, (rows, LANES), 1)
        logits = jnp.where(lane < experts, logits, -1e30)
        peak = jnp.max(logits, axis=-1, keepdims=True)
        ex = jnp.where(lane < experts, jnp.exp(logits - peak), 0.0)
        probs = ex / jnp.sum(ex, axis=-1, keepdims=True)
        lane_f = lane.astype(jnp.float32)
        for i, r in enumerate((r0, r1)):
            g = jnp.sum(jnp.where(lane_f == r, probs, 0.0), axis=-1, keepdims=True)
            gates[t, chip, i] = jnp.broadcast_to(g, (rows, LANES))

        def expert(e, carry):
            act = dot_f32(h[...].reshape(rows, d_model), vgu[e])
            inner = (jax.nn.gelu(act[:, :cols]) * act[:, cols:]).astype(jnp.bfloat16).astype(jnp.float32)
            e_f = e.astype(jnp.float32)
            us[0] = jnp.where(route[t, pl.ds(2 * chip, 2), 0].reshape(rows, LANES).astype(jnp.float32) == e_f, inner, us[0])
            us[1] = jnp.where(route[t, pl.ds(2 * chip, 2), 1].reshape(rows, LANES).astype(jnp.float32) == e_f, inner, us[1])
            return carry

        us[...] = jnp.zeros_like(us)
        lax.fori_loop(0, experts, expert, 0)
        for i in range(2):
            u_all[t, chip, me, :, pl.ds(i * cols, cols)] = us[i].astype(jnp.bfloat16)
        gather = Gather(wires, ('u', t, q), lambda owner: u_all.at[t, u_owner_chip(owner, q), owner],
                        lambda owner, side: u_all.at[t, u_owner_chip(owner, q), owner, pl.ds(side * seq, seq), :])
        gather.start(u_all.at[t, chip, me])
        u_gathers[t, q] = gather

    def phase_a(t):
        for q in range(4):
            arrive(t, q)
            loads = fetch(t, q, q % 2)
            for desc in loads:
                desc.start()
            for desc in loads:
                desc.wait()
            if t == 0 and q == 0:
                for desc in w_loads:
                    desc.wait()
            up_part(t, q, q % 2)

    def u_near(t):
        for q in range(4):
            u_gathers[t, q].near_in(0)
            u_gathers[t, q].near_in(1)

    m_open = []

    def phase_b(t):
        if t == 0:
            d_load.wait()
        for q in range(4):
            gather = u_gathers[t, q]
            gather.far_in()
            gather.sib_own()
            gather.sib_near(0)
            gather.sib_near(1)
            gather.sib_far()
        for q in range(4):
            chip = place.chip_at(offsets[q])
            rows = 2 * seq
            acc = mbuf.at[t, q]
            acc[...] = jnp.zeros_like(acc)

            def expert(e, carry):
                e_b = e.astype(jnp.bfloat16)
                r0 = route[t, pl.ds(2 * chip, 2), 0].reshape(rows, LANES)
                r1 = route[t, pl.ds(2 * chip, 2), 1].reshape(rows, LANES)
                m0, m1 = r0 == e_b, r1 == e_b
                zero = jnp.zeros((rows, LANES), jnp.bfloat16)
                parts = []
                for j in range(n):
                    parts.append(jnp.where(m0, u_all[t, chip, j, :, pl.ds(0, cols)],
                                           jnp.where(m1, u_all[t, chip, j, :, pl.ds(cols, cols)], zero)))
                ue = jnp.concatenate(parts, axis=1)
                out = dot_f32(ue, vd[e])
                e_f = e.astype(jnp.float32)
                gate = jnp.where(r0.astype(jnp.float32) == e_f, gates[t, chip, 0],
                                 jnp.where(r1.astype(jnp.float32) == e_f, gates[t, chip, 1], 0.0))
                acc[...] += jnp.concatenate([gate] * (dcols // LANES), axis=1) * out
                return carry

            lax.fori_loop(0, experts, expert, 0)
            own_cols = pl.ds(pl.multiple_of(me * dcols, LANES), dcols)
            dst = m_out.at[t, :, own_cols]
            for rel in (0, 1):
                target_core = (place.core + rel) % 2
                part = acc.at[pl.ds(pl.multiple_of(target_core * seq, seq), seq), :]
                if q == 0 and rel == 0:
                    desc = pltpu.make_async_copy(part, dst, out_sems.at[t])
                    desc.start()
                    m_open.append(desc)
                elif q < 3:
                    wires.send(('m', t, q, rel), part, dst, wg=place.at(offsets[q], rel))
                else:
                    wires.send(('m1', t, rel), part, relay_m.at[t, rel], wg=place.at(DIRS[rel], 0))

    def m_relay(t):
        for rel, d in enumerate(DIRS):
            wires.recv(('m1', t, rel), relay_m.at[t, rel])
            src = place.at(-d, 0)
            wires.send(('m2', t, rel), relay_m.at[t, rel], m_out.at[t, :, pl.ds(pl.multiple_of(src * dcols, LANES), dcols)],
                       wg=place.at(d, rel))

    def m_in(t):
        for q in range(4):
            for rel in (0, 1):
                src = place.at(-offsets[q], rel)
                dst = m_out.at[t, :, pl.ds(pl.multiple_of(src * dcols, LANES), dcols)]
                if q == 0 and rel == 0:
                    continue
                wires.recv(('m', t, q, rel) if q < 3 else ('m2', t, rel), dst)

    phase_a(0)
    for t in range(1, steps):
        phase_a(t)
        u_near(t - 1)
    phase_b(0)
    u_near(steps - 1)
    for t in range(1, steps):
        phase_b(t)
        m_relay(t - 1)
    m_relay(steps - 1)
    for t in range(steps):
        m_in(t)
    for desc in m_open:
        desc.wait()
    wires.finish()


def moe(n, h2, route, wr, wgu, wd):
    steps, seq, d_model = h2.shape
    experts, _, two_cols = wgu.shape
    ff, dcols = wd.shape[1:]
    bf16, f32 = jnp.bfloat16, jnp.float32
    n_sems = steps * 64
    outs = pl.pallas_call(
        functools.partial(moe_kernel, n, experts),
        name='moe',
        out_shape=(
            jax.ShapeDtypeStruct((steps, seq, d_model), f32),
            jax.ShapeDtypeStruct((steps, n, seq, d_model), bf16),
            jax.ShapeDtypeStruct((steps, 2, seq, dcols), f32),
        ),
        in_specs=[ANY, VMEM_FULL, VMEM_FULL, ANY, ANY],
        out_specs=(ANY,) * 3,
        scratch_shapes=[
            pltpu.VMEM((experts, d_model, two_cols), bf16),
            pltpu.VMEM((experts, ff, dcols), bf16),
            pltpu.VMEM((2, 2, seq, d_model), bf16),
            pltpu.VMEM((steps, n // 2, n, 2 * seq, two_cols), bf16),
            pltpu.VMEM((steps, n // 2, 2, 2 * seq, LANES), f32),
            pltpu.VMEM((2, 2 * seq, two_cols // 2), f32),
            pltpu.VMEM((steps, 4, 2 * seq, dcols), f32),
            pltpu.SemaphoreType.DMA((n_sems,)),
            pltpu.SemaphoreType.DMA((n_sems,)),
            pltpu.SemaphoreType.DMA((2, 2)),
            pltpu.SemaphoreType.DMA((experts + 1,)),
            pltpu.SemaphoreType.DMA((steps,)),
        ],
        compiler_params=pltpu.CompilerParams(collective_id=1, has_side_effects=True, vmem_limit_bytes=66_000_000),
        cost_estimate=pl.CostEstimate(flops=77_000_000_000, bytes_accessed=100_000_000, transcendentals=0),
    )(h2, route, wr, wgu, wd)
    return outs[0]


def solution(mesh):
    n = mesh.shape['wg']
    row_spec = P(('dp', 'wg'))
    dim0_spec = P('wg', None)
    dim1_spec = P(None, 'wg', None)
    gather_dim0 = functools.partial(lax.all_gather, axis_name='wg', axis=0, tiled=True)

    def device_fn(hidden, seq_lens, route_idx, g_attn_in, w_query, w_key, w_value, w_attn_out, g_attn_out, g_moe_in, w_router, w_gate, w_up, w_down, g_moe_out):
        n_prompts, seq_len, d_model = hidden.shape
        experts = w_router.shape[1]
        small = jnp.concatenate([w_router] + [g[:, None] for g in (g_attn_in, g_attn_out, g_moe_in, g_moe_out)], axis=1)
        small = gather_dim0(small)
        g_attn_in, g_attn_out, g_moe_in, g_moe_out = (small[:, experts + i] for i in range(4))
        wr = jnp.pad(small[:, :experts], ((0, 0), (0, LANES - experts)))
        route = lax.all_gather(route_idx, 'wg', axis=0, tiled=False)
        route = route.reshape(n, n_prompts, seq_len, 2).transpose(1, 0, 3, 2).astype(jnp.bfloat16)
        route = jnp.broadcast_to(route[..., None], route.shape + (LANES,))
        wgu, wd = reshard(n, w_gate, w_up, w_down)

        tok_rows = hidden.reshape(n_prompts * seq_len, d_model)
        h_attn = rms_norm(tok_rows, g_attn_in).astype(jnp.bfloat16)
        q_proj = dot_f32(h_attn, gather_dim0(w_query)).astype(jnp.bfloat16)
        k_proj = dot_f32(h_attn, gather_dim0(w_key)).astype(jnp.bfloat16)
        v_proj = dot_f32(h_attn, gather_dim0(w_value)).astype(jnp.bfloat16)
        context_rows, k_rope, v_heads = attend_rows(q_proj, k_proj, v_proj, seq_lens)
        attn_out = dot_f32(context_rows, gather_dim0(w_attn_out))
        mid_rows = (tok_rows.astype(jnp.float32) + rms_norm(attn_out, g_attn_out)).astype(jnp.bfloat16)
        h_moe = rms_norm(mid_rows, g_moe_in).astype(jnp.bfloat16)
        moe_out = moe(n, h_moe.reshape(hidden.shape), route, wr, wgu, wd).reshape(tok_rows.shape)
        y_rows = (mid_rows.astype(jnp.float32) + rms_norm(moe_out, g_moe_out)).astype(jnp.bfloat16)
        return y_rows.reshape(hidden.shape), k_rope, v_heads

    return jax.shard_map(
        device_fn,
        mesh=mesh,
        in_specs=(row_spec, row_spec, row_spec, P('wg'), dim0_spec, dim0_spec, dim0_spec, dim0_spec, P('wg'), P('wg'), dim0_spec, dim1_spec, dim1_spec, dim1_spec, P('wg')),
        out_specs=(row_spec, row_spec, row_spec),
        check_vma=False,
    )
```

```python
import functools
import jax
import jax.numpy as jnp
from jax import lax
from jax.experimental import pallas as pl
from jax.experimental.pallas import tpu as pltpu
from jax.sharding import PartitionSpec as P

HEAD_DIM = 128
LANES = 128
SOFT_CAP = 30.0
NORM_EPS = 1e-5
ROPE_BASE = 10000.0
ATTN_SCALE = HEAD_DIM ** -0.5
MESH = pl.DeviceIdType.MESH
ANY = pl.BlockSpec(memory_space=pl.ANY)
VMEM_FULL = pl.BlockSpec(memory_space=pltpu.VMEM)
DIRS = (1, -1)


def dot_f32(left_op, right_op):
    return jnp.dot(left_op, right_op, preferred_element_type=jnp.float32)


def rms_norm(values, gain_vec):
    values_f32 = values.astype(jnp.float32)
    inv_rms = lax.rsqrt(jnp.mean(values_f32 * values_f32, axis=-1, keepdims=True) + NORM_EPS)
    return values_f32 * inv_rms * gain_vec.astype(jnp.float32)


def rope_tables(seq_len):
    half_dim = HEAD_DIM // 2
    inv_freq = ROPE_BASE ** (-jnp.arange(half_dim, dtype=jnp.float32) * (2.0 / HEAD_DIM))
    angles = jnp.arange(seq_len, dtype=jnp.float32)[:, None] * inv_freq[None, :]
    cos_t, sin_t = jnp.cos(angles), jnp.sin(angles)
    return jnp.concatenate([cos_t, cos_t], axis=1), jnp.concatenate([-sin_t, sin_t], axis=1)


class Place:
    def __init__(self, n):
        self.n = n
        self.chips = n // 2
        self.me = lax.axis_index('wg')
        self.dp = lax.axis_index('dp')
        self.chip = self.me // 2
        self.core = self.me % 2
        self.parity = self.dp % 2
        self.twin = self.dp + 1 - 2 * self.parity

    def at(self, offset, rel):
        return ((self.chip + offset + self.chips) % self.chips) * 2 + (self.core + rel) % 2

    def chip_at(self, offset):
        return (self.chip + offset + self.chips) % self.chips


class Wires:
    def __init__(self, place, send_sems, recv_sems):
        self.place, self.send_sems, self.recv_sems = place, send_sems, recv_sems
        self.slots = {}
        self.open = []

    def copy(self, name, src, dst, wg=None, dp=None):
        slot = self.slots.setdefault(name, len(self.slots))
        return pltpu.make_async_remote_copy(
            src_ref=src, dst_ref=dst, send_sem=self.send_sems.at[slot], recv_sem=self.recv_sems.at[slot],
            device_id={'dp': self.place.dp if dp is None else dp, 'wg': self.place.me if wg is None else wg},
            device_id_type=MESH)

    def send(self, name, src, dst, wg=None, dp=None):
        desc = self.copy(name, src, dst, wg, dp)
        desc.start()
        self.open.append(desc)

    def recv(self, name, dst):
        self.copy(name, dst, dst).wait_recv()

    def finish(self):
        for desc in self.open:
            desc.wait_send()
        self.open = []


def enter(place, with_twin):
    barrier = pltpu.get_barrier_semaphore()
    peers = [(place.dp, place.at(off, rel)) for off in (1, -1, 2) for rel in (0, 1)] + [(place.dp, place.at(0, 1))]
    if with_twin:
        peers.append((place.twin, place.me))
    for dp, wg in peers:
        pl.semaphore_signal(barrier, inc=1, device_id={'dp': dp, 'wg': wg}, device_id_type=MESH)
    pl.semaphore_wait(barrier, len(peers))


class Reshard:
    def __init__(self, wires, gate, up, down, wgu, wd, relay_gu, relay_d, loc_sems):
        self.wires, self.place = wires, wires.place
        n = self.place.n
        self.gate, self.up, self.down, self.wgu, self.wd = gate, up, down, wgu, wd
        self.relay_gu, self.relay_d, self.loc_sems = relay_gu, relay_d, loc_sems
        self.experts, self.rows, self.cols = gate.shape[0], gate.shape[1], gate.shape[2] // n
        self.drows, self.dcols = down.shape[1], down.shape[2] // n
        self.half, self.quarter = self.experts // 2, self.experts // 4
        self.mine = self.place.parity * self.half
        self.theirs = self.half - self.mine

    def piece(self, arr, e0, cnt, j):
        if arr == 'd':
            return self.down.at[pl.ds(e0, cnt), :, pl.ds(pl.multiple_of(j * self.dcols, LANES), self.dcols)]
        ref = self.gate if arr == 'g' else self.up
        return ref.at[pl.ds(e0, cnt), :, pl.ds(pl.multiple_of(j * self.cols, LANES), self.cols)]

    def land(self, arr, e0, cnt, src):
        if arr == 'd':
            return self.wd.at[pl.ds(e0, cnt), pl.ds(pl.multiple_of(src * self.drows, self.drows), self.drows), :]
        row = pl.ds(pl.multiple_of(src * self.rows, self.rows), self.rows)
        if arr == 'gu':
            return self.wgu.at[pl.ds(e0, cnt), row, :]
        return self.wgu.at[pl.ds(e0, cnt), row, pl.ds(0 if arr == 'g' else self.cols, self.cols)]

    def relay(self, arr, side, rel):
        if arr == 'd':
            return self.relay_d.at[side, rel]
        if arr == 'gu':
            return self.relay_gu.at[side, rel]
        return self.relay_gu.at[side, rel, :, :, pl.ds(0 if arr == 'g' else self.cols, self.cols)]

    def span(self, arr):
        return (self.mine, self.half) if arr == 'd' else (0, self.experts)

    def near(self):
        me, sib = self.place.me, self.place.at(0, 1)
        self.local = []
        for i, arr in enumerate('gud'):
            e0, cnt = self.span(arr)
            self.wires.send(('sib', arr), self.piece(arr, e0, cnt, sib), self.land(arr, e0, cnt, me), wg=sib)
            desc = pltpu.make_async_copy(self.piece(arr, e0, cnt, me), self.land(arr, e0, cnt, me), self.loc_sems.at[i])
            desc.start()
            self.local.append(desc)

    def direct(self, rel, arrs):
        for arr in arrs:
            for d in DIRS:
                to = self.place.at(d, rel)
                self.wires.send(('direct', d, rel, arr), self.piece(arr, self.mine, self.half, to),
                                self.land(arr, self.mine, self.half, self.place.me), wg=to)

    def first_leg(self, rel, arrs):
        for arr in arrs:
            for side, d in enumerate(DIRS):
                e0 = self.mine + side * self.quarter
                self.wires.send(('leg1', d, rel, arr), self.piece(arr, e0, self.quarter, self.place.at(2 * d, rel)),
                                self.relay(arr, side, rel), wg=self.place.at(d, 0))

    def to_twin(self, name, arr, e0, cnt, src):
        if arr != 'd':
            region = self.land(arr, e0, cnt, src)
            self.wires.send(name, region, region, dp=self.place.twin)

    def direct_in(self, rel):
        for arr in ('gu', 'd'):
            for d in DIRS:
                src = self.place.at(-d, rel)
                for part in arr:
                    self.wires.recv(('direct', d, rel, part), self.land(part, self.mine, self.half, src))
                self.to_twin(('twin', d, rel, arr), arr, self.mine, self.half, src)

    def second_leg(self, rel):
        for arr in ('gu', 'd'):
            for side, d in enumerate(DIRS):
                for part in arr:
                    self.wires.recv(('leg1', d, rel, part), self.relay(part, side, rel))
                self.wires.send(('leg2', d, rel, arr), self.relay(arr, side, rel),
                                self.land(arr, self.mine + side * self.quarter, self.quarter, self.place.at(-d, 0)),
                                wg=self.place.at(d, rel))

    def far_in(self):
        for arr in ('gu', 'd'):
            for rel in (0, 1):
                for side, d in enumerate(DIRS):
                    src = self.place.at(2 * d, rel)
                    e0 = self.mine + side * self.quarter
                    self.wires.recv(('leg2', d, rel, arr), self.land(arr, e0, self.quarter, src))
                    self.to_twin(('twin2', d, rel, arr), arr, e0, self.quarter, src)

    def finish(self):
        for arr in 'gud':
            e0, cnt = self.span(arr)
            self.wires.recv(('sib', arr), self.land(arr, e0, cnt, self.place.at(0, 1)))
        for rel in (0, 1):
            for side, d in enumerate(DIRS):
                self.wires.recv(('twin', d, rel, 'gu'), self.land('gu', self.theirs, self.half, self.place.at(-d, rel)))
                self.wires.recv(('twin2', d, rel, 'gu'),
                                self.land('gu', self.theirs + side * self.quarter, self.quarter, self.place.at(2 * d, rel)))
        for desc in self.local:
            desc.wait()


class PairGather:
    def __init__(self, wires, name, src, dst):
        self.wires, self.place, self.name, self.src, self.dst = wires, wires.place, name, src, dst
        rows = src.shape[0]
        self.rows = rows
        self.given = rows * 5 // 16
        self.reach = rows - self.given
        parity = self.place.parity
        self.start_row = parity * self.given
        self.give_row = parity * self.reach
        self.take_row = self.reach - self.give_row

    def part(self, owner, row, cnt):
        return self.dst.at[owner, pl.ds(pl.multiple_of(row, 16), cnt), :]

    def line(self, owner):
        return self.part(owner, self.start_row, self.reach)

    def half(self, owner, side):
        return self.part(owner, self.start_row + side * (self.reach // 2), self.reach // 2)

    def start(self):
        place, me = self.place, self.place.me
        own = self.src.at[pl.ds(pl.multiple_of(self.start_row, 16), self.reach), :]
        for d in DIRS:
            self.wires.send((self.name, 'own', d), own, self.line(me), wg=place.at(d, 0))
        self.wires.send((self.name, 'own', 0), self.src, self.dst.at[me], wg=place.at(0, 1))

    def give(self, tag, owner):
        part = self.part(owner, self.give_row, self.given)
        self.wires.send((self.name, 'give', tag), part, part, dp=self.place.twin)

    def near_in(self):
        place = self.place
        for side, d in enumerate(DIRS):
            owner = place.at(-d, 0)
            self.wires.recv((self.name, 'own', d), self.line(owner))
            far = self.half(owner, side)
            self.wires.send((self.name, 'far', d), far, far, wg=place.at(d, 0))
            self.give(d, owner)
            self.wires.send((self.name, 'across', d), self.line(owner), self.line(owner), wg=place.at(0, 1))

    def far_in(self):
        place = self.place
        owner = place.at(2, 0)
        for side, d in enumerate(DIRS):
            part = self.half(owner, side)
            self.wires.recv((self.name, 'far', d), part)
            self.wires.send((self.name, 'across2', d), part, part, wg=place.at(0, 1))
        self.give(2, owner)

    def twin_in(self, tags):
        for tag in tags:
            part = self.part(self.place.at(-tag, 0), self.take_row, self.given)
            self.wires.recv((self.name, 'give', tag), part)
            self.wires.send((self.name, 'across3', tag), part, part, wg=self.place.at(0, 1))

    def sib_in(self):
        place = self.place
        self.wires.recv((self.name, 'own', 0), self.dst.at[place.at(0, 1)])
        for side, d in enumerate(DIRS):
            self.wires.recv((self.name, 'across', d), self.line(place.at(-d, 1)))
            self.wires.recv((self.name, 'across2', d), self.half(place.at(2, 1), side))
        for tag in (1, -1, 2):
            self.wires.recv((self.name, 'across3', tag), self.part(place.at(-tag, 1), self.take_row, self.given))


def attention_kernel(n, experts, hidden, small, mask, cos_t, sin_t, wq, wk, wv, wo, gate, up, down,
                     x1, h2, k_out, v_out, small_all, gq, gk, gv, go, wgu, wd, relay_gu, relay_d,
                     h, acc, ctx, wbuf, send_sems, recv_sems, loc_sems, load_sems):
    place = Place(n)
    wires = Wires(place, send_sems, recv_sems)
    me = place.me
    prompts, seq = mask.shape[0], mask.shape[1]
    rows, d_model = hidden.shape
    depth = wq.shape[0]
    q_dim, kv_dim = wq.shape[1], wk.shape[1]
    n_kv = kv_dim // HEAD_DIM
    group = q_dim // kv_dim
    tile = 512
    row_tile = seq

    enter(place, True)
    others = [(off, rel) for off in (0, 1, -1, 2) for rel in (0, 1)][1:]
    for off, rel in others:
        wires.send(('small', off, rel), small, small_all.at[me], wg=place.at(off, rel))
    gather_q = PairGather(wires, 'q', wq, gq)
    gather_k = PairGather(wires, 'k', wk, gk)
    gather_v = PairGather(wires, 'v', wv, gv)
    gather_o = PairGather(wires, 'o', wo, go)
    moving = Reshard(wires, gate, up, down, wgu, wd, relay_gu, relay_d, loc_sems)
    gather_q.start()
    gather_k.start()
    gather_v.start()
    small_all[me] = small[...]
    for off, rel in others:
        wires.recv(('small', off, rel), small_all.at[place.at(-off, rel)])

    def gain(i):
        return jnp.concatenate([small_all[j, pl.ds(experts + i, 1), :] for j in range(n)], axis=1).astype(jnp.float32)

    def norm(values):
        return values * lax.rsqrt(jnp.mean(values * values, axis=-1, keepdims=True) + NORM_EPS)

    def norm_in(i, carry):
        r = pl.ds(pl.multiple_of(i * 16, 16), 16)
        h[r, :] = (norm(hidden[r, :].astype(jnp.float32)) * gain(0)).astype(jnp.bfloat16)
        return carry

    lax.fori_loop(0, rows // 16, norm_in, 0)
    acc[...] = jnp.zeros_like(acc)

    gather_q.near_in()
    gather_o.start()
    gather_k.near_in()
    gather_v.near_in()
    moving.direct(0, 'gu')
    moving.near()
    gather_q.twin_in((1, -1))
    gather_q.far_in()
    gather_k.twin_in((1, -1))
    gather_v.twin_in((1, -1))
    gather_k.far_in()
    gather_v.far_in()
    gather_q.twin_in((2,))
    gather_k.twin_in((2,))
    gather_v.twin_in((2,))
    gather_q.sib_in()
    gather_k.sib_in()
    gather_v.sib_in()

    def owner_of(i):
        return (me + i) % n

    def product(lhs, weights, first_col):
        def loads(i, slot):
            owner = owner_of(i)

            def start(own):
                col = 0
                for w, (src, gathered) in enumerate(weights):
                    width = src.shape[1]
                    pltpu.make_async_copy(src if own else gathered.at[owner], wbuf.at[slot, :, pl.ds(col, width)],
                                          load_sems.at[slot, w]).start()
                    col += width

            @pl.when(i == 0)
            def _():
                start(True)

            @pl.when(i > 0)
            def _():
                start(False)

        def step(i, carry):
            slot = i % 2
            owner = owner_of(i)

            @pl.when(i + 1 < n)
            def _():
                loads(i + 1, 1 - slot)

            col = 0
            for w, (src, gathered) in enumerate(weights):
                width = src.shape[1]
                pltpu.make_async_copy(gathered.at[owner], wbuf.at[slot, :, pl.ds(col, width)], load_sems.at[slot, w]).wait()
                col += width

            def tiles(j, carry):
                c = pl.ds(pl.multiple_of(j * tile, tile), tile)
                acc[:, c] += dot_f32(lhs[:, pl.ds(pl.multiple_of(owner * depth, depth), depth)], wbuf[slot, :, c])
                return carry

            return lax.fori_loop(0, col // tile, tiles, carry)

        loads(0, 0)
        lax.fori_loop(0, n, step, 0)

    product(h, ((wq, gq), (wk, gk), (wv, gv)), 0)

    def rope(values):
        values = values.astype(jnp.bfloat16).astype(jnp.float32)
        cos_v, sin_v = cos_t[...], sin_t[...]
        times = values.shape[0] // seq
        if times > 1:
            cos_v, sin_v = jnp.concatenate([cos_v] * times, axis=0), jnp.concatenate([sin_v] * times, axis=0)
        return (values * cos_v + pltpu.roll(values, HEAD_DIM // 2, 1) * sin_v).astype(jnp.bfloat16)

    def attend(i, carry):
        p, g = i // n_kv, i % n_kv
        r = pl.ds(pl.multiple_of(p * seq, seq), seq)
        kv_cols = pl.ds(pl.multiple_of(g * HEAD_DIM, HEAD_DIM), HEAD_DIM)
        q = jnp.concatenate([acc[r, pl.ds(pl.multiple_of((g * group + j) * HEAD_DIM, HEAD_DIM), HEAD_DIM)]
                             for j in range(group)], axis=0)
        q = rope(q)
        k = rope(acc[r, pl.ds(pl.multiple_of(q_dim + g * HEAD_DIM, HEAD_DIM), HEAD_DIM)])
        v = acc[r, pl.ds(pl.multiple_of(q_dim + kv_dim + g * HEAD_DIM, HEAD_DIM), HEAD_DIM)].astype(jnp.bfloat16)
        k_out[r, kv_cols] = k
        v_out[r, kv_cols] = v
        scores = lax.dot_general(q, k, (((1,), (1,)), ((), ())), preferred_element_type=jnp.float32) * ATTN_SCALE
        scores = SOFT_CAP * jnp.tanh(scores / SOFT_CAP)
        allowed = jnp.concatenate([mask[p]] * group, axis=0) > 0.5
        scores = jnp.where(allowed, scores, -1e30)
        ex = jnp.exp(scores - jnp.max(scores, axis=-1, keepdims=True))
        probs = (ex / jnp.sum(ex, axis=-1, keepdims=True)).astype(jnp.bfloat16)
        out = dot_f32(probs, v).astype(jnp.bfloat16)
        for j in range(group):
            ctx[r, pl.ds(pl.multiple_of((g * group + j) * HEAD_DIM, HEAD_DIM), HEAD_DIM)] = out[j * seq:(j + 1) * seq]
        return carry

    lax.fori_loop(0, prompts * n_kv, attend, 0)

    gather_o.near_in()
    moving.direct(0, 'd')
    moving.first_leg(0, 'gud')
    moving.first_leg(1, 'gud')
    moving.direct(1, 'gud')
    gather_o.twin_in((1, -1))
    gather_o.far_in()
    moving.direct_in(0)
    gather_o.twin_in((2,))
    gather_o.sib_in()
    acc[...] = jnp.zeros_like(acc)
    product(ctx, ((wo, go),), 0)

    def finish_rows(i, carry):
        r = pl.ds(pl.multiple_of(i * 16, 16), 16)
        mid = (hidden[r, :].astype(jnp.float32) + norm(acc[r, pl.ds(0, d_model)]) * gain(1)).astype(jnp.bfloat16)
        x1[r, :] = mid
        h2[r, :] = (norm(mid.astype(jnp.float32)) * gain(2)).astype(jnp.bfloat16)
        return carry

    lax.fori_loop(0, rows // 16, finish_rows, 0)
    moving.second_leg(0)
    moving.second_leg(1)
    moving.direct_in(1)
    moving.far_in()
    moving.finish()
    wires.finish()


def attention(n, experts, hidden, small, mask, cos_t, sin_t, wq, wk, wv, wo, gate, up, down):
    rows, d_model = hidden.shape
    ff = gate.shape[2]
    drows = down.shape[1]
    cols, dcols = ff // n, d_model // n
    bf16, f32 = jnp.bfloat16, jnp.float32
    quarter = experts // 4

    def full(w):
        return jax.ShapeDtypeStruct((n,) + w.shape, bf16)

    outs = pl.pallas_call(
        functools.partial(attention_kernel, n, experts),
        name='attention',
        out_shape=(
            jax.ShapeDtypeStruct((rows, d_model), bf16),
            jax.ShapeDtypeStruct((rows, d_model), bf16),
            jax.ShapeDtypeStruct((rows, wk.shape[1]), bf16),
            jax.ShapeDtypeStruct((rows, wv.shape[1]), bf16),
            full(small), full(wq), full(wk), full(wv), full(wo),
            jax.ShapeDtypeStruct((experts, d_model, 2 * cols), bf16),
            jax.ShapeDtypeStruct((experts, drows * n, dcols), bf16),
            jax.ShapeDtypeStruct((2, 2, quarter, gate.shape[1], 2 * cols), bf16),
            jax.ShapeDtypeStruct((2, 2, quarter, drows, dcols), bf16),
        ),
        in_specs=[VMEM_FULL] * 5 + [ANY] * 7,
        out_specs=(VMEM_FULL,) * 5 + (ANY,) * 8,
        scratch_shapes=[
            pltpu.VMEM((rows, d_model), bf16),
            pltpu.VMEM((rows, wq.shape[1] + 2 * wk.shape[1]), f32),
            pltpu.VMEM((rows, wq.shape[1]), bf16),
            pltpu.VMEM((2, wq.shape[0], wq.shape[1] + 2 * wk.shape[1]), bf16),
            pltpu.SemaphoreType.DMA((160,)),
            pltpu.SemaphoreType.DMA((160,)),
            pltpu.SemaphoreType.DMA((4,)),
            pltpu.SemaphoreType.DMA((2, 3)),
        ],
        compiler_params=pltpu.CompilerParams(collective_id=0, has_side_effects=True, vmem_limit_bytes=62_000_000),
        cost_estimate=pl.CostEstimate(flops=33_000_000_000, bytes_accessed=300_000_000, transcendentals=0),
    )(hidden, small, mask, cos_t, sin_t, wq, wk, wv, wo, gate, up, down)
    return outs[0], outs[1], outs[2], outs[3], outs[4], outs[9], outs[10]


class Gather:
    def __init__(self, wires, name, region, half_region):
        self.wires, self.place, self.name = wires, wires.place, name
        self.region, self.half_region = region, half_region

    def start(self, src):
        place, dst = self.place, self.region(self.place.me)
        for d in DIRS:
            self.wires.send((self.name, 'own', d), src, dst, wg=place.at(d, 0))
        self.wires.send((self.name, 'own', 0), src, dst, wg=place.at(0, 1))

    def near_in(self, side):
        d, place = DIRS[side], self.place
        owner = place.at(-d, 0)
        block, part = self.region(owner), self.half_region(owner, side)
        self.wires.recv((self.name, 'own', d), block)
        self.wires.send((self.name, 'far', d), part, part, wg=place.at(d, 0))
        self.wires.send((self.name, 'across', d), block, block, wg=place.at(0, 1))

    def far_in(self):
        place = self.place
        owner = place.at(2, 0)
        for side, d in enumerate(DIRS):
            part = self.half_region(owner, side)
            self.wires.recv((self.name, 'far', d), part)
            self.wires.send((self.name, 'across2', d), part, part, wg=place.at(0, 1))

    def sib_own(self):
        self.wires.recv((self.name, 'own', 0), self.region(self.place.at(0, 1)))

    def sib_near(self, side):
        self.wires.recv((self.name, 'across', DIRS[side]), self.region(self.place.at(-DIRS[side], 1)))

    def sib_far(self):
        for side, d in enumerate(DIRS):
            self.wires.recv((self.name, 'across2', d), self.half_region(self.place.at(2, 1), side))


def moe_kernel(n, experts, h2, route, wr, wgu, wd, m_out, hg, relay_m,
               vgu, vd, hbuf, u_all, gates, us, mbuf, send_sems, recv_sems, load_sems, w_sems, out_sems):
    place = Place(n)
    wires = Wires(place, send_sems, recv_sems)
    steps, seq, d_model = h2.shape
    chips, me = place.chips, place.me
    cols = vgu.shape[2] // 2
    dcols = vd.shape[2]
    offsets = (0, -1, 1, 2)

    enter(place, True)
    h_gathers = []
    for t in range(steps):
        gather = Gather(wires, ('h', t), lambda owner, t=t: hg.at[t, owner],
                        lambda owner, side, t=t: hg.at[t, owner, pl.ds(side * (seq // 2), seq // 2), :])
        gather.start(h2.at[t])
        h_gathers.append(gather)
    w_loads = []
    for e in range(experts):
        desc = pltpu.make_async_copy(wgu.at[e], vgu.at[e], w_sems.at[e])
        desc.start()
        w_loads.append(desc)
    half = experts // 2
    mine, theirs = place.parity * half, half - place.parity * half
    own_half, their_half = vd.at[pl.ds(mine, half)], vd.at[pl.ds(theirs, half)]
    d_load = pltpu.make_async_copy(wd.at[pl.ds(mine, half)], own_half, w_sems.at[experts])
    d_load.start()
    d_load.wait()
    wires.send('d', own_half, own_half, dp=place.twin)

    def u_owner_chip(owner, q):
        return (owner // 2 + offsets[q] + chips) % chips

    u_gathers = {}

    def fetch(t, q, slot):
        if q == 0:
            first = pltpu.make_async_copy(h2.at[t], hbuf.at[slot, place.core], load_sems.at[slot, 0])
            sib = 1 - place.core
            second = pltpu.make_async_copy(hg.at[t, place.at(0, 1)], hbuf.at[slot, sib], load_sems.at[slot, 1])
            return [first, second]
        chip = place.chip_at(offsets[q])
        return [pltpu.make_async_copy(hg.at[t, pl.ds(2 * chip, 2)], hbuf.at[slot], load_sems.at[slot, 0])]

    def arrive(t, q):
        gather = h_gathers[t]
        if q == 0:
            gather.sib_own()
        elif q < 3:
            gather.near_in(q - 1)
            gather.sib_near(q - 1)
        else:
            gather.far_in()
            gather.sib_far()

    def up_part(t, q, slot):
        chip = place.chip_at(offsets[q])
        h = hbuf.at[slot]
        rows = 2 * seq
        r0 = route[t, pl.ds(2 * chip, 2), 0].reshape(rows, LANES).astype(jnp.float32)
        r1 = route[t, pl.ds(2 * chip, 2), 1].reshape(rows, LANES).astype(jnp.float32)
        logits = dot_f32(h[...].reshape(rows, d_model), wr[...])
        lane = lax.broadcasted_iota(jnp.int32, (rows, LANES), 1)
        logits = jnp.where(lane < experts, logits, -1e30)
        peak = jnp.max(logits, axis=-1, keepdims=True)
        ex = jnp.where(lane < experts, jnp.exp(logits - peak), 0.0)
        probs = ex / jnp.sum(ex, axis=-1, keepdims=True)
        lane_f = lane.astype(jnp.float32)
        for i, r in enumerate((r0, r1)):
            g = jnp.sum(jnp.where(lane_f == r, probs, 0.0), axis=-1, keepdims=True)
            gates[t, chip, i] = jnp.broadcast_to(g, (rows, LANES))

        def expert(e, carry):
            act = dot_f32(h[...].reshape(rows, d_model), vgu[e])
            inner = (jax.nn.gelu(act[:, :cols]) * act[:, cols:]).astype(jnp.bfloat16).astype(jnp.float32)
            e_f = e.astype(jnp.float32)
            us[0] = jnp.where(route[t, pl.ds(2 * chip, 2), 0].reshape(rows, LANES).astype(jnp.float32) == e_f, inner, us[0])
            us[1] = jnp.where(route[t, pl.ds(2 * chip, 2), 1].reshape(rows, LANES).astype(jnp.float32) == e_f, inner, us[1])
            return carry

        us[...] = jnp.zeros_like(us)
        lax.fori_loop(0, experts, expert, 0)
        for i in range(2):
            u_all[t, chip, me, :, pl.ds(i * cols, cols)] = us[i].astype(jnp.bfloat16)
        gather = Gather(wires, ('u', t, q), lambda owner: u_all.at[t, u_owner_chip(owner, q), owner],
                        lambda owner, side: u_all.at[t, u_owner_chip(owner, q), owner, pl.ds(side * seq, seq), :])
        gather.start(u_all.at[t, chip, me])
        u_gathers[t, q] = gather

    def phase_a(t):
        for q in range(4):
            arrive(t, q)
            loads = fetch(t, q, q % 2)
            for desc in loads:
                desc.start()
            for desc in loads:
                desc.wait()
            if t == 0 and q == 0:
                for desc in w_loads:
                    desc.wait()
            up_part(t, q, q % 2)

    def u_near(t):
        for q in range(4):
            u_gathers[t, q].near_in(0)
            u_gathers[t, q].near_in(1)

    m_open = []

    def phase_b(t):
        if t == 0:
            wires.recv('d', their_half)
        for q in range(4):
            gather = u_gathers[t, q]
            gather.far_in()
            gather.sib_own()
            gather.sib_near(0)
            gather.sib_near(1)
            gather.sib_far()
        for q in range(4):
            chip = place.chip_at(offsets[q])
            rows = 2 * seq
            acc = mbuf.at[t, q]
            acc[...] = jnp.zeros_like(acc)

            def expert(e, carry):
                e_b = e.astype(jnp.bfloat16)
                r0 = route[t, pl.ds(2 * chip, 2), 0].reshape(rows, LANES)
                r1 = route[t, pl.ds(2 * chip, 2), 1].reshape(rows, LANES)
                m0, m1 = r0 == e_b, r1 == e_b
                zero = jnp.zeros((rows, LANES), jnp.bfloat16)
                parts = []
                for j in range(n):
                    parts.append(jnp.where(m0, u_all[t, chip, j, :, pl.ds(0, cols)],
                                           jnp.where(m1, u_all[t, chip, j, :, pl.ds(cols, cols)], zero)))
                ue = jnp.concatenate(parts, axis=1)
                out = dot_f32(ue, vd[e])
                e_f = e.astype(jnp.float32)
                gate = jnp.where(r0.astype(jnp.float32) == e_f, gates[t, chip, 0],
                                 jnp.where(r1.astype(jnp.float32) == e_f, gates[t, chip, 1], 0.0))
                acc[...] += jnp.concatenate([gate] * (dcols // LANES), axis=1) * out
                return carry

            lax.fori_loop(0, experts, expert, 0)
            own_cols = pl.ds(pl.multiple_of(me * dcols, LANES), dcols)
            dst = m_out.at[t, :, own_cols]
            for rel in (0, 1):
                target_core = (place.core + rel) % 2
                part = acc.at[pl.ds(pl.multiple_of(target_core * seq, seq), seq), :]
                if q == 0 and rel == 0:
                    desc = pltpu.make_async_copy(part, dst, out_sems.at[t])
                    desc.start()
                    m_open.append(desc)
                elif q < 3:
                    wires.send(('m', t, q, rel), part, dst, wg=place.at(offsets[q], rel))
                else:
                    wires.send(('m1', t, rel), part, relay_m.at[t, rel], wg=place.at(DIRS[rel], 0))

    def m_relay(t):
        for rel, d in enumerate(DIRS):
            wires.recv(('m1', t, rel), relay_m.at[t, rel])
            src = place.at(-d, 0)
            wires.send(('m2', t, rel), relay_m.at[t, rel], m_out.at[t, :, pl.ds(pl.multiple_of(src * dcols, LANES), dcols)],
                       wg=place.at(d, rel))

    def m_in(t):
        for q in range(4):
            for rel in (0, 1):
                src = place.at(-offsets[q], rel)
                dst = m_out.at[t, :, pl.ds(pl.multiple_of(src * dcols, LANES), dcols)]
                if q == 0 and rel == 0:
                    continue
                wires.recv(('m', t, q, rel) if q < 3 else ('m2', t, rel), dst)

    phase_a(0)
    for t in range(1, steps):
        phase_a(t)
        u_near(t - 1)
    phase_b(0)
    u_near(steps - 1)
    for t in range(1, steps):
        phase_b(t)
        m_relay(t - 1)
    m_relay(steps - 1)
    for t in range(steps):
        m_in(t)
    for desc in m_open:
        desc.wait()
    wires.finish()


def moe(n, h2, route, wr, wgu, wd):
    steps, seq, d_model = h2.shape
    experts, _, two_cols = wgu.shape
    ff, dcols = wd.shape[1:]
    bf16, f32 = jnp.bfloat16, jnp.float32
    n_sems = steps * 64
    outs = pl.pallas_call(
        functools.partial(moe_kernel, n, experts),
        name='moe',
        out_shape=(
            jax.ShapeDtypeStruct((steps, seq, d_model), f32),
            jax.ShapeDtypeStruct((steps, n, seq, d_model), bf16),
            jax.ShapeDtypeStruct((steps, 2, seq, dcols), f32),
        ),
        in_specs=[ANY, VMEM_FULL, VMEM_FULL, ANY, ANY],
        out_specs=(ANY,) * 3,
        scratch_shapes=[
            pltpu.VMEM((experts, d_model, two_cols), bf16),
            pltpu.VMEM((experts, ff, dcols), bf16),
            pltpu.VMEM((2, 2, seq, d_model), bf16),
            pltpu.VMEM((steps, n // 2, n, 2 * seq, two_cols), bf16),
            pltpu.VMEM((steps, n // 2, 2, 2 * seq, LANES), f32),
            pltpu.VMEM((2, 2 * seq, two_cols // 2), f32),
            pltpu.VMEM((steps, 4, 2 * seq, dcols), f32),
            pltpu.SemaphoreType.DMA((n_sems,)),
            pltpu.SemaphoreType.DMA((n_sems,)),
            pltpu.SemaphoreType.DMA((2, 2)),
            pltpu.SemaphoreType.DMA((experts + 1,)),
            pltpu.SemaphoreType.DMA((steps,)),
        ],
        compiler_params=pltpu.CompilerParams(collective_id=1, has_side_effects=True, vmem_limit_bytes=66_000_000),
        cost_estimate=pl.CostEstimate(flops=77_000_000_000, bytes_accessed=100_000_000, transcendentals=0),
    )(h2, route, wr, wgu, wd)
    return outs[0]


def solution(mesh):
    n = mesh.shape['wg']
    row_spec = P(('dp', 'wg'))
    dim0_spec = P('wg', None)
    dim1_spec = P(None, 'wg', None)

    def device_fn(hidden, seq_lens, route_idx, g_attn_in, w_query, w_key, w_value, w_attn_out, g_attn_out, g_moe_in, w_router, w_gate, w_up, w_down, g_moe_out):
        n_prompts, seq_len, d_model = hidden.shape
        experts = w_router.shape[1]
        rows = n_prompts * seq_len
        depth = w_query.shape[0]
        routes = jnp.pad(route_idx.T.astype(jnp.bfloat16), ((0, 0), (0, depth - rows)))
        small = jnp.concatenate([w_router.T] + [g[None] for g in (g_attn_in, g_attn_out, g_moe_in, g_moe_out)] + [routes], axis=0)
        small = jnp.pad(small, ((0, -small.shape[0] % 16), (0, 0)))
        pos = jnp.arange(seq_len)
        mask = ((pos[None, None, :] <= pos[None, :, None]) & (pos[None, None, :] < seq_lens[:, None, None])).astype(jnp.float32)
        cos_t, sin_t = rope_tables(seq_len)
        tok_rows = hidden.reshape(rows, d_model)
        x1, h2, k_rope, v_rows, small_all, wgu, wd = attention(
            n, experts, tok_rows, small, mask, cos_t, sin_t, w_query, w_key, w_value, w_attn_out, w_gate, w_up, w_down)
        wr = jnp.pad(small_all[:, :experts].transpose(0, 2, 1).reshape(d_model, experts), ((0, 0), (0, LANES - experts)))
        route = small_all[:, experts + 4:experts + 6, :rows].reshape(n, 2, n_prompts, seq_len).transpose(2, 0, 1, 3)
        route = jnp.broadcast_to(route[..., None], route.shape + (LANES,))
        gain_out = small_all[:, experts + 3].reshape(-1)
        moe_out = moe(n, h2.reshape(hidden.shape), route, wr, wgu, wd).reshape(rows, d_model)
        y_rows = (x1.astype(jnp.float32) + rms_norm(moe_out, gain_out)).astype(jnp.bfloat16)
        cache = (n_prompts, seq_len, w_key.shape[1] // HEAD_DIM, HEAD_DIM)
        return y_rows.reshape(hidden.shape), k_rope.reshape(cache), v_rows.reshape(cache)

    return jax.shard_map(
        device_fn,
        mesh=mesh,
        in_specs=(row_spec, row_spec, row_spec, P('wg'), dim0_spec, dim0_spec, dim0_spec, dim0_spec, P('wg'), P('wg'), dim0_spec, dim1_spec, dim1_spec, dim1_spec, P('wg')),
        out_specs=(row_spec, row_spec, row_spec),
        check_vma=False,
    )
```

```python
import functools
import jax
import jax.numpy as jnp
from jax import lax
from jax.experimental import pallas as pl
from jax.experimental.pallas import tpu as pltpu
from jax.sharding import PartitionSpec as P

HEAD_DIM = 128
LANES = 128
SOFT_CAP = 30.0
NORM_EPS = 1e-5
ROPE_BASE = 10000.0
ATTN_SCALE = HEAD_DIM ** -0.5
MESH = pl.DeviceIdType.MESH
ANY = pl.BlockSpec(memory_space=pl.ANY)
VMEM_FULL = pl.BlockSpec(memory_space=pltpu.VMEM)
DIRS = (1, -1)


def dot_f32(left_op, right_op):
    return jnp.dot(left_op, right_op, preferred_element_type=jnp.float32)


def rms_norm(values, gain_vec):
    values_f32 = values.astype(jnp.float32)
    inv_rms = lax.rsqrt(jnp.mean(values_f32 * values_f32, axis=-1, keepdims=True) + NORM_EPS)
    return values_f32 * inv_rms * gain_vec.astype(jnp.float32)


def rope_tables(seq_len):
    half_dim = HEAD_DIM // 2
    inv_freq = ROPE_BASE ** (-jnp.arange(half_dim, dtype=jnp.float32) * (2.0 / HEAD_DIM))
    angles = jnp.arange(seq_len, dtype=jnp.float32)[:, None] * inv_freq[None, :]
    cos_t, sin_t = jnp.cos(angles), jnp.sin(angles)
    return jnp.concatenate([cos_t, cos_t], axis=1), jnp.concatenate([-sin_t, sin_t], axis=1)


class Place:
    def __init__(self, n):
        self.n = n
        self.chips = n // 2
        self.me = lax.axis_index('wg')
        self.dp = lax.axis_index('dp')
        self.chip = self.me // 2
        self.core = self.me % 2
        self.parity = self.dp % 2
        self.twin = self.dp + 1 - 2 * self.parity

    def at(self, offset, rel):
        return ((self.chip + offset + self.chips) % self.chips) * 2 + (self.core + rel) % 2

    def chip_at(self, offset):
        return (self.chip + offset + self.chips) % self.chips


class Wires:
    def __init__(self, place, send_sems, recv_sems):
        self.place, self.send_sems, self.recv_sems = place, send_sems, recv_sems
        self.slots = {}
        self.open = []

    def copy(self, name, src, dst, wg=None, dp=None):
        slot = self.slots.setdefault(name, len(self.slots))
        return pltpu.make_async_remote_copy(
            src_ref=src, dst_ref=dst, send_sem=self.send_sems.at[slot], recv_sem=self.recv_sems.at[slot],
            device_id={'dp': self.place.dp if dp is None else dp, 'wg': self.place.me if wg is None else wg},
            device_id_type=MESH)

    def send(self, name, src, dst, wg=None, dp=None):
        desc = self.copy(name, src, dst, wg, dp)
        desc.start()
        self.open.append(desc)

    def recv(self, name, dst):
        self.copy(name, dst, dst).wait_recv()

    def finish(self):
        for desc in self.open:
            desc.wait_send()
        self.open = []


def enter(place, with_twin):
    barrier = pltpu.get_barrier_semaphore()
    peers = [(place.dp, place.at(off, rel)) for off in (1, -1, 2) for rel in (0, 1)] + [(place.dp, place.at(0, 1))]
    if with_twin:
        peers.append((place.twin, place.me))
    for dp, wg in peers:
        pl.semaphore_signal(barrier, inc=1, device_id={'dp': dp, 'wg': wg}, device_id_type=MESH)
    pl.semaphore_wait(barrier, len(peers))


class Reshard:
    def __init__(self, wires, gate, up, down, wgu, wd, relay_gu, relay_d, loc_sems):
        self.wires, self.place = wires, wires.place
        n = self.place.n
        self.gate, self.up, self.down, self.wgu, self.wd = gate, up, down, wgu, wd
        self.relay_gu, self.relay_d, self.loc_sems = relay_gu, relay_d, loc_sems
        self.experts, self.rows, self.cols = gate.shape[0], gate.shape[1], gate.shape[2] // n
        self.drows, self.dcols = down.shape[1], down.shape[2] // n
        self.half, self.quarter = self.experts // 2, self.experts // 4
        self.mine = self.place.parity * self.half
        self.theirs = self.half - self.mine

    def piece(self, arr, e0, cnt, j):
        if arr == 'd':
            return self.down.at[pl.ds(e0, cnt), :, pl.ds(pl.multiple_of(j * self.dcols, LANES), self.dcols)]
        ref = self.gate if arr == 'g' else self.up
        return ref.at[pl.ds(e0, cnt), :, pl.ds(pl.multiple_of(j * self.cols, LANES), self.cols)]

    def land(self, arr, e0, cnt, src):
        if arr == 'd':
            return self.wd.at[pl.ds(e0, cnt), pl.ds(pl.multiple_of(src * self.drows, self.drows), self.drows), :]
        row = pl.ds(pl.multiple_of(src * self.rows, self.rows), self.rows)
        if arr == 'gu':
            return self.wgu.at[pl.ds(e0, cnt), row, :]
        return self.wgu.at[pl.ds(e0, cnt), row, pl.ds(0 if arr == 'g' else self.cols, self.cols)]

    def relay(self, arr, side, rel):
        if arr == 'd':
            return self.relay_d.at[side, rel]
        if arr == 'gu':
            return self.relay_gu.at[side, rel]
        return self.relay_gu.at[side, rel, :, :, pl.ds(0 if arr == 'g' else self.cols, self.cols)]

    def span(self, arr):
        return (self.mine, self.half) if arr == 'd' else (0, self.experts)

    def near(self):
        me, sib = self.place.me, self.place.at(0, 1)
        self.local = []
        for i, arr in enumerate('gud'):
            e0, cnt = self.span(arr)
            self.wires.send(('sib', arr), self.piece(arr, e0, cnt, sib), self.land(arr, e0, cnt, me), wg=sib)
            desc = pltpu.make_async_copy(self.piece(arr, e0, cnt, me), self.land(arr, e0, cnt, me), self.loc_sems.at[i])
            desc.start()
            self.local.append(desc)

    def direct(self, rel, arrs):
        for arr in arrs:
            for d in DIRS:
                to = self.place.at(d, rel)
                self.wires.send(('direct', d, rel, arr), self.piece(arr, self.mine, self.half, to),
                                self.land(arr, self.mine, self.half, self.place.me), wg=to)

    def first_leg(self, rel, arrs):
        for arr in arrs:
            for side, d in enumerate(DIRS):
                e0 = self.mine + side * self.quarter
                self.wires.send(('leg1', d, rel, arr), self.piece(arr, e0, self.quarter, self.place.at(2 * d, rel)),
                                self.relay(arr, side, rel), wg=self.place.at(d, 0))

    def to_twin(self, name, arr, e0, cnt, src):
        if arr != 'd':
            region = self.land(arr, e0, cnt, src)
            self.wires.send(name, region, region, dp=self.place.twin)

    def direct_in(self, rel, arrs):
        for arr in arrs:
            for d in DIRS:
                src = self.place.at(-d, rel)
                for part in arr:
                    self.wires.recv(('direct', d, rel, part), self.land(part, self.mine, self.half, src))
                self.to_twin(('twin', d, rel, arr), arr, self.mine, self.half, src)

    def second_leg(self, rel, arrs):
        for arr in arrs:
            for side, d in enumerate(DIRS):
                for part in arr:
                    self.wires.recv(('leg1', d, rel, part), self.relay(part, side, rel))
                self.wires.send(('leg2', d, rel, arr), self.relay(arr, side, rel),
                                self.land(arr, self.mine + side * self.quarter, self.quarter, self.place.at(-d, 0)),
                                wg=self.place.at(d, rel))

    def far_in(self, arrs):
        for arr in arrs:
            for rel in (0, 1):
                for side, d in enumerate(DIRS):
                    src = self.place.at(2 * d, rel)
                    e0 = self.mine + side * self.quarter
                    self.wires.recv(('leg2', d, rel, arr), self.land(arr, e0, self.quarter, src))
                    self.to_twin(('twin2', d, rel, arr), arr, e0, self.quarter, src)

    def finish(self):
        for arr in 'gud':
            e0, cnt = self.span(arr)
            self.wires.recv(('sib', arr), self.land(arr, e0, cnt, self.place.at(0, 1)))
        for rel in (0, 1):
            for side, d in enumerate(DIRS):
                self.wires.recv(('twin', d, rel, 'gu'), self.land('gu', self.theirs, self.half, self.place.at(-d, rel)))
                self.wires.recv(('twin2', d, rel, 'gu'),
                                self.land('gu', self.theirs + side * self.quarter, self.quarter, self.place.at(2 * d, rel)))
        for desc in self.local:
            desc.wait()


class PairGather:
    def __init__(self, wires, name, src, dst, give_side):
        self.wires, self.place, self.name, self.src, self.dst = wires, wires.place, name, src, dst
        rows = src.shape[0]
        given = rows * 9 // 32
        parity = self.place.parity
        last = rows - given
        self.spans = {'give': (parity * last, given), 'both': (given, rows - 2 * given), 'take': (last - parity * last, given)}
        self.far_side = {'give': give_side, 'both': 1 - give_side}

    def part(self, owner, what):
        row, cnt = self.spans[what]
        return self.dst.at[owner, pl.ds(pl.multiple_of(row, 16), cnt), :]

    def start(self):
        place, me = self.place, self.place.me
        for what in ('give', 'both'):
            row, cnt = self.spans[what]
            own = self.src.at[pl.ds(pl.multiple_of(row, 16), cnt), :]
            for d in DIRS:
                self.wires.send((self.name, 'own', what, d), own, self.part(me, what), wg=place.at(d, 0))
        self.wires.send((self.name, 'sib'), self.src, self.dst.at[me], wg=place.at(0, 1))

    def give(self, tag, owner):
        part = self.part(owner, 'give')
        self.wires.send((self.name, 'give', tag), part, part, dp=self.place.twin)

    def near_in(self, *whats):
        place = self.place
        for what in whats:
            for side, d in enumerate(DIRS):
                owner = place.at(-d, 0)
                part = self.part(owner, what)
                self.wires.recv((self.name, 'own', what, d), part)
                if what == 'give':
                    self.give(d, owner)
                if self.far_side[what] == side:
                    self.wires.send((self.name, 'far', what), part, part, wg=place.at(d, 0))
                self.wires.send((self.name, 'across', what, d), part, part, wg=place.at(0, 1))

    def far_in(self, *whats):
        place = self.place
        owner = place.at(2, 0)
        for what in whats:
            part = self.part(owner, what)
            self.wires.recv((self.name, 'far', what), part)
            if what == 'give':
                self.give(2, owner)
            self.wires.send((self.name, 'across', what, 2), part, part, wg=place.at(0, 1))

    def twin_in(self, *tags):
        for tag in tags:
            part = self.part(self.place.at(-tag, 0), 'take')
            self.wires.recv((self.name, 'give', tag), part)
            self.wires.send((self.name, 'across', 'take', tag), part, part, wg=self.place.at(0, 1))

    def sib_in(self):
        place = self.place
        self.wires.recv((self.name, 'sib'), self.dst.at[place.at(0, 1)])
        for tag in (1, -1, 2):
            for what in ('give', 'both', 'take'):
                self.wires.recv((self.name, 'across', what, tag), self.part(place.at(-tag, 1), what))


def attention_kernel(n, experts, hidden, small, mask, cos_t, sin_t, wq, wk, wv, wo, gate, up, down,
                     x1, h2, k_out, v_out, small_all, gq, gk, gv, go, wgu, wd, relay_gu, relay_d,
                     h, acc, ctx, wbuf, send_sems, recv_sems, loc_sems, load_sems):
    place = Place(n)
    wires = Wires(place, send_sems, recv_sems)
    me = place.me
    prompts, seq = mask.shape[0], mask.shape[1]
    rows, d_model = hidden.shape
    depth = wq.shape[0]
    q_dim, kv_dim = wq.shape[1], wk.shape[1]
    n_kv = kv_dim // HEAD_DIM
    group = q_dim // kv_dim
    tile = 512
    row_tile = seq

    enter(place, True)
    others = [(off, rel) for off in (0, 1, -1, 2) for rel in (0, 1)][1:]
    for off, rel in others:
        wires.send(('small', off, rel), small, small_all.at[me], wg=place.at(off, rel))
    gather_q = PairGather(wires, 'q', wq, gq, 0)
    gather_k = PairGather(wires, 'k', wk, gk, 1)
    gather_v = PairGather(wires, 'v', wv, gv, 1)
    gather_o = PairGather(wires, 'o', wo, go, 0)
    moving = Reshard(wires, gate, up, down, wgu, wd, relay_gu, relay_d, loc_sems)
    gather_q.start()
    gather_k.start()
    gather_v.start()
    small_all[me] = small[...]
    for off, rel in others:
        wires.recv(('small', off, rel), small_all.at[place.at(-off, rel)])

    def gain(i):
        return jnp.concatenate([small_all[j, pl.ds(experts + i, 1), :] for j in range(n)], axis=1).astype(jnp.float32)

    def norm(values):
        return values * lax.rsqrt(jnp.mean(values * values, axis=-1, keepdims=True) + NORM_EPS)

    def norm_in(i, carry):
        r = pl.ds(pl.multiple_of(i * 16, 16), 16)
        h[r, :] = (norm(hidden[r, :].astype(jnp.float32)) * gain(0)).astype(jnp.bfloat16)
        return carry

    with jax.named_scope('norm_in'):
        lax.fori_loop(0, rows // 16, norm_in, 0)
        acc[...] = jnp.zeros_like(acc)

    with jax.named_scope('near'):
        gather_q.near_in('give', 'both')
        gather_k.near_in('give', 'both')
        gather_v.near_in('give', 'both')
        gather_o.start()
        moving.direct(0, 'gu')
        moving.first_leg(0, 'gu')
        moving.first_leg(1, 'gu')
        moving.near()
    with jax.named_scope('qkv_far'):
        gather_q.twin_in(1, -1)
        gather_k.twin_in(1, -1)
        gather_v.twin_in(1, -1)
        gather_q.far_in('give', 'both')
        gather_k.far_in('give', 'both')
        gather_v.far_in('give', 'both')
    with jax.named_scope('qkv_last'):
        gather_q.twin_in(2)
        gather_k.twin_in(2)
        gather_v.twin_in(2)
        gather_q.sib_in()
        gather_k.sib_in()
        gather_v.sib_in()
    with jax.named_scope('o_near_give'):
        gather_o.near_in('give')

    def owner_of(i):
        return (me + i) % n

    def product(lhs, weights, first_col):
        def loads(i, slot):
            owner = owner_of(i)

            def start(own):
                col = 0
                for w, (src, gathered) in enumerate(weights):
                    width = src.shape[1]
                    pltpu.make_async_copy(src if own else gathered.at[owner], wbuf.at[slot, :, pl.ds(col, width)],
                                          load_sems.at[slot, w]).start()
                    col += width

            @pl.when(i == 0)
            def _():
                start(True)

            @pl.when(i > 0)
            def _():
                start(False)

        def step(i, carry):
            slot = i % 2
            owner = owner_of(i)

            @pl.when(i + 1 < n)
            def _():
                loads(i + 1, 1 - slot)

            col = 0
            for w, (src, gathered) in enumerate(weights):
                width = src.shape[1]
                pltpu.make_async_copy(gathered.at[owner], wbuf.at[slot, :, pl.ds(col, width)], load_sems.at[slot, w]).wait()
                col += width

            def tiles(j, carry):
                c = pl.ds(pl.multiple_of(j * tile, tile), tile)
                acc[:, c] += dot_f32(lhs[:, pl.ds(pl.multiple_of(owner * depth, depth), depth)], wbuf[slot, :, c])
                return carry

            return lax.fori_loop(0, col // tile, tiles, carry)

        loads(0, 0)
        lax.fori_loop(0, n, step, 0)

    with jax.named_scope('qkv_mm'):
        product(h, ((wq, gq), (wk, gk), (wv, gv)), 0)

    def rope(values):
        values = values.astype(jnp.bfloat16).astype(jnp.float32)
        cos_v, sin_v = cos_t[...], sin_t[...]
        times = values.shape[0] // seq
        if times > 1:
            cos_v, sin_v = jnp.concatenate([cos_v] * times, axis=0), jnp.concatenate([sin_v] * times, axis=0)
        return (values * cos_v + pltpu.roll(values, HEAD_DIM // 2, 1) * sin_v).astype(jnp.bfloat16)

    def attend(i, carry):
        p, g = i // n_kv, i % n_kv
        r = pl.ds(pl.multiple_of(p * seq, seq), seq)
        kv_cols = pl.ds(pl.multiple_of(g * HEAD_DIM, HEAD_DIM), HEAD_DIM)
        q = jnp.concatenate([acc[r, pl.ds(pl.multiple_of((g * group + j) * HEAD_DIM, HEAD_DIM), HEAD_DIM)]
                             for j in range(group)], axis=0)
        q = rope(q)
        k = rope(acc[r, pl.ds(pl.multiple_of(q_dim + g * HEAD_DIM, HEAD_DIM), HEAD_DIM)])
        v = acc[r, pl.ds(pl.multiple_of(q_dim + kv_dim + g * HEAD_DIM, HEAD_DIM), HEAD_DIM)].astype(jnp.bfloat16)
        k_out[r, kv_cols] = k
        v_out[r, kv_cols] = v
        scores = lax.dot_general(q, k, (((1,), (1,)), ((), ())), preferred_element_type=jnp.float32) * ATTN_SCALE
        scores = SOFT_CAP * jnp.tanh(scores / SOFT_CAP)
        allowed = jnp.concatenate([mask[p]] * group, axis=0) > 0.5
        scores = jnp.where(allowed, scores, -1e30)
        ex = jnp.exp(scores - jnp.max(scores, axis=-1, keepdims=True))
        probs = (ex / jnp.sum(ex, axis=-1, keepdims=True)).astype(jnp.bfloat16)
        out = dot_f32(probs, v).astype(jnp.bfloat16)
        for j in range(group):
            ctx[r, pl.ds(pl.multiple_of((g * group + j) * HEAD_DIM, HEAD_DIM), HEAD_DIM)] = out[j * seq:(j + 1) * seq]
        return carry

    with jax.named_scope('attend'):
        lax.fori_loop(0, prompts * n_kv, attend, 0)

    with jax.named_scope('o_near_both'):
        gather_o.near_in('both')
    with jax.named_scope('direct_in0'):
        moving.direct_in(0, ('gu',))
    with jax.named_scope('leg2'):
        moving.second_leg(0, ('gu',))
        moving.second_leg(1, ('gu',))
        moving.direct(1, 'gu')
        moving.direct(0, 'd')
        moving.first_leg(0, 'd')
        moving.first_leg(1, 'd')
        moving.direct(1, 'd')
    with jax.named_scope('o_far'):
        gather_o.twin_in(1, -1)
        gather_o.far_in('give', 'both')
    with jax.named_scope('mv_far'):
        moving.far_in(('gu',))
    with jax.named_scope('o_last'):
        gather_o.twin_in(2)
        gather_o.sib_in()
    with jax.named_scope('o_mm'):
        acc[...] = jnp.zeros_like(acc)
        product(ctx, ((wo, go),), 0)

    def finish_rows(i, carry):
        r = pl.ds(pl.multiple_of(i * 16, 16), 16)
        mid = (hidden[r, :].astype(jnp.float32) + norm(acc[r, pl.ds(0, d_model)]) * gain(1)).astype(jnp.bfloat16)
        x1[r, :] = mid
        h2[r, :] = (norm(mid.astype(jnp.float32)) * gain(2)).astype(jnp.bfloat16)
        return carry

    with jax.named_scope('finish_rows'):
        lax.fori_loop(0, rows // 16, finish_rows, 0)
    with jax.named_scope('direct_in1'):
        moving.direct_in(1, ('gu',))
    with jax.named_scope('mv_d'):
        moving.second_leg(0, ('d',))
        moving.second_leg(1, ('d',))
        moving.direct_in(0, ('d',))
        moving.direct_in(1, ('d',))
        moving.far_in(('d',))
    with jax.named_scope('mv_fin'):
        moving.finish()
    wires.finish()


def attention(n, experts, hidden, small, mask, cos_t, sin_t, wq, wk, wv, wo, gate, up, down):
    rows, d_model = hidden.shape
    ff = gate.shape[2]
    drows = down.shape[1]
    cols, dcols = ff // n, d_model // n
    bf16, f32 = jnp.bfloat16, jnp.float32
    quarter = experts // 4

    def full(w):
        return jax.ShapeDtypeStruct((n,) + w.shape, bf16)

    outs = pl.pallas_call(
        functools.partial(attention_kernel, n, experts),
        name='attention',
        out_shape=(
            jax.ShapeDtypeStruct((rows, d_model), bf16),
            jax.ShapeDtypeStruct((rows, d_model), bf16),
            jax.ShapeDtypeStruct((rows, wk.shape[1]), bf16),
            jax.ShapeDtypeStruct((rows, wv.shape[1]), bf16),
            full(small), full(wq), full(wk), full(wv), full(wo),
            jax.ShapeDtypeStruct((experts, d_model, 2 * cols), bf16),
            jax.ShapeDtypeStruct((experts, drows * n, dcols), bf16),
            jax.ShapeDtypeStruct((2, 2, quarter, gate.shape[1], 2 * cols), bf16),
            jax.ShapeDtypeStruct((2, 2, quarter, drows, dcols), bf16),
        ),
        in_specs=[VMEM_FULL] * 5 + [ANY] * 7,
        out_specs=(VMEM_FULL,) * 5 + (ANY,) * 8,
        scratch_shapes=[
            pltpu.VMEM((rows, d_model), bf16),
            pltpu.VMEM((rows, wq.shape[1] + 2 * wk.shape[1]), f32),
            pltpu.VMEM((rows, wq.shape[1]), bf16),
            pltpu.VMEM((2, wq.shape[0], wq.shape[1] + 2 * wk.shape[1]), bf16),
            pltpu.SemaphoreType.DMA((160,)),
            pltpu.SemaphoreType.DMA((160,)),
            pltpu.SemaphoreType.DMA((4,)),
            pltpu.SemaphoreType.DMA((2, 3)),
        ],
        compiler_params=pltpu.CompilerParams(collective_id=0, has_side_effects=True, vmem_limit_bytes=62_000_000),
        cost_estimate=pl.CostEstimate(flops=33_000_000_000, bytes_accessed=300_000_000, transcendentals=0),
    )(hidden, small, mask, cos_t, sin_t, wq, wk, wv, wo, gate, up, down)
    return outs[0], outs[1], outs[2], outs[3], outs[4], outs[9], outs[10]


class Gather:
    def __init__(self, wires, name, region, half_region):
        self.wires, self.place, self.name = wires, wires.place, name
        self.region, self.half_region = region, half_region

    def start(self, src):
        place, dst = self.place, self.region(self.place.me)
        for d in DIRS:
            self.wires.send((self.name, 'own', d), src, dst, wg=place.at(d, 0))
        self.wires.send((self.name, 'own', 0), src, dst, wg=place.at(0, 1))

    def near_in(self, side):
        d, place = DIRS[side], self.place
        owner = place.at(-d, 0)
        block, part = self.region(owner), self.half_region(owner, side)
        self.wires.recv((self.name, 'own', d), block)
        self.wires.send((self.name, 'far', d), part, part, wg=place.at(d, 0))
        self.wires.send((self.name, 'across', d), block, block, wg=place.at(0, 1))

    def far_in(self):
        place = self.place
        owner = place.at(2, 0)
        for side, d in enumerate(DIRS):
            part = self.half_region(owner, side)
            self.wires.recv((self.name, 'far', d), part)
            self.wires.send((self.name, 'across2', d), part, part, wg=place.at(0, 1))

    def sib_own(self):
        self.wires.recv((self.name, 'own', 0), self.region(self.place.at(0, 1)))

    def sib_near(self, side):
        self.wires.recv((self.name, 'across', DIRS[side]), self.region(self.place.at(-DIRS[side], 1)))

    def sib_far(self):
        for side, d in enumerate(DIRS):
            self.wires.recv((self.name, 'across2', d), self.half_region(self.place.at(2, 1), side))


def moe_kernel(n, experts, h2, route, wr, wgu, wd, m_out, hg, relay_m,
               vgu, vd, hbuf, u_all, gates, us, mbuf, send_sems, recv_sems, load_sems, w_sems, out_sems):
    place = Place(n)
    wires = Wires(place, send_sems, recv_sems)
    steps, seq, d_model = h2.shape
    chips, me = place.chips, place.me
    cols = vgu.shape[2] // 2
    dcols = vd.shape[2]
    offsets = (0, -1, 1, 2)

    enter(place, True)
    h_gathers = []
    for t in range(steps):
        gather = Gather(wires, ('h', t), lambda owner, t=t: hg.at[t, owner],
                        lambda owner, side, t=t: hg.at[t, owner, pl.ds(side * (seq // 2), seq // 2), :])
        h_gathers.append(gather)
    h_gathers[0].start(h2.at[0])
    w_loads = []
    for e in range(experts):
        desc = pltpu.make_async_copy(wgu.at[e], vgu.at[e], w_sems.at[e])
        desc.start()
        w_loads.append(desc)
    half = experts // 2
    mine, theirs = place.parity * half, half - place.parity * half
    own_half, their_half = vd.at[pl.ds(mine, half)], vd.at[pl.ds(theirs, half)]
    d_load = pltpu.make_async_copy(wd.at[pl.ds(mine, half)], own_half, w_sems.at[experts])
    d_load.start()
    d_load.wait()
    wires.send('d', own_half, own_half, dp=place.twin)

    def u_owner_chip(owner, q):
        return (owner // 2 + offsets[q] + chips) % chips

    u_gathers = {}

    def fetch(t, q, slot):
        if q == 0:
            first = pltpu.make_async_copy(h2.at[t], hbuf.at[slot, place.core], load_sems.at[slot, 0])
            sib = 1 - place.core
            second = pltpu.make_async_copy(hg.at[t, place.at(0, 1)], hbuf.at[slot, sib], load_sems.at[slot, 1])
            return [first, second]
        chip = place.chip_at(offsets[q])
        return [pltpu.make_async_copy(hg.at[t, pl.ds(2 * chip, 2)], hbuf.at[slot], load_sems.at[slot, 0])]

    def up_part(t, q, slot):
        chip = place.chip_at(offsets[q])
        h = hbuf.at[slot]
        rows = 2 * seq
        r0 = route[t, pl.ds(2 * chip, 2), 0].reshape(rows, LANES).astype(jnp.float32)
        r1 = route[t, pl.ds(2 * chip, 2), 1].reshape(rows, LANES).astype(jnp.float32)
        logits = dot_f32(h[...].reshape(rows, d_model), wr[...])
        lane = lax.broadcasted_iota(jnp.int32, (rows, LANES), 1)
        logits = jnp.where(lane < experts, logits, -1e30)
        peak = jnp.max(logits, axis=-1, keepdims=True)
        ex = jnp.where(lane < experts, jnp.exp(logits - peak), 0.0)
        probs = ex / jnp.sum(ex, axis=-1, keepdims=True)
        lane_f = lane.astype(jnp.float32)
        for i, r in enumerate((r0, r1)):
            g = jnp.sum(jnp.where(lane_f == r, probs, 0.0), axis=-1, keepdims=True)
            gates[t, chip, i] = jnp.broadcast_to(g, (rows, LANES))

        def expert(e, carry):
            act = dot_f32(h[...].reshape(rows, d_model), vgu[e])
            inner = (jax.nn.gelu(act[:, :cols]) * act[:, cols:]).astype(jnp.bfloat16).astype(jnp.float32)
            e_f = e.astype(jnp.float32)
            us[0] = jnp.where(route[t, pl.ds(2 * chip, 2), 0].reshape(rows, LANES).astype(jnp.float32) == e_f, inner, us[0])
            us[1] = jnp.where(route[t, pl.ds(2 * chip, 2), 1].reshape(rows, LANES).astype(jnp.float32) == e_f, inner, us[1])
            return carry

        us[...] = jnp.zeros_like(us)
        lax.fori_loop(0, experts, expert, 0)
        for i in range(2):
            u_all[t, chip, me, :, pl.ds(i * cols, cols)] = us[i].astype(jnp.bfloat16)
        gather = Gather(wires, ('u', t, q), lambda owner: u_all.at[t, u_owner_chip(owner, q), owner],
                        lambda owner, side: u_all.at[t, u_owner_chip(owner, q), owner, pl.ds(side * seq, seq), :])
        gather.start(u_all.at[t, chip, me])
        u_gathers[t, q] = gather

    def begin(t, q):
        loads = fetch(t, q, (4 * t + q) % 3)
        for desc in loads:
            desc.start()
        return loads

    def phase_a(t, between):
        gather = h_gathers[t]
        with jax.named_scope('arrive'):
            gather.sib_own()
            own = begin(t, 0)
            if t == 0:
                for desc in w_loads:
                    desc.wait()
        use(t, 0, own)
        with jax.named_scope('arrive'):
            gather.near_in(0)
            gather.near_in(1)
            if t + 1 < steps:
                h_gathers[t + 1].start(h2.at[t + 1])
            gather.sib_near(0)
            left = begin(t, 1)
            gather.sib_near(1)
            right = begin(t, 2)
        use(t, 1, left)
        between()
        use(t, 2, right)
        with jax.named_scope('arrive'):
            gather.far_in()
            gather.sib_far()
            far = begin(t, 3)
        use(t, 3, far)

    def use(t, q, loads):
        with jax.named_scope('load'):
            for desc in loads:
                desc.wait()
        with jax.named_scope('up'):
            up_part(t, q, (4 * t + q) % 3)

    def u_near(t):
        for q in range(4):
            with jax.named_scope('u_near'):
                u_gathers[t, q].near_in(0)
                u_gathers[t, q].near_in(1)

    m_open = []

    def phase_b(t):
        if t == 0:
            wires.recv('d', their_half)
        for q in range(4):
            gather = u_gathers[t, q]
            with jax.named_scope('u_wait'):
                gather.far_in()
                gather.sib_own()
                gather.sib_near(0)
                gather.sib_near(1)
                gather.sib_far()
        for q in range(4):
            chip = place.chip_at(offsets[q])
            rows = 2 * seq
            acc = mbuf.at[t, q]
            acc[...] = jnp.zeros_like(acc)

            def expert(e, carry):
                e_b = e.astype(jnp.bfloat16)
                r0 = route[t, pl.ds(2 * chip, 2), 0].reshape(rows, LANES)
                r1 = route[t, pl.ds(2 * chip, 2), 1].reshape(rows, LANES)
                m0, m1 = r0 == e_b, r1 == e_b
                zero = jnp.zeros((rows, LANES), jnp.bfloat16)
                parts = []
                for j in range(n):
                    parts.append(jnp.where(m0, u_all[t, chip, j, :, pl.ds(0, cols)],
                                           jnp.where(m1, u_all[t, chip, j, :, pl.ds(cols, cols)], zero)))
                ue = jnp.concatenate(parts, axis=1)
                out = dot_f32(ue, vd[e])
                e_f = e.astype(jnp.float32)
                gate = jnp.where(r0.astype(jnp.float32) == e_f, gates[t, chip, 0],
                                 jnp.where(r1.astype(jnp.float32) == e_f, gates[t, chip, 1], 0.0))
                acc[...] += jnp.concatenate([gate] * (dcols // LANES), axis=1) * out
                return carry

            with jax.named_scope('down'):
                lax.fori_loop(0, experts, expert, 0)
            own_cols = pl.ds(pl.multiple_of(me * dcols, LANES), dcols)
            dst = m_out.at[t, :, own_cols]
            for rel in (0, 1):
                target_core = (place.core + rel) % 2
                part = acc.at[pl.ds(pl.multiple_of(target_core * seq, seq), seq), :]
                if q == 0 and rel == 0:
                    desc = pltpu.make_async_copy(part, dst, out_sems.at[t])
                    desc.start()
                    m_open.append(desc)
                elif q < 3:
                    wires.send(('m', t, q, rel), part, dst, wg=place.at(offsets[q], rel))
                else:
                    wires.send(('m1', t, rel), part, relay_m.at[t, rel], wg=place.at(DIRS[rel], 0))

    def m_relay(t):
        for rel, d in enumerate(DIRS):
            wires.recv(('m1', t, rel), relay_m.at[t, rel])
            src = place.at(-d, 0)
            wires.send(('m2', t, rel), relay_m.at[t, rel], m_out.at[t, :, pl.ds(pl.multiple_of(src * dcols, LANES), dcols)],
                       wg=place.at(d, rel))

    def m_in(t):
        for q in range(4):
            for rel in (0, 1):
                src = place.at(-offsets[q], rel)
                dst = m_out.at[t, :, pl.ds(pl.multiple_of(src * dcols, LANES), dcols)]
                if q == 0 and rel == 0:
                    continue
                wires.recv(('m', t, q, rel) if q < 3 else ('m2', t, rel), dst)

    phase_a(0, lambda: None)
    for t in range(1, steps):
        phase_a(t, lambda: u_near(t - 1))
        if t == steps - 1:
            u_near(t)
        phase_b(t - 1)
        if t > 1:
            m_relay(t - 2)
    phase_b(steps - 1)
    m_relay(steps - 2)
    m_relay(steps - 1)
    for t in range(steps):
        with jax.named_scope('m_in'):
            m_in(t)
    for desc in m_open:
        desc.wait()
    wires.finish()


def moe(n, h2, route, wr, wgu, wd):
    steps, seq, d_model = h2.shape
    experts, _, two_cols = wgu.shape
    ff, dcols = wd.shape[1:]
    bf16, f32 = jnp.bfloat16, jnp.float32
    n_sems = steps * 64
    outs = pl.pallas_call(
        functools.partial(moe_kernel, n, experts),
        name='moe',
        out_shape=(
            jax.ShapeDtypeStruct((steps, seq, d_model), f32),
            jax.ShapeDtypeStruct((steps, n, seq, d_model), bf16),
            jax.ShapeDtypeStruct((steps, 2, seq, dcols), f32),
        ),
        in_specs=[ANY, VMEM_FULL, VMEM_FULL, ANY, ANY],
        out_specs=(ANY,) * 3,
        scratch_shapes=[
            pltpu.VMEM((experts, d_model, two_cols), bf16),
            pltpu.VMEM((experts, ff, dcols), bf16),
            pltpu.VMEM((3, 2, seq, d_model), bf16),
            pltpu.VMEM((steps, n // 2, n, 2 * seq, two_cols), bf16),
            pltpu.VMEM((steps, n // 2, 2, 2 * seq, LANES), f32),
            pltpu.VMEM((2, 2 * seq, two_cols // 2), f32),
            pltpu.VMEM((steps, 4, 2 * seq, dcols), f32),
            pltpu.SemaphoreType.DMA((n_sems,)),
            pltpu.SemaphoreType.DMA((n_sems,)),
            pltpu.SemaphoreType.DMA((3, 2)),
            pltpu.SemaphoreType.DMA((experts + 1,)),
            pltpu.SemaphoreType.DMA((steps,)),
        ],
        compiler_params=pltpu.CompilerParams(collective_id=1, has_side_effects=True, vmem_limit_bytes=66_000_000),
        cost_estimate=pl.CostEstimate(flops=77_000_000_000, bytes_accessed=100_000_000, transcendentals=0),
    )(h2, route, wr, wgu, wd)
    return outs[0]


def solution(mesh):
    n = mesh.shape['wg']
    row_spec = P(('dp', 'wg'))
    dim0_spec = P('wg', None)
    dim1_spec = P(None, 'wg', None)

    def device_fn(hidden, seq_lens, route_idx, g_attn_in, w_query, w_key, w_value, w_attn_out, g_attn_out, g_moe_in, w_router, w_gate, w_up, w_down, g_moe_out):
        n_prompts, seq_len, d_model = hidden.shape
        experts = w_router.shape[1]
        rows = n_prompts * seq_len
        depth = w_query.shape[0]
        routes = jnp.pad(route_idx.T.astype(jnp.bfloat16), ((0, 0), (0, depth - rows)))
        small = jnp.concatenate([w_router.T] + [g[None] for g in (g_attn_in, g_attn_out, g_moe_in, g_moe_out)] + [routes], axis=0)
        small = jnp.pad(small, ((0, -small.shape[0] % 16), (0, 0)))
        pos = jnp.arange(seq_len)
        mask = ((pos[None, None, :] <= pos[None, :, None]) & (pos[None, None, :] < seq_lens[:, None, None])).astype(jnp.float32)
        cos_t, sin_t = rope_tables(seq_len)
        tok_rows = hidden.reshape(rows, d_model)
        x1, h2, k_rope, v_rows, small_all, wgu, wd = attention(
            n, experts, tok_rows, small, mask, cos_t, sin_t, w_query, w_key, w_value, w_attn_out, w_gate, w_up, w_down)
        wr = jnp.pad(small_all[:, :experts].transpose(0, 2, 1).reshape(d_model, experts), ((0, 0), (0, LANES - experts)))
        route = small_all[:, experts + 4:experts + 6, :rows].reshape(n, 2, n_prompts, seq_len).transpose(2, 0, 1, 3)
        route = jnp.broadcast_to(route[..., None], route.shape + (LANES,))
        gain_out = small_all[:, experts + 3].reshape(-1)
        moe_out = moe(n, h2.reshape(hidden.shape), route, wr, wgu, wd).reshape(rows, d_model)
        y_rows = (x1.astype(jnp.float32) + rms_norm(moe_out, gain_out)).astype(jnp.bfloat16)
        cache = (n_prompts, seq_len, w_key.shape[1] // HEAD_DIM, HEAD_DIM)
        return y_rows.reshape(hidden.shape), k_rope.reshape(cache), v_rows.reshape(cache)

    return jax.shard_map(
        device_fn,
        mesh=mesh,
        in_specs=(row_spec, row_spec, row_spec, P('wg'), dim0_spec, dim0_spec, dim0_spec, dim0_spec, P('wg'), P('wg'), dim0_spec, dim1_spec, dim1_spec, dim1_spec, P('wg')),
        out_specs=(row_spec, row_spec, row_spec),
        check_vma=False,
    )
```

```python
import functools
import jax
import jax.numpy as jnp
from jax import lax
from jax.experimental import pallas as pl
from jax.experimental.pallas import tpu as pltpu
from jax.sharding import PartitionSpec as P

HEAD_DIM = 128
LANES = 128
SOFT_CAP = 30.0
NORM_EPS = 1e-5
ROPE_BASE = 10000.0
ATTN_SCALE = HEAD_DIM ** -0.5
MESH = pl.DeviceIdType.MESH
ANY = pl.BlockSpec(memory_space=pl.ANY)
VMEM_FULL = pl.BlockSpec(memory_space=pltpu.VMEM)
DIRS = (1, -1)


def dot_f32(left_op, right_op):
    return jnp.dot(left_op, right_op, preferred_element_type=jnp.float32)


def rms_norm(values, gain_vec):
    values_f32 = values.astype(jnp.float32)
    inv_rms = lax.rsqrt(jnp.mean(values_f32 * values_f32, axis=-1, keepdims=True) + NORM_EPS)
    return values_f32 * inv_rms * gain_vec.astype(jnp.float32)


def rope_tables(seq_len):
    half_dim = HEAD_DIM // 2
    inv_freq = ROPE_BASE ** (-jnp.arange(half_dim, dtype=jnp.float32) * (2.0 / HEAD_DIM))
    angles = jnp.arange(seq_len, dtype=jnp.float32)[:, None] * inv_freq[None, :]
    cos_t, sin_t = jnp.cos(angles), jnp.sin(angles)
    return jnp.concatenate([cos_t, cos_t], axis=1), jnp.concatenate([-sin_t, sin_t], axis=1)


class Place:
    def __init__(self, n):
        self.n = n
        self.chips = n // 2
        self.me = lax.axis_index('wg')
        self.dp = lax.axis_index('dp')
        self.chip = self.me // 2
        self.core = self.me % 2
        self.parity = self.dp % 2
        self.twin = self.dp + 1 - 2 * self.parity

    def at(self, offset, rel):
        return ((self.chip + offset + self.chips) % self.chips) * 2 + (self.core + rel) % 2

    def chip_at(self, offset):
        return (self.chip + offset + self.chips) % self.chips


def still(ref):
    if not hasattr(ref, 'transforms'):
        return ref
    out = ref.ref
    for step in ref.transforms:
        out = out.at[tuple(pl.ds(0, index.size) if hasattr(index, 'start') else pl.ds(0, 1) for index in step.indices)]
    return out


class Wires:
    def __init__(self, place, send_sems, recv_sems):
        self.place, self.send_sems, self.recv_sems = place, send_sems, recv_sems
        self.slots = {}
        self.open = []

    def copy(self, name, src, dst, wg=None, dp=None):
        slot = self.slots.setdefault(name, len(self.slots))
        return pltpu.make_async_remote_copy(
            src_ref=src, dst_ref=dst, send_sem=self.send_sems.at[slot], recv_sem=self.recv_sems.at[slot],
            device_id={'dp': self.place.dp if dp is None else dp, 'wg': self.place.me if wg is None else wg},
            device_id_type=MESH)

    def send(self, name, src, dst, wg=None, dp=None):
        desc = self.copy(name, src, dst, wg, dp)
        desc.start()
        self.open.append((name, still(src)))

    def recv(self, name, dst):
        self.copy(name, dst, dst).wait_recv()

    def finish(self):
        for name, src in self.open:
            self.copy(name, src, src).wait_send()
        self.open = []


def enter(place):
    barrier = pltpu.get_barrier_semaphore()
    peers = [(place.dp, place.at(off, rel)) for off in (1, -1, 2) for rel in (0, 1)] + [(place.dp, place.at(0, 1))]
    peers.append((place.twin, place.me))
    for dp, wg in peers:
        pl.semaphore_signal(barrier, inc=1, device_id={'dp': dp, 'wg': wg}, device_id_type=MESH)
    pl.semaphore_wait(barrier, len(peers))


class Reshard:
    def __init__(self, wires, gate, up, down, wgu, wd, relay_gu, relay_d, loc_sems):
        self.wires, self.place = wires, wires.place
        n = self.place.n
        self.gate, self.up, self.down, self.wgu, self.wd = gate, up, down, wgu, wd
        self.relay_gu, self.relay_d, self.loc_sems = relay_gu, relay_d, loc_sems
        self.experts, self.rows, self.cols = gate.shape[0], gate.shape[1], gate.shape[2] // n
        self.drows, self.dcols = down.shape[1], down.shape[2] // n
        self.half, self.quarter = self.experts // 2, self.experts // 4
        self.mine = self.place.parity * self.half
        self.theirs = self.half - self.mine

    def piece(self, arr, e0, cnt, j):
        if arr == 'd':
            return self.down.at[pl.ds(e0, cnt), :, pl.ds(pl.multiple_of(j * self.dcols, LANES), self.dcols)]
        ref = self.gate if arr == 'g' else self.up
        return ref.at[pl.ds(e0, cnt), :, pl.ds(pl.multiple_of(j * self.cols, LANES), self.cols)]

    def land(self, arr, e0, cnt, src):
        if arr == 'd':
            return self.wd.at[pl.ds(e0, cnt), pl.ds(pl.multiple_of(src * self.drows, self.drows), self.drows), :]
        row = pl.ds(pl.multiple_of(src * self.rows, self.rows), self.rows)
        if arr == 'gu':
            return self.wgu.at[pl.ds(e0, cnt), row, :]
        return self.wgu.at[pl.ds(e0, cnt), row, pl.ds(0 if arr == 'g' else self.cols, self.cols)]

    def relay(self, arr, side, rel):
        if arr == 'd':
            return self.relay_d.at[side, rel]
        if arr == 'gu':
            return self.relay_gu.at[side, rel]
        return self.relay_gu.at[side, rel, :, :, pl.ds(0 if arr == 'g' else self.cols, self.cols)]

    def near(self):
        me, sib = self.place.me, self.place.at(0, 1)
        for i, arr in enumerate('gud'):
            self.wires.send(('sib', arr), self.piece(arr, 0, self.experts, sib), self.land(arr, 0, self.experts, me), wg=sib)
            self.own(i, arr).start()

    def own(self, i, arr):
        me = self.place.me
        return pltpu.make_async_copy(self.piece(arr, 0, self.experts, me), self.land(arr, 0, self.experts, me), self.loc_sems.at[i])

    def direct(self, rel, arrs):
        for arr in arrs:
            for d in DIRS:
                to = self.place.at(d, rel)
                self.wires.send(('direct', d, rel, arr), self.piece(arr, self.mine, self.half, to),
                                self.land(arr, self.mine, self.half, self.place.me), wg=to)

    def first_leg(self, rel, arrs):
        for arr in arrs:
            for side, d in enumerate(DIRS):
                e0 = self.mine + side * self.quarter
                self.wires.send(('leg1', d, rel, arr), self.piece(arr, e0, self.quarter, self.place.at(2 * d, rel)),
                                self.relay(arr, side, rel), wg=self.place.at(d, 0))

    def to_twin(self, name, arr, e0, cnt, src):
        region = self.land(arr, e0, cnt, src)
        self.wires.send(name, region, region, dp=self.place.twin)

    def direct_in(self, rel, arrs):
        for arr in arrs:
            for d in DIRS:
                src = self.place.at(-d, rel)
                for part in arr:
                    self.wires.recv(('direct', d, rel, part), self.land(part, self.mine, self.half, src))
                self.to_twin(('twin', d, rel, arr), arr, self.mine, self.half, src)

    def second_leg(self, rel, arrs):
        for arr in arrs:
            for side, d in enumerate(DIRS):
                for part in arr:
                    self.wires.recv(('leg1', d, rel, part), self.relay(part, side, rel))
                self.wires.send(('leg2', d, rel, arr), self.relay(arr, side, rel),
                                self.land(arr, self.mine + side * self.quarter, self.quarter, self.place.at(-d, 0)),
                                wg=self.place.at(d, rel))

    def far_in(self, arrs):
        for arr in arrs:
            for rel in (0, 1):
                for side, d in enumerate(DIRS):
                    src = self.place.at(2 * d, rel)
                    e0 = self.mine + side * self.quarter
                    self.wires.recv(('leg2', d, rel, arr), self.land(arr, e0, self.quarter, src))
                    self.to_twin(('twin2', d, rel, arr), arr, e0, self.quarter, src)

    def finish(self, arr):
        for part in arr:
            self.wires.recv(('sib', part), self.land(part, 0, self.experts, self.place.at(0, 1)))
            self.own('gud'.index(part), part).wait()
        for rel in (0, 1):
            for side, d in enumerate(DIRS):
                self.wires.recv(('twin', d, rel, arr), self.land(arr, self.theirs, self.half, self.place.at(-d, rel)))
                self.wires.recv(('twin2', d, rel, arr),
                                self.land(arr, self.theirs + side * self.quarter, self.quarter, self.place.at(2 * d, rel)))


class PairGather:
    def __init__(self, wires, name, src, dst, give_side):
        self.wires, self.place, self.name, self.src, self.dst = wires, wires.place, name, src, dst
        rows = src.shape[0]
        given = rows * 9 // 32
        parity = self.place.parity
        last = rows - given
        self.spans = {'give': (parity * last, given), 'both': (given, rows - 2 * given), 'take': (last - parity * last, given)}
        self.far_side = {'give': give_side, 'both': 1 - give_side}

    def part(self, owner, what):
        row, cnt = self.spans[what]
        return self.dst.at[owner, pl.ds(pl.multiple_of(row, 16), cnt), :]

    def start(self):
        place, me = self.place, self.place.me
        for what in ('give', 'both'):
            row, cnt = self.spans[what]
            own = self.src.at[pl.ds(pl.multiple_of(row, 16), cnt), :]
            for d in DIRS:
                self.wires.send((self.name, 'own', what, d), own, self.part(me, what), wg=place.at(d, 0))
        self.wires.send((self.name, 'sib'), self.src, self.dst.at[me], wg=place.at(0, 1))

    def give(self, tag, owner):
        part = self.part(owner, 'give')
        self.wires.send((self.name, 'give', tag), part, part, dp=self.place.twin)

    def near_in(self, *whats):
        place = self.place
        for what in whats:
            for side, d in enumerate(DIRS):
                owner = place.at(-d, 0)
                part = self.part(owner, what)
                self.wires.recv((self.name, 'own', what, d), part)
                if what == 'give':
                    self.give(d, owner)
                if self.far_side[what] == side:
                    self.wires.send((self.name, 'far', what), part, part, wg=place.at(d, 0))
                self.wires.send((self.name, 'across', what, d), part, part, wg=place.at(0, 1))

    def far_in(self, *whats):
        place = self.place
        owner = place.at(2, 0)
        for what in whats:
            part = self.part(owner, what)
            self.wires.recv((self.name, 'far', what), part)
            if what == 'give':
                self.give(2, owner)
            self.wires.send((self.name, 'across', what, 2), part, part, wg=place.at(0, 1))

    def twin_in(self, *tags):
        for tag in tags:
            part = self.part(self.place.at(-tag, 0), 'take')
            self.wires.recv((self.name, 'give', tag), part)
            self.wires.send((self.name, 'across', 'take', tag), part, part, wg=self.place.at(0, 1))

    def sib_in(self):
        place = self.place
        self.wires.recv((self.name, 'sib'), self.dst.at[place.at(0, 1)])
        for tag in (1, -1, 2):
            for what in ('give', 'both', 'take'):
                self.wires.recv((self.name, 'across', what, tag), self.part(place.at(-tag, 1), what))


class Gather:
    def __init__(self, wires, name, region, half_region):
        self.wires, self.place, self.name = wires, wires.place, name
        self.region, self.half_region = region, half_region

    def start(self, src):
        place, dst = self.place, self.region(self.place.me)
        for d in DIRS:
            self.wires.send((self.name, 'own', d), src, dst, wg=place.at(d, 0))
        self.wires.send((self.name, 'own', 0), src, dst, wg=place.at(0, 1))

    def near_in(self, side):
        d, place = DIRS[side], self.place
        owner = place.at(-d, 0)
        block, part = self.region(owner), self.half_region(owner, side)
        self.wires.recv((self.name, 'own', d), block)
        self.wires.send((self.name, 'far', d), part, part, wg=place.at(d, 0))
        self.wires.send((self.name, 'across', d), block, block, wg=place.at(0, 1))

    def far_in(self):
        place = self.place
        owner = place.at(2, 0)
        for side, d in enumerate(DIRS):
            part = self.half_region(owner, side)
            self.wires.recv((self.name, 'far', d), part)
            self.wires.send((self.name, 'across2', d), part, part, wg=place.at(0, 1))

    def sib_own(self):
        self.wires.recv((self.name, 'own', 0), self.region(self.place.at(0, 1)))

    def sib_near(self, side):
        self.wires.recv((self.name, 'across', DIRS[side]), self.region(self.place.at(-DIRS[side], 1)))

    def sib_far(self):
        for side, d in enumerate(DIRS):
            self.wires.recv((self.name, 'across2', d), self.half_region(self.place.at(2, 1), side))


def attention_phase(n, place, small_all, mask, cos_t, sin_t, hidden_hbm, weights, gathered, gathers, moving, gain, norm, k_out, v_out,
                    xg, loc_sems, hidden, h, acc, ctx, wbuf, load_sems, x_sems):
    wq, wk, wv, wo = weights
    gq, gk, gv, go = gathered
    gather_q, gather_k, gather_v, gather_o = gathers
    me = place.me
    prompts, seq = mask.shape[0], mask.shape[1]
    rows, d_model = hidden.shape
    depth = wq.shape[0]
    q_dim, kv_dim = wq.shape[1], wk.shape[1]
    n_kv = kv_dim // HEAD_DIM
    group = q_dim // kv_dim
    tile = 512
    load = pltpu.make_async_copy(hidden_hbm, hidden, x_sems.at[prompts])
    load.start()
    load.wait()

    def norm_in(i, carry):
        r = pl.ds(pl.multiple_of(i * 16, 16), 16)
        h[r, :] = (norm(hidden[r, :].astype(jnp.float32)) * gain(0)).astype(jnp.bfloat16)
        return carry

    with jax.named_scope('norm_in'):
        lax.fori_loop(0, rows // 16, norm_in, 0)
        acc[...] = jnp.zeros_like(acc)

    with jax.named_scope('near'):
        gather_q.near_in('give', 'both')
        gather_k.near_in('give', 'both')
        gather_v.near_in('give', 'both')
        gather_o.start()
        moving.direct(0, 'gu')
        moving.first_leg(0, 'gu')
        moving.first_leg(1, 'gu')
        moving.near()
    with jax.named_scope('qkv_far'):
        gather_q.twin_in(1, -1)
        gather_k.twin_in(1, -1)
        gather_v.twin_in(1, -1)
        gather_q.far_in('give', 'both')
        gather_k.far_in('give', 'both')
        gather_v.far_in('give', 'both')
    with jax.named_scope('qkv_last'):
        gather_q.twin_in(2)
        gather_k.twin_in(2)
        gather_v.twin_in(2)
        gather_q.sib_in()
        gather_k.sib_in()
        gather_v.sib_in()
    with jax.named_scope('o_near_give'):
        gather_o.near_in('give')

    def owner_of(i):
        return (me + i) % n

    def product(lhs, weights, first_col):
        def loads(i, slot):
            owner = owner_of(i)

            def start(own):
                col = 0
                for w, (src, gathered) in enumerate(weights):
                    width = src.shape[1]
                    pltpu.make_async_copy(src if own else gathered.at[owner], wbuf.at[slot, :, pl.ds(col, width)],
                                          load_sems.at[slot, w]).start()
                    col += width

            @pl.when(i == 0)
            def _():
                start(True)

            @pl.when(i > 0)
            def _():
                start(False)

        def step(i, carry):
            slot = i % 2
            owner = owner_of(i)

            @pl.when(i + 1 < n)
            def _():
                loads(i + 1, 1 - slot)

            col = 0
            for w, (src, gathered) in enumerate(weights):
                width = src.shape[1]
                pltpu.make_async_copy(gathered.at[owner], wbuf.at[slot, :, pl.ds(col, width)], load_sems.at[slot, w]).wait()
                col += width

            def tiles(j, carry):
                c = pl.ds(pl.multiple_of(j * tile, tile), tile)
                acc[:, c] += dot_f32(lhs[:, pl.ds(pl.multiple_of(owner * depth, depth), depth)], wbuf[slot, :, c])
                return carry

            return lax.fori_loop(0, col // tile, tiles, carry)

        loads(0, 0)
        lax.fori_loop(0, n, step, 0)

    with jax.named_scope('qkv_mm'):
        product(h, ((wq, gq), (wk, gk), (wv, gv)), 0)

    def rope(values):
        values = values.astype(jnp.bfloat16).astype(jnp.float32)
        cos_v, sin_v = cos_t[...], sin_t[...]
        times = values.shape[0] // seq
        if times > 1:
            cos_v, sin_v = jnp.concatenate([cos_v] * times, axis=0), jnp.concatenate([sin_v] * times, axis=0)
        return (values * cos_v + pltpu.roll(values, HEAD_DIM // 2, 1) * sin_v).astype(jnp.bfloat16)

    def attend(i, carry):
        p, g = i // n_kv, i % n_kv
        r = pl.ds(pl.multiple_of(p * seq, seq), seq)
        kv_cols = pl.ds(pl.multiple_of(g * HEAD_DIM, HEAD_DIM), HEAD_DIM)
        q = jnp.concatenate([acc[r, pl.ds(pl.multiple_of((g * group + j) * HEAD_DIM, HEAD_DIM), HEAD_DIM)]
                             for j in range(group)], axis=0)
        q = rope(q)
        k = rope(acc[r, pl.ds(pl.multiple_of(q_dim + g * HEAD_DIM, HEAD_DIM), HEAD_DIM)])
        v = acc[r, pl.ds(pl.multiple_of(q_dim + kv_dim + g * HEAD_DIM, HEAD_DIM), HEAD_DIM)].astype(jnp.bfloat16)
        k_out[r, kv_cols] = k
        v_out[r, kv_cols] = v
        scores = lax.dot_general(q, k, (((1,), (1,)), ((), ())), preferred_element_type=jnp.float32) * ATTN_SCALE
        scores = SOFT_CAP * jnp.tanh(scores / SOFT_CAP)
        allowed = jnp.concatenate([mask[p]] * group, axis=0) > 0.5
        scores = jnp.where(allowed, scores, -1e30)
        ex = jnp.exp(scores - jnp.max(scores, axis=-1, keepdims=True))
        probs = (ex / jnp.sum(ex, axis=-1, keepdims=True)).astype(jnp.bfloat16)
        out = dot_f32(probs, v).astype(jnp.bfloat16)
        for j in range(group):
            ctx[r, pl.ds(pl.multiple_of((g * group + j) * HEAD_DIM, HEAD_DIM), HEAD_DIM)] = out[j * seq:(j + 1) * seq]
        return carry

    with jax.named_scope('attend'):
        lax.fori_loop(0, prompts * n_kv, attend, 0)

    with jax.named_scope('o_near_both'):
        gather_o.near_in('both')
    with jax.named_scope('direct_in0'):
        moving.direct_in(0, ('gu',))
    with jax.named_scope('leg2'):
        moving.second_leg(0, ('gu',))
        moving.second_leg(1, ('gu',))
        moving.direct(1, 'gu')
        moving.direct(0, 'd')
        moving.first_leg(0, 'd')
        moving.first_leg(1, 'd')
        moving.direct(1, 'd')
    with jax.named_scope('o_far'):
        gather_o.twin_in(1, -1)
        gather_o.far_in('give', 'both')
    with jax.named_scope('mv_far'):
        moving.far_in(('gu',))
    with jax.named_scope('o_last'):
        gather_o.twin_in(2)
        gather_o.sib_in()
    with jax.named_scope('o_mm'):
        acc[...] = jnp.zeros_like(acc)
        product(ctx, ((wo, go),), 0)

    def finish_rows(i, carry):
        r = pl.ds(pl.multiple_of(i * 16, 16), 16)
        mid = (hidden[r, :].astype(jnp.float32) + norm(acc[r, pl.ds(0, d_model)]) * gain(1)).astype(jnp.bfloat16)
        ctx[r, :] = mid
        return carry

    with jax.named_scope('finish_rows'):
        lax.fori_loop(0, rows // 16, finish_rows, 0)
    stores = []
    for t in range(prompts):
        desc = pltpu.make_async_copy(ctx.at[pl.ds(t * seq, seq), :], xg.at[t, me], x_sems.at[t])
        desc.start()
        stores.append(desc)
    for desc in stores:
        desc.wait()


def moe_phase(n, experts, wires, moving, h_gathers, small, small_all, gain, norm, wgu, wd, xg, y_out, relay_y, u_all, vd, ss_all,
              vgu, hbuf, gates, us, mbuf, ybuf, xcols, route, router, gain_in, load_sems, w_sems, x_sems, out_sems):
    place = wires.place
    steps, seq, d_model = route.shape[0], route.shape[3], hbuf.shape[3]
    chips, me = place.chips, place.me
    rows = 2 * seq
    depth = small.shape[1]
    cols = vgu.shape[2] // 2
    dcols = vd.shape[2]
    offsets = (0, -1, 1, 2)

    with jax.named_scope('tables'):
        gain_in[...] = gain(2)
        for j in range(n):
            router[:, pl.ds(j * depth, depth)] = small_all[j]

        def route_of(j, carry):
            for t in range(steps):
                for i in range(2):
                    line = small_all[j, pl.ds(experts + 4 + i, 1), pl.ds(t * seq, seq)].astype(jnp.float32)
                    route[t, j, i] = jnp.transpose(jnp.broadcast_to(line, (LANES, seq))).astype(jnp.bfloat16)
            return carry

        lax.fori_loop(0, n, route_of, 0)

    own_cols = pl.ds(pl.multiple_of(me * dcols, LANES), dcols)

    def u_owner_chip(owner, q):
        return (owner // 2 + offsets[q] + chips) % chips

    u_gathers = {t: [] for t in range(steps)}
    others = [(off, rel) for off in (0, 1, -1, 2) for rel in (0, 1)][1:]

    def fetch(t, q, slot):
        chip = place.chip_at(offsets[q])
        return [pltpu.make_async_copy(xg.at[t, pl.ds(2 * chip, 2)], hbuf.at[slot], load_sems.at[slot])]

    def up_part(t, q, slot):
        chip = place.chip_at(offsets[q])
        h = hbuf.at[slot]
        r0 = route[t, pl.ds(2 * chip, 2), 0].reshape(rows, LANES).astype(jnp.float32)
        r1 = route[t, pl.ds(2 * chip, 2), 1].reshape(rows, LANES).astype(jnp.float32)

        def norm_rows(i, carry):
            r = pl.ds(pl.multiple_of(i % (seq // 32) * 32, 32), 32)
            x = h[i // (seq // 32), r, :].astype(jnp.float32)
            h[i // (seq // 32), r, :] = (norm(x) * gain_in[...]).astype(jnp.bfloat16)
            return carry

        with jax.named_scope('norm'):
            lax.fori_loop(0, rows // 32, norm_rows, 0)
        logits = lax.dot_general(h[...].reshape(rows, d_model), router[...], (((1,), (1,)), ((), ())),
                                 preferred_element_type=jnp.float32)
        lane = lax.broadcasted_iota(jnp.int32, logits.shape, 1)
        logits = jnp.where(lane < experts, logits, -1e30)
        peak = jnp.max(logits, axis=-1, keepdims=True)
        ex = jnp.where(lane < experts, jnp.exp(logits - peak), 0.0)
        probs = ex / jnp.sum(ex, axis=-1, keepdims=True)
        lane_f = lane.astype(jnp.float32)
        for i, r in enumerate((r0, r1)):
            g = jnp.sum(jnp.where(lane_f == r[:, :logits.shape[1]], probs, 0.0), axis=-1, keepdims=True)
            gates[t, chip, i] = jnp.broadcast_to(g, (rows, LANES))

        def expert(e, carry):
            act = dot_f32(h[...].reshape(rows, d_model), vgu[e])
            inner = (jax.nn.gelu(act[:, :cols]) * act[:, cols:]).astype(jnp.bfloat16).astype(jnp.float32)
            e_f = e.astype(jnp.float32)
            us[0] = jnp.where(route[t, pl.ds(2 * chip, 2), 0].reshape(rows, LANES).astype(jnp.float32) == e_f, inner, us[0])
            us[1] = jnp.where(route[t, pl.ds(2 * chip, 2), 1].reshape(rows, LANES).astype(jnp.float32) == e_f, inner, us[1])
            return carry

        us[...] = jnp.zeros_like(us)
        lax.fori_loop(0, experts, expert, 0)
        for i in range(2):
            u_all[t, chip, me, :, pl.ds(i * cols, cols)] = us[i].astype(jnp.bfloat16)
        if t == steps - 1:
            gather = Gather(wires, ('u', t, q), lambda owner: u_all.at[t, u_owner_chip(owner, q), owner],
                            lambda owner, side: u_all.at[t, u_owner_chip(owner, q), owner, pl.ds(side * seq, seq), :])
            gather.start(u_all.at[t, chip, me])
            u_gathers[t].append(gather)
        elif q == 3:
            gather = Gather(wires, ('u', t), lambda owner: u_all.at[t, :, owner],
                            lambda owner, side: u_all.at[t, pl.ds(side * (chips // 2), chips // 2), owner])
            gather.start(u_all.at[t, :, me])
            u_gathers[t].append(gather)

    def begin(t, q):
        loads = fetch(t, q, (4 * t + q) % 3)
        for desc in loads:
            desc.start()
        return loads

    def chunk_near(t):
        h_gathers[t].near_in(0)
        h_gathers[t].near_in(1)
        if t + 1 < steps:
            h_gathers[t + 1].start(xg.at[t + 1, me])

    def phase_a(t, between):
        gather = h_gathers[t]
        if t == 0:
            with jax.named_scope('first'):
                chunk_near(0)
                moving.far_in(('d',))
            with jax.named_scope('gu_in'):
                moving.finish('gu')
            w_loads = []
            for e in range(experts):
                desc = pltpu.make_async_copy(wgu.at[e], vgu.at[e], w_sems.at[e])
                desc.start()
                w_loads.append(desc)
        with jax.named_scope('arrive'):
            gather.sib_own()
            own = begin(t, 0)
            if t == 0:
                for desc in w_loads:
                    desc.wait()
        use(t, 0, own)
        with jax.named_scope('arrive'):
            if t > 0:
                chunk_near(t)
            gather.sib_near(0)
            left = begin(t, 1)
            gather.sib_near(1)
            right = begin(t, 2)
        use(t, 1, left)
        between()
        use(t, 2, right)
        with jax.named_scope('arrive'):
            gather.far_in()
            gather.sib_far()
            far = begin(t, 3)
        use(t, 3, far)

    def use(t, q, loads):
        with jax.named_scope('load'):
            for desc in loads:
                desc.wait()
        with jax.named_scope('up'):
            up_part(t, q, (4 * t + q) % 3)

    def u_near(t):
        with jax.named_scope('u_near'):
            for gather in u_gathers[t]:
                gather.near_in(0)
                gather.near_in(1)

    def phase_b(t):
        if t == 0:
            with jax.named_scope('d_in'):
                moving.finish('d')
                d_load = pltpu.make_async_copy(wd, vd, w_sems.at[experts])
                d_load.start()
                d_load.wait()
        for gather in u_gathers[t]:
            with jax.named_scope('u_wait'):
                gather.far_in()
                gather.sib_own()
                gather.sib_near(0)
                gather.sib_near(1)
                gather.sib_far()
        for q in range(4):
            chip = place.chip_at(offsets[q])
            acc = mbuf.at[q]
            acc[...] = jnp.zeros_like(acc)

            def expert(e, carry):
                e_b = e.astype(jnp.bfloat16)
                r0 = route[t, pl.ds(2 * chip, 2), 0].reshape(rows, LANES)
                r1 = route[t, pl.ds(2 * chip, 2), 1].reshape(rows, LANES)
                m0, m1 = r0 == e_b, r1 == e_b
                zero = jnp.zeros((rows, LANES), jnp.bfloat16)
                parts = []
                for j in range(n):
                    parts.append(jnp.where(m0, u_all[t, chip, j, :, pl.ds(0, cols)],
                                           jnp.where(m1, u_all[t, chip, j, :, pl.ds(cols, cols)], zero)))
                ue = jnp.concatenate(parts, axis=1)
                out = dot_f32(ue, vd[e])
                e_f = e.astype(jnp.float32)
                gate = jnp.where(r0.astype(jnp.float32) == e_f, gates[t, chip, 0],
                                 jnp.where(r1.astype(jnp.float32) == e_f, gates[t, chip, 1], 0.0))
                acc[...] += jnp.concatenate([gate] * (dcols // LANES), axis=1) * out
                return carry

            with jax.named_scope('down'):
                lax.fori_loop(0, experts, expert, 0)
            part = acc[...]
            squares = jnp.sum(part * part, axis=-1, keepdims=True)
            ss_all[t, chip, me] = jnp.transpose(jnp.broadcast_to(squares, (rows, LANES)))[:ss_all.shape[3]]
        for off, rel in others:
            region = ss_all.at[t, :, me]
            wires.send(('ss', t, off, rel), region, region, wg=place.at(off, rel))

    y_open = []

    def phase_c(t):
        loads = []
        for q in range(4):
            chip = place.chip_at(offsets[q])
            desc = pltpu.make_async_copy(xg.at[t, pl.ds(2 * chip, 2), :, own_cols], xcols.at[q], x_sems.at[q])
            desc.start()
            loads.append(desc)
        gain_out = small[pl.ds(experts + 3, 1), :].astype(jnp.float32)
        with jax.named_scope('ss_wait'):
            for off, rel in others:
                wires.recv(('ss', t, off, rel), ss_all.at[t, :, place.at(-off, rel)])
        for q in range(4):
            chip = place.chip_at(offsets[q])
            loads[q].wait()
            with jax.named_scope('y'):
                total = ss_all[t, chip, 0]
                for j in range(1, n):
                    total += ss_all[t, chip, j]
                line = jnp.broadcast_to(total[:1], (LANES, rows))
                scale = lax.rsqrt(jnp.transpose(line) * (1.0 / d_model) + NORM_EPS)
                scale = jnp.concatenate([scale] * (dcols // LANES), axis=1)
                x1 = xcols[q].reshape(rows, dcols).astype(jnp.float32)
                ybuf[t, q] = (x1 + mbuf[q] * scale * gain_out).astype(jnp.bfloat16).reshape(2, seq, dcols)
            dst = y_out.at[t, :, own_cols]
            for rel in (0, 1):
                part = ybuf.at[t, q, (place.core + rel) % 2]
                if q == 0 and rel == 0:
                    desc = pltpu.make_async_copy(part, dst, out_sems.at[t])
                    desc.start()
                    y_open.append(desc)
                elif q < 3:
                    wires.send(('y', t, q, rel), part, dst, wg=place.at(offsets[q], rel))
                else:
                    wires.send(('y1', t, rel), part, relay_y.at[t, rel], wg=place.at(DIRS[rel], 0))

    def y_cols(src):
        return pl.ds(pl.multiple_of(src * dcols, LANES), dcols)

    def y_relay(t):
        for rel, d in enumerate(DIRS):
            wires.recv(('y1', t, rel), relay_y.at[t, rel])
            wires.send(('y2', t, rel), relay_y.at[t, rel], y_out.at[t, :, y_cols(place.at(-d, 0))], wg=place.at(d, rel))

    def y_in(t):
        for q in range(4):
            for rel in (0, 1):
                if q == 0 and rel == 0:
                    continue
                wires.recv(('y', t, q, rel) if q < 3 else ('y2', t, rel), y_out.at[t, :, y_cols(place.at(-offsets[q], rel))])

    phase_a(0, lambda: None)
    for t in range(1, steps):
        phase_a(t, lambda: u_near(t - 1))
        if t == steps - 1:
            u_near(t)
        if t > 1:
            phase_c(t - 2)
        phase_b(t - 1)
    phase_c(steps - 2)
    for t in range(steps - 2):
        y_relay(t)
    phase_b(steps - 1)
    y_relay(steps - 2)
    phase_c(steps - 1)
    y_relay(steps - 1)
    with jax.named_scope('y_in'):
        for t in range(steps):
            y_in(t)
        for desc in y_open:
            desc.wait()
        wires.finish()


def layer_kernel(n, experts, small, mask, cos_t, sin_t, hidden, wq, wk, wv, wo, gate, up, down,
                 k_out, v_out, small_all, y_out, gq, gk, gv, go, wgu, wd, relay_gu, relay_d, xg, relay_y,
                 u_all, vd, ss_all, send_sems, recv_sems, loc_sems):
    place = Place(n)
    wires = Wires(place, send_sems, recv_sems)
    me = place.me
    prompts, seq = mask.shape[0], mask.shape[1]
    rows, d_model = hidden.shape
    cols, dcols = gate.shape[2] // n, down.shape[2] // n
    q_dim, kv_dim = wq.shape[1], wk.shape[1]
    bf16, f32 = jnp.bfloat16, jnp.float32

    enter(place)
    others = [(off, rel) for off in (0, 1, -1, 2) for rel in (0, 1)][1:]
    for off, rel in others:
        wires.send(('small', off, rel), small, small_all.at[me], wg=place.at(off, rel))
    gather_q = PairGather(wires, 'q', wq, gq, 0)
    gather_k = PairGather(wires, 'k', wk, gk, 1)
    gather_v = PairGather(wires, 'v', wv, gv, 1)
    gather_o = PairGather(wires, 'o', wo, go, 0)
    moving = Reshard(wires, gate, up, down, wgu, wd, relay_gu, relay_d, loc_sems)
    gather_q.start()
    gather_k.start()
    gather_v.start()
    small_all[me] = small[...]
    for off, rel in others:
        wires.recv(('small', off, rel), small_all.at[place.at(-off, rel)])

    def gain(i):
        return jnp.concatenate([small_all[j, pl.ds(experts + i, 1), :] for j in range(n)], axis=1).astype(jnp.float32)

    def norm(values):
        return values * lax.rsqrt(jnp.mean(values * values, axis=-1, keepdims=True) + NORM_EPS)

    h_gathers = [Gather(wires, ('h', t), lambda owner, t=t: xg.at[t, owner],
                        lambda owner, side, t=t: xg.at[t, owner, pl.ds(side * (seq // 2), seq // 2), :]) for t in range(prompts)]
    pl.run_scoped(
        functools.partial(attention_phase, n, place, small_all, mask, cos_t, sin_t, hidden, (wq, wk, wv, wo), (gq, gk, gv, go),
                          (gather_q, gather_k, gather_v, gather_o), moving, gain, norm, k_out, v_out, xg, loc_sems),
        pltpu.VMEM((rows, d_model), bf16),
        pltpu.VMEM((rows, d_model), bf16),
        pltpu.VMEM((rows, q_dim + 2 * kv_dim), f32),
        pltpu.VMEM((rows, q_dim), bf16),
        pltpu.VMEM((2, wq.shape[0], q_dim + 2 * kv_dim), bf16),
        pltpu.SemaphoreType.DMA((2, 3)),
        pltpu.SemaphoreType.DMA((prompts + 1,)),
    )
    h_gathers[0].start(xg.at[0, me])
    with jax.named_scope('services'):
        moving.direct_in(1, ('gu',))
        moving.second_leg(0, ('d',))
        moving.second_leg(1, ('d',))
        moving.direct_in(0, ('d',))
        moving.direct_in(1, ('d',))
    pl.run_scoped(
        functools.partial(moe_phase, n, experts, wires, moving, h_gathers, small, small_all, gain, norm, wgu, wd, xg, y_out, relay_y,
                          u_all, vd, ss_all),
        pltpu.VMEM((experts, d_model, 2 * cols), bf16),
        pltpu.VMEM((3, 2, seq, d_model), bf16),
        pltpu.VMEM((prompts, n // 2, 2, 2 * seq, LANES), f32),
        pltpu.VMEM((2, 2 * seq, cols), f32),
        pltpu.VMEM((4, 2 * seq, dcols), f32),
        pltpu.VMEM((prompts, 4, 2, seq, dcols), bf16),
        pltpu.VMEM((4, 2, seq, dcols), bf16),
        pltpu.VMEM((prompts, n, 2, seq, LANES), bf16),
        pltpu.VMEM((small.shape[0], d_model), bf16),
        pltpu.VMEM((1, d_model), f32),
        pltpu.SemaphoreType.DMA((3,)),
        pltpu.SemaphoreType.DMA((experts + 1,)),
        pltpu.SemaphoreType.DMA((4,)),
        pltpu.SemaphoreType.DMA((prompts,)),
    )


def layer(n, experts, prompts, small, mask, cos_t, sin_t, hidden, wq, wk, wv, wo, gate, up, down):
    rows, d_model = hidden.shape
    seq = rows // prompts
    ff = gate.shape[2]
    drows = down.shape[1]
    cols, dcols = ff // n, d_model // n
    bf16, f32 = jnp.bfloat16, jnp.float32
    quarter = experts // 4

    def full(w):
        return jax.ShapeDtypeStruct((n,) + w.shape, bf16)

    outs = pl.pallas_call(
        functools.partial(layer_kernel, n, experts),
        name='layer',
        out_shape=(
            jax.ShapeDtypeStruct((rows, wk.shape[1]), bf16),
            jax.ShapeDtypeStruct((rows, wv.shape[1]), bf16),
            full(small),
            jax.ShapeDtypeStruct((prompts, seq, d_model), bf16),
            full(wq), full(wk), full(wv), full(wo),
            jax.ShapeDtypeStruct((experts, d_model, 2 * cols), bf16),
            jax.ShapeDtypeStruct((experts, ff, dcols), bf16),
            jax.ShapeDtypeStruct((2, 2, quarter, gate.shape[1], 2 * cols), bf16),
            jax.ShapeDtypeStruct((2, 2, quarter, drows, dcols), bf16),
            jax.ShapeDtypeStruct((prompts, n, seq, d_model), bf16),
            jax.ShapeDtypeStruct((prompts, 2, seq, dcols), bf16),
        ),
        in_specs=[VMEM_FULL] * 4 + [ANY] * 8,
        out_specs=(VMEM_FULL,) * 3 + (ANY,) * 11,
        scratch_shapes=[
            pltpu.VMEM((prompts, n // 2, n, 2 * seq, 2 * cols), bf16),
            pltpu.VMEM((experts, ff, dcols), bf16),
            pltpu.VMEM((prompts, n // 2, n, 8, 2 * seq), f32),
            pltpu.SemaphoreType.DMA((416,)),
            pltpu.SemaphoreType.DMA((416,)),
            pltpu.SemaphoreType.DMA((4,)),
        ],
        compiler_params=pltpu.CompilerParams(collective_id=0, has_side_effects=True, vmem_limit_bytes=66_500_000),
        cost_estimate=pl.CostEstimate(flops=110_000_000_000, bytes_accessed=400_000_000, transcendentals=0),
    )(small, mask, cos_t, sin_t, hidden, wq, wk, wv, wo, gate, up, down)
    return outs[3], outs[0], outs[1]


def solution(mesh):
    n = mesh.shape['wg']
    row_spec = P(('dp', 'wg'))
    dim0_spec = P('wg', None)
    dim1_spec = P(None, 'wg', None)

    def device_fn(hidden, seq_lens, route_idx, g_attn_in, w_query, w_key, w_value, w_attn_out, g_attn_out, g_moe_in, w_router, w_gate, w_up, w_down, g_moe_out):
        n_prompts, seq_len, d_model = hidden.shape
        experts = w_router.shape[1]
        rows = n_prompts * seq_len
        depth = w_query.shape[0]
        routes = jnp.pad(route_idx.T.astype(jnp.bfloat16), ((0, 0), (0, depth - rows)))
        small = jnp.concatenate([w_router.T] + [g[None] for g in (g_attn_in, g_attn_out, g_moe_in, g_moe_out)] + [routes], axis=0)
        small = jnp.pad(small, ((0, -small.shape[0] % 16), (0, 0)))
        pos = jnp.arange(seq_len)
        mask = ((pos[None, None, :] <= pos[None, :, None]) & (pos[None, None, :] < seq_lens[:, None, None])).astype(jnp.float32)
        cos_t, sin_t = rope_tables(seq_len)
        tok_rows = hidden.reshape(rows, d_model)
        y_out, k_rope, v_rows = layer(
            n, experts, n_prompts, small, mask, cos_t, sin_t, tok_rows, w_query, w_key, w_value, w_attn_out, w_gate, w_up, w_down)
        cache = (n_prompts, seq_len, w_key.shape[1] // HEAD_DIM, HEAD_DIM)
        return y_out, k_rope.reshape(cache), v_rows.reshape(cache)

    return jax.shard_map(
        device_fn,
        mesh=mesh,
        in_specs=(row_spec, row_spec, row_spec, P('wg'), dim0_spec, dim0_spec, dim0_spec, dim0_spec, P('wg'), P('wg'), dim0_spec, dim1_spec, dim1_spec, dim1_spec, P('wg')),
        out_specs=(row_spec, row_spec, row_spec),
        check_vma=False,
    )
```

```python
import functools
import jax
import jax.numpy as jnp
from jax import lax
from jax.experimental import pallas as pl
from jax.experimental.pallas import tpu as pltpu
from jax.sharding import PartitionSpec as P

HEAD_DIM = 128
LANES = 128
SOFT_CAP = 30.0
NORM_EPS = 1e-5
ROPE_BASE = 10000.0
ATTN_SCALE = HEAD_DIM ** -0.5
MESH = pl.DeviceIdType.MESH
ANY = pl.BlockSpec(memory_space=pl.ANY)
VMEM_FULL = pl.BlockSpec(memory_space=pltpu.VMEM)
DIRS = (1, -1)


def dot_f32(left_op, right_op):
    return jnp.dot(left_op, right_op, preferred_element_type=jnp.float32)


def rms_norm(values, gain_vec):
    values_f32 = values.astype(jnp.float32)
    inv_rms = lax.rsqrt(jnp.mean(values_f32 * values_f32, axis=-1, keepdims=True) + NORM_EPS)
    return values_f32 * inv_rms * gain_vec.astype(jnp.float32)


def rope_tables(seq_len):
    half_dim = HEAD_DIM // 2
    inv_freq = ROPE_BASE ** (-jnp.arange(half_dim, dtype=jnp.float32) * (2.0 / HEAD_DIM))
    angles = jnp.arange(seq_len, dtype=jnp.float32)[:, None] * inv_freq[None, :]
    cos_t, sin_t = jnp.cos(angles), jnp.sin(angles)
    return jnp.concatenate([cos_t, cos_t], axis=1), jnp.concatenate([-sin_t, sin_t], axis=1)


class Place:
    def __init__(self, n):
        self.n = n
        self.chips = n // 2
        self.me = lax.axis_index('wg')
        self.dp = lax.axis_index('dp')
        self.chip = self.me // 2
        self.core = self.me % 2
        self.parity = self.dp % 2
        self.twin = self.dp + 1 - 2 * self.parity

    def at(self, offset, rel):
        return ((self.chip + offset + self.chips) % self.chips) * 2 + (self.core + rel) % 2

    def chip_at(self, offset):
        return (self.chip + offset + self.chips) % self.chips


def still(ref):
    if not hasattr(ref, 'transforms'):
        return ref
    out = ref.ref
    for step in ref.transforms:
        out = out.at[tuple(pl.ds(0, index.size) if hasattr(index, 'start') else pl.ds(0, 1) for index in step.indices)]
    return out


class Wires:
    def __init__(self, place, send_sems, recv_sems):
        self.place, self.send_sems, self.recv_sems = place, send_sems, recv_sems
        self.slots = {}
        self.open = []

    def copy(self, name, src, dst, wg=None, dp=None):
        slot = self.slots.setdefault(name, len(self.slots))
        return pltpu.make_async_remote_copy(
            src_ref=src, dst_ref=dst, send_sem=self.send_sems.at[slot], recv_sem=self.recv_sems.at[slot],
            device_id={'dp': self.place.dp if dp is None else dp, 'wg': self.place.me if wg is None else wg},
            device_id_type=MESH)

    def send(self, name, src, dst, wg=None, dp=None):
        desc = self.copy(name, src, dst, wg, dp)
        desc.start()
        self.open.append((name, still(src)))

    def recv(self, name, dst):
        self.copy(name, dst, dst).wait_recv()

    def finish(self):
        for name, src in self.open:
            self.copy(name, src, src).wait_send()
        self.open = []


def enter(place):
    barrier = pltpu.get_barrier_semaphore()
    peers = [(place.dp, place.at(off, rel)) for off in (1, -1, 2) for rel in (0, 1)] + [(place.dp, place.at(0, 1))]
    peers.append((place.twin, place.me))
    for dp, wg in peers:
        pl.semaphore_signal(barrier, inc=1, device_id={'dp': dp, 'wg': wg}, device_id_type=MESH)
    pl.semaphore_wait(barrier, len(peers))


class Reshard:
    def __init__(self, wires, gate, up, down, wgu, wd, relay_gu, relay_d, loc_sems):
        self.wires, self.place = wires, wires.place
        n = self.place.n
        self.gate, self.up, self.down, self.wgu, self.wd = gate, up, down, wgu, wd
        self.relay_gu, self.relay_d, self.loc_sems = relay_gu, relay_d, loc_sems
        self.experts, self.rows, self.cols = gate.shape[0], gate.shape[1], gate.shape[2] // n
        self.drows, self.dcols = down.shape[1], down.shape[2] // n
        self.half, self.quarter = self.experts // 2, self.experts // 4
        self.mine = self.place.parity * self.half
        self.theirs = self.half - self.mine

    def piece(self, arr, e0, cnt, j):
        if arr == 'd':
            return self.down.at[pl.ds(e0, cnt), :, pl.ds(pl.multiple_of(j * self.dcols, LANES), self.dcols)]
        ref = self.gate if arr == 'g' else self.up
        return ref.at[pl.ds(e0, cnt), :, pl.ds(pl.multiple_of(j * self.cols, LANES), self.cols)]

    def land(self, arr, e0, cnt, src):
        if arr == 'd':
            return self.wd.at[pl.ds(e0, cnt), pl.ds(pl.multiple_of(src * self.drows, self.drows), self.drows), :]
        row = pl.ds(pl.multiple_of(src * self.rows, self.rows), self.rows)
        if arr == 'gu':
            return self.wgu.at[pl.ds(e0, cnt), row, :]
        return self.wgu.at[pl.ds(e0, cnt), row, pl.ds(0 if arr == 'g' else self.cols, self.cols)]

    def relay(self, arr, side, rel):
        if arr == 'd':
            return self.relay_d.at[side, rel]
        if arr == 'gu':
            return self.relay_gu.at[side, rel]
        return self.relay_gu.at[side, rel, :, :, pl.ds(0 if arr == 'g' else self.cols, self.cols)]

    def near(self):
        me, sib = self.place.me, self.place.at(0, 1)
        for i, arr in enumerate('gud'):
            self.wires.send(('sib', arr), self.piece(arr, 0, self.experts, sib), self.land(arr, 0, self.experts, me), wg=sib)
            self.own(i, arr).start()

    def own(self, i, arr):
        me = self.place.me
        return pltpu.make_async_copy(self.piece(arr, 0, self.experts, me), self.land(arr, 0, self.experts, me), self.loc_sems.at[i])

    def direct(self, rel, arrs):
        for arr in arrs:
            for d in DIRS:
                to = self.place.at(d, rel)
                self.wires.send(('direct', d, rel, arr), self.piece(arr, self.mine, self.half, to),
                                self.land(arr, self.mine, self.half, self.place.me), wg=to)

    def first_leg(self, rel, arrs):
        for arr in arrs:
            for side, d in enumerate(DIRS):
                e0 = self.mine + side * self.quarter
                self.wires.send(('leg1', d, rel, arr), self.piece(arr, e0, self.quarter, self.place.at(2 * d, rel)),
                                self.relay(arr, side, rel), wg=self.place.at(d, 0))

    def to_twin(self, name, arr, e0, cnt, src):
        region = self.land(arr, e0, cnt, src)
        self.wires.send(name, region, region, dp=self.place.twin)

    def direct_in(self, rel, arrs):
        for arr in arrs:
            for d in DIRS:
                src = self.place.at(-d, rel)
                for part in arr:
                    self.wires.recv(('direct', d, rel, part), self.land(part, self.mine, self.half, src))
                self.to_twin(('twin', d, rel, arr), arr, self.mine, self.half, src)

    def second_leg(self, rel, arrs):
        for arr in arrs:
            for side, d in enumerate(DIRS):
                for part in arr:
                    self.wires.recv(('leg1', d, rel, part), self.relay(part, side, rel))
                self.wires.send(('leg2', d, rel, arr), self.relay(arr, side, rel),
                                self.land(arr, self.mine + side * self.quarter, self.quarter, self.place.at(-d, 0)),
                                wg=self.place.at(d, rel))

    def far_in(self, arrs):
        for arr in arrs:
            for rel in (0, 1):
                for side, d in enumerate(DIRS):
                    src = self.place.at(2 * d, rel)
                    e0 = self.mine + side * self.quarter
                    self.wires.recv(('leg2', d, rel, arr), self.land(arr, e0, self.quarter, src))
                    self.to_twin(('twin2', d, rel, arr), arr, e0, self.quarter, src)

    def finish_near(self, arr):
        for part in arr:
            self.wires.recv(('sib', part), self.land(part, 0, self.experts, self.place.at(0, 1)))
            self.own('gud'.index(part), part).wait()

    def finish_twin(self, arr):
        for rel in (0, 1):
            for side, d in enumerate(DIRS):
                self.wires.recv(('twin', d, rel, arr), self.land(arr, self.theirs, self.half, self.place.at(-d, rel)))
                self.wires.recv(('twin2', d, rel, arr),
                                self.land(arr, self.theirs + side * self.quarter, self.quarter, self.place.at(2 * d, rel)))


class PairGather:
    def __init__(self, wires, name, src, dst, give_side):
        self.wires, self.place, self.name, self.src, self.dst = wires, wires.place, name, src, dst
        rows = src.shape[0]
        given = rows * 9 // 32
        parity = self.place.parity
        last = rows - given
        self.spans = {'give': (parity * last, given), 'both': (given, rows - 2 * given), 'take': (last - parity * last, given)}
        self.far_side = {'give': give_side, 'both': 1 - give_side}

    def part(self, owner, what):
        row, cnt = self.spans[what]
        return self.dst.at[owner, pl.ds(pl.multiple_of(row, 16), cnt), :]

    def start(self):
        place, me = self.place, self.place.me
        for what in ('give', 'both'):
            row, cnt = self.spans[what]
            own = self.src.at[pl.ds(pl.multiple_of(row, 16), cnt), :]
            for d in DIRS:
                self.wires.send((self.name, 'own', what, d), own, self.part(me, what), wg=place.at(d, 0))
        self.wires.send((self.name, 'sib'), self.src, self.dst.at[me], wg=place.at(0, 1))

    def give(self, tag, owner):
        part = self.part(owner, 'give')
        self.wires.send((self.name, 'give', tag), part, part, dp=self.place.twin)

    def near_in(self, *whats):
        place = self.place
        for what in whats:
            for side, d in enumerate(DIRS):
                owner = place.at(-d, 0)
                part = self.part(owner, what)
                self.wires.recv((self.name, 'own', what, d), part)
                if what == 'give':
                    self.give(d, owner)
                if self.far_side[what] == side:
                    self.wires.send((self.name, 'far', what), part, part, wg=place.at(d, 0))
                self.wires.send((self.name, 'across', what, d), part, part, wg=place.at(0, 1))

    def far_in(self, *whats):
        place = self.place
        owner = place.at(2, 0)
        for what in whats:
            part = self.part(owner, what)
            self.wires.recv((self.name, 'far', what), part)
            if what == 'give':
                self.give(2, owner)
            self.wires.send((self.name, 'across', what, 2), part, part, wg=place.at(0, 1))

    def twin_in(self, *tags):
        for tag in tags:
            part = self.part(self.place.at(-tag, 0), 'take')
            self.wires.recv((self.name, 'give', tag), part)
            self.wires.send((self.name, 'across', 'take', tag), part, part, wg=self.place.at(0, 1))

    def sib_in(self):
        place = self.place
        self.wires.recv((self.name, 'sib'), self.dst.at[place.at(0, 1)])
        for tag in (1, -1, 2):
            for what in ('give', 'both', 'take'):
                self.wires.recv((self.name, 'across', what, tag), self.part(place.at(-tag, 1), what))


class Gather:
    def __init__(self, wires, name, region, half_region):
        self.wires, self.place, self.name = wires, wires.place, name
        self.region, self.half_region = region, half_region

    def start(self, src):
        place, dst = self.place, self.region(self.place.me)
        for d in DIRS:
            self.wires.send((self.name, 'own', d), src, dst, wg=place.at(d, 0))
        self.wires.send((self.name, 'own', 0), src, dst, wg=place.at(0, 1))

    def near_in(self, side):
        d, place = DIRS[side], self.place
        owner = place.at(-d, 0)
        block, part = self.region(owner), self.half_region(owner, side)
        self.wires.recv((self.name, 'own', d), block)
        self.wires.send((self.name, 'far', d), part, part, wg=place.at(d, 0))
        self.wires.send((self.name, 'across', d), block, block, wg=place.at(0, 1))

    def far_in(self):
        place = self.place
        owner = place.at(2, 0)
        for side, d in enumerate(DIRS):
            part = self.half_region(owner, side)
            self.wires.recv((self.name, 'far', d), part)
            self.wires.send((self.name, 'across2', d), part, part, wg=place.at(0, 1))

    def sib_own(self):
        self.wires.recv((self.name, 'own', 0), self.region(self.place.at(0, 1)))

    def sib_near(self, side):
        self.wires.recv((self.name, 'across', DIRS[side]), self.region(self.place.at(-DIRS[side], 1)))

    def sib_far(self):
        for side, d in enumerate(DIRS):
            self.wires.recv((self.name, 'across2', d), self.half_region(self.place.at(2, 1), side))


def attention_phase(n, place, small_all, mask, cos_t, sin_t, hidden_hbm, weights, gathered, gathers, moving, gain, norm, k_out, v_out,
                    xg, loc_sems, hidden, h, acc, ctx, wbuf, load_sems, x_sems):
    wq, wk, wv, wo = weights
    gq, gk, gv, go = gathered
    gather_q, gather_k, gather_v, gather_o = gathers
    me = place.me
    prompts, seq = mask.shape[0], mask.shape[1]
    rows, d_model = hidden.shape
    depth = wq.shape[0]
    q_dim, kv_dim = wq.shape[1], wk.shape[1]
    n_kv = kv_dim // HEAD_DIM
    group = q_dim // kv_dim
    tile = 512
    load = pltpu.make_async_copy(hidden_hbm, hidden, x_sems.at[prompts])
    load.start()
    load.wait()

    def norm_in(i, carry):
        r = pl.ds(pl.multiple_of(i * 16, 16), 16)
        h[r, :] = (norm(hidden[r, :].astype(jnp.float32)) * gain(0)).astype(jnp.bfloat16)
        return carry

    with jax.named_scope('norm_in'):
        lax.fori_loop(0, rows // 16, norm_in, 0)
        acc[...] = jnp.zeros_like(acc)

    with jax.named_scope('near'):
        gather_q.near_in('give', 'both')
        gather_k.near_in('give', 'both')
        gather_v.near_in('give', 'both')
        gather_o.start()
        moving.direct(0, 'gu')
        moving.first_leg(0, 'gu')
        moving.first_leg(1, 'gu')
        moving.near()
    with jax.named_scope('qkv_far'):
        gather_q.twin_in(1, -1)
        gather_k.twin_in(1, -1)
        gather_v.twin_in(1, -1)
        gather_q.far_in('give', 'both')
        gather_k.far_in('give', 'both')
        gather_v.far_in('give', 'both')
    with jax.named_scope('qkv_last'):
        gather_q.twin_in(2)
        gather_k.twin_in(2)
        gather_v.twin_in(2)
        gather_q.sib_in()
        gather_k.sib_in()
        gather_v.sib_in()
    with jax.named_scope('o_near_give'):
        gather_o.near_in('give')

    def owner_of(i):
        return (me + i) % n

    def product(lhs, weights, first_col):
        def loads(i, slot):
            owner = owner_of(i)

            def start(own):
                col = 0
                for w, (src, gathered) in enumerate(weights):
                    width = src.shape[1]
                    pltpu.make_async_copy(src if own else gathered.at[owner], wbuf.at[slot, :, pl.ds(col, width)],
                                          load_sems.at[slot, w]).start()
                    col += width

            @pl.when(i == 0)
            def _():
                start(True)

            @pl.when(i > 0)
            def _():
                start(False)

        def step(i, carry):
            slot = i % 2
            owner = owner_of(i)

            @pl.when(i + 1 < n)
            def _():
                loads(i + 1, 1 - slot)

            col = 0
            for w, (src, gathered) in enumerate(weights):
                width = src.shape[1]
                pltpu.make_async_copy(gathered.at[owner], wbuf.at[slot, :, pl.ds(col, width)], load_sems.at[slot, w]).wait()
                col += width

            def tiles(j, carry):
                c = pl.ds(pl.multiple_of(j * tile, tile), tile)
                acc[:, c] += dot_f32(lhs[:, pl.ds(pl.multiple_of(owner * depth, depth), depth)], wbuf[slot, :, c])
                return carry

            return lax.fori_loop(0, col // tile, tiles, carry)

        loads(0, 0)
        lax.fori_loop(0, n, step, 0)

    with jax.named_scope('qkv_mm'):
        product(h, ((wq, gq), (wk, gk), (wv, gv)), 0)

    def rope(values):
        values = values.astype(jnp.bfloat16).astype(jnp.float32)
        cos_v, sin_v = cos_t[...], sin_t[...]
        times = values.shape[0] // seq
        if times > 1:
            cos_v, sin_v = jnp.concatenate([cos_v] * times, axis=0), jnp.concatenate([sin_v] * times, axis=0)
        return (values * cos_v + pltpu.roll(values, HEAD_DIM // 2, 1) * sin_v).astype(jnp.bfloat16)

    def attend(i, carry):
        p, g = i // n_kv, i % n_kv
        r = pl.ds(pl.multiple_of(p * seq, seq), seq)
        kv_cols = pl.ds(pl.multiple_of(g * HEAD_DIM, HEAD_DIM), HEAD_DIM)
        q = jnp.concatenate([acc[r, pl.ds(pl.multiple_of((g * group + j) * HEAD_DIM, HEAD_DIM), HEAD_DIM)]
                             for j in range(group)], axis=0)
        q = rope(q)
        k = rope(acc[r, pl.ds(pl.multiple_of(q_dim + g * HEAD_DIM, HEAD_DIM), HEAD_DIM)])
        v = acc[r, pl.ds(pl.multiple_of(q_dim + kv_dim + g * HEAD_DIM, HEAD_DIM), HEAD_DIM)].astype(jnp.bfloat16)
        k_out[r, kv_cols] = k
        v_out[r, kv_cols] = v
        scores = lax.dot_general(q, k, (((1,), (1,)), ((), ())), preferred_element_type=jnp.float32) * ATTN_SCALE
        scores = SOFT_CAP * jnp.tanh(scores / SOFT_CAP)
        allowed = jnp.concatenate([mask[p]] * group, axis=0) > 0.5
        scores = jnp.where(allowed, scores, -1e30)
        ex = jnp.exp(scores - jnp.max(scores, axis=-1, keepdims=True))
        probs = (ex / jnp.sum(ex, axis=-1, keepdims=True)).astype(jnp.bfloat16)
        out = dot_f32(probs, v).astype(jnp.bfloat16)
        for j in range(group):
            ctx[r, pl.ds(pl.multiple_of((g * group + j) * HEAD_DIM, HEAD_DIM), HEAD_DIM)] = out[j * seq:(j + 1) * seq]
        return carry

    with jax.named_scope('attend'):
        lax.fori_loop(0, prompts * n_kv, attend, 0)

    with jax.named_scope('o_near_both'):
        gather_o.near_in('both')
    with jax.named_scope('direct_in0'):
        moving.direct_in(0, ('gu',))
    with jax.named_scope('leg2'):
        moving.second_leg(0, ('gu',))
        moving.second_leg(1, ('gu',))
        moving.direct(1, 'gu')
        moving.direct(0, 'd')
        moving.direct(1, 'd')
    with jax.named_scope('o_far'):
        gather_o.twin_in(1, -1)
        gather_o.far_in('give', 'both')
    with jax.named_scope('mv_far'):
        moving.far_in(('gu',))
    with jax.named_scope('o_last'):
        gather_o.twin_in(2)
        gather_o.sib_in()
    with jax.named_scope('o_mm'):
        acc[...] = jnp.zeros_like(acc)
        product(ctx, ((wo, go),), 0)

    def finish_rows(i, carry):
        r = pl.ds(pl.multiple_of(i * 16, 16), 16)
        mid = (hidden[r, :].astype(jnp.float32) + norm(acc[r, pl.ds(0, d_model)]) * gain(1)).astype(jnp.bfloat16)
        ctx[r, :] = mid
        return carry

    with jax.named_scope('finish_rows'):
        lax.fori_loop(0, rows // 16, finish_rows, 0)
    stores = []
    for t in range(prompts):
        desc = pltpu.make_async_copy(ctx.at[pl.ds(t * seq, seq), :], xg.at[t, me], x_sems.at[t])
        desc.start()
        stores.append(desc)
    for desc in stores:
        desc.wait()


def moe_phase(n, experts, wires, moving, h_gathers, small, small_all, gain, norm, wgu, wd, xg, y_out, relay_y, u_all, vd, ss_all,
              vgu, hbuf, gates, us, mbuf, ybuf, xcols, route, router, gain_in, load_sems, w_sems, x_sems, out_sems):
    place = wires.place
    steps, seq, d_model = route.shape[0], route.shape[3], hbuf.shape[3]
    chips, me = place.chips, place.me
    rows = 2 * seq
    depth = small.shape[1]
    cols = vgu.shape[2] // 2
    dcols = vd.shape[2]
    offsets = (0, -1, 1, 2)

    with jax.named_scope('tables'):
        gain_in[...] = gain(2)
        for j in range(n):
            router[:, pl.ds(j * depth, depth)] = small_all[j]

        def route_of(j, carry):
            for t in range(steps):
                for i in range(2):
                    line = small_all[j, pl.ds(experts + 4 + i, 1), pl.ds(t * seq, seq)].astype(jnp.float32)
                    route[t, j, i] = jnp.transpose(jnp.broadcast_to(line, (LANES, seq))).astype(jnp.bfloat16)
            return carry

        lax.fori_loop(0, n, route_of, 0)

    own_cols = pl.ds(pl.multiple_of(me * dcols, LANES), dcols)
    half = experts // 2

    def u_owner_chip(owner, q):
        return (owner // 2 + offsets[q] + chips) % chips

    u_gathers = {t: [] for t in range(steps)}
    others = [(off, rel) for off in (0, 1, -1, 2) for rel in (0, 1)][1:]

    pairs = ((0, 1), (2, 3))

    def begin(t, pair):
        loads = []
        for s, q in enumerate(pairs[pair]):
            chip = place.chip_at(offsets[q])
            desc = pltpu.make_async_copy(xg.at[t, pl.ds(2 * chip, 2)], hbuf.at[pair, pl.ds(2 * s, 2)], load_sems.at[pair, s])
            desc.start()
            loads.append(desc)
        return loads

    def routes(t, chips_of):
        def one(i):
            return jnp.concatenate([route[t, pl.ds(2 * chip, 2), i].reshape(rows, LANES) for chip in chips_of], axis=0)

        return one(0), one(1)

    def prepare(t, pair, loads):
        with jax.named_scope('load'):
            for desc in loads:
                desc.wait()
        h = hbuf.at[pair]

        def norm_rows(i, carry):
            r = pl.ds(pl.multiple_of(i % (seq // 32) * 32, 32), 32)
            x = h[i // (seq // 32), r, :].astype(jnp.float32)
            h[i // (seq // 32), r, :] = (norm(x) * gain_in[...]).astype(jnp.bfloat16)
            return carry

        with jax.named_scope('norm'):
            lax.fori_loop(0, 2 * rows // 32, norm_rows, 0)
        logits = lax.dot_general(h[...].reshape(2 * rows, d_model), router[...], (((1,), (1,)), ((), ())),
                                 preferred_element_type=jnp.float32)
        lane = lax.broadcasted_iota(jnp.int32, logits.shape, 1)
        logits = jnp.where(lane < experts, logits, -1e30)
        peak = jnp.max(logits, axis=-1, keepdims=True)
        ex = jnp.where(lane < experts, jnp.exp(logits - peak), 0.0)
        probs = ex / jnp.sum(ex, axis=-1, keepdims=True)
        lane_f = lane.astype(jnp.float32)
        chips_of = [place.chip_at(offsets[q]) for q in pairs[pair]]
        g0, g1 = (jnp.sum(jnp.where(lane_f == r[:, :logits.shape[1]].astype(jnp.float32), probs, 0.0), axis=-1, keepdims=True)
                  for r in routes(t, chips_of))
        both = jnp.where(lax.broadcasted_iota(jnp.int32, (2 * rows, LANES), 1) == 0, g0, g1)
        for s, chip in enumerate(chips_of):
            gates[t, chip] = both[s * rows:(s + 1) * rows]
        us[...] = jnp.zeros_like(us)

    def up_part(t, pair, e0, cnt):
        h = hbuf.at[pair]
        chips_of = [place.chip_at(offsets[q]) for q in pairs[pair]]

        def expert(i, carry):
            e = e0 + i
            act = dot_f32(h[...].reshape(2 * rows, d_model), vgu[e])
            inner = (jax.nn.gelu(act[:, :cols]) * act[:, cols:]).astype(jnp.bfloat16).astype(jnp.float32)
            e_f = e.astype(jnp.float32)
            r0, r1 = routes(t, chips_of)
            us[0] = jnp.where(r0.astype(jnp.float32) == e_f, inner, us[0])
            us[1] = jnp.where(r1.astype(jnp.float32) == e_f, inner, us[1])
            return carry

        with jax.named_scope('up'):
            lax.fori_loop(0, cnt, expert, 0)

    def emit(t, pair):
        for s, q in enumerate(pairs[pair]):
            chip = place.chip_at(offsets[q])
            for i in range(2):
                u_all[t, chip, me, :, pl.ds(i * cols, cols)] = us[i, s * rows:(s + 1) * rows].astype(jnp.bfloat16)
            if t == steps - 1:
                gather = Gather(wires, ('u', t, q), lambda owner, q=q: u_all.at[t, u_owner_chip(owner, q), owner],
                                lambda owner, side, q=q: u_all.at[t, u_owner_chip(owner, q), owner, pl.ds(side * seq, seq), :])
                gather.start(u_all.at[t, chip, me])
                u_gathers[t].append(gather)
        if t < steps - 1 and pair == 1:
            gather = Gather(wires, ('u', t), lambda owner: u_all.at[t, :, owner],
                            lambda owner, side: u_all.at[t, pl.ds(side * (chips // 2), chips // 2), owner])
            gather.start(u_all.at[t, :, me])
            u_gathers[t].append(gather)

    def chunk_near(t):
        h_gathers[t].near_in(0)
        h_gathers[t].near_in(1)
        if t + 1 < steps:
            h_gathers[t + 1].start(xg.at[t + 1, me])

    def load_experts(e0):
        loads = []
        for i in range(half):
            desc = pltpu.make_async_copy(wgu.at[e0 + i], vgu.at[e0 + i], w_sems.at[i])
            desc.start()
            loads.append(desc)
        return loads

    def phase_a(t):
        gather = h_gathers[t]
        mine_loads = []
        if t == 0:
            with jax.named_scope('mine_in'):
                moving.finish_near('gu')
                mine_loads = load_experts(moving.mine)
        with jax.named_scope('near'):
            gather.sib_own()
            chunk_near(t)
            gather.sib_near(0)
            loads = begin(t, 0)
        if t > 0:
            u_near(t - 1)
        prepare(t, 0, loads)
        if t == 0:
            for desc in mine_loads:
                desc.wait()
            up_part(t, 0, moving.mine, half)
            with jax.named_scope('d_relay'):
                moving.second_leg(0, ('d',))
                moving.second_leg(1, ('d',))
            with jax.named_scope('theirs_in'):
                moving.finish_twin('gu')
                theirs_loads = load_experts(moving.theirs)
                moving.direct_in(0, ('d',))
                moving.direct_in(1, ('d',))
                for desc in theirs_loads:
                    desc.wait()
            up_part(t, 0, moving.theirs, half)
        else:
            up_part(t, 0, 0, experts)
        emit(t, 0)
        with jax.named_scope('far'):
            gather.sib_near(1)
            gather.far_in()
            gather.sib_far()
            loads = begin(t, 1)
        prepare(t, 1, loads)
        if t == 0:
            with jax.named_scope('d_far'):
                moving.far_in(('d',))
        up_part(t, 1, 0, experts)
        emit(t, 1)

    def u_near(t):
        with jax.named_scope('u_near'):
            for gather in u_gathers[t]:
                gather.near_in(0)
                gather.near_in(1)

    def phase_b(t):
        if t == 0:
            with jax.named_scope('d_in'):
                moving.finish_near('d')
                moving.finish_twin('d')
                d_load = pltpu.make_async_copy(wd, vd, w_sems.at[experts])
                d_load.start()
        with jax.named_scope('u_wait'):
            for gather in u_gathers[t]:
                gather.far_in()
                gather.sib_own()
                gather.sib_near(0)
                gather.sib_near(1)
                gather.sib_far()
        if t == 0:
            d_load.wait()
        for first in range(0, chips, 2):
            chips_of = (first, first + 1)
            acc = mbuf.at[pl.ds(first, 2)]
            acc[...] = jnp.zeros_like(acc)

            def expert(e, carry):
                e_b = e.astype(jnp.bfloat16)
                r0, r1 = routes(t, chips_of)
                m0, m1 = r0 == e_b, r1 == e_b
                zero = jnp.zeros((2 * rows, LANES), jnp.bfloat16)
                parts = []
                for j in range(n):
                    u0 = u_all[t, pl.ds(first, 2), j, :, pl.ds(0, cols)].reshape(2 * rows, cols)
                    u1 = u_all[t, pl.ds(first, 2), j, :, pl.ds(cols, cols)].reshape(2 * rows, cols)
                    parts.append(jnp.where(m0, u0, jnp.where(m1, u1, zero)))
                ue = jnp.concatenate(parts, axis=1)
                out = dot_f32(ue, vd[e])
                e_f = e.astype(jnp.float32)
                both = gates[t, pl.ds(first, 2)].reshape(2 * rows, LANES)
                gate = jnp.where(r0.astype(jnp.float32) == e_f, both[:, :1], jnp.where(r1.astype(jnp.float32) == e_f, both[:, 1:2], 0.0))
                acc[...] += (jnp.concatenate([gate] * (dcols // LANES), axis=1) * out).reshape(2, rows, dcols)
                return carry

            with jax.named_scope('down'):
                lax.fori_loop(0, experts, expert, 0)
            for chip in chips_of:
                part = mbuf[chip]
                squares = jnp.sum(part * part, axis=-1, keepdims=True)
                ss_all[t, chip, me] = jnp.transpose(jnp.broadcast_to(squares, (rows, LANES)))[:ss_all.shape[3]]
        for off, rel in others:
            region = ss_all.at[t, :, me]
            wires.send(('ss', t, off, rel), region, region, wg=place.at(off, rel))

    y_open = []

    def phase_c(t):
        loads = []
        for q in range(4):
            chip = place.chip_at(offsets[q])
            desc = pltpu.make_async_copy(xg.at[t, pl.ds(2 * chip, 2), :, own_cols], xcols.at[q], x_sems.at[q])
            desc.start()
            loads.append(desc)
        gain_out = small[pl.ds(experts + 3, 1), :].astype(jnp.float32)
        with jax.named_scope('ss_wait'):
            for off, rel in others:
                wires.recv(('ss', t, off, rel), ss_all.at[t, :, place.at(-off, rel)])
        for q in range(4):
            chip = place.chip_at(offsets[q])
            loads[q].wait()
            with jax.named_scope('y'):
                total = ss_all[t, chip, 0]
                for j in range(1, n):
                    total += ss_all[t, chip, j]
                line = jnp.broadcast_to(total[:1], (LANES, rows))
                scale = lax.rsqrt(jnp.transpose(line) * (1.0 / d_model) + NORM_EPS)
                scale = jnp.concatenate([scale] * (dcols // LANES), axis=1)
                x1 = xcols[q].reshape(rows, dcols).astype(jnp.float32)
                ybuf[t, q] = (x1 + mbuf[chip] * scale * gain_out).astype(jnp.bfloat16).reshape(2, seq, dcols)
            dst = y_out.at[t, :, own_cols]
            for rel in (0, 1):
                part = ybuf.at[t, q, (place.core + rel) % 2]
                if q == 0 and rel == 0:
                    desc = pltpu.make_async_copy(part, dst, out_sems.at[t])
                    desc.start()
                    y_open.append(desc)
                elif q < 3:
                    wires.send(('y', t, q, rel), part, dst, wg=place.at(offsets[q], rel))
                else:
                    wires.send(('y1', t, rel), part, relay_y.at[t, rel], wg=place.at(DIRS[rel], 0))

    def y_cols(src):
        return pl.ds(pl.multiple_of(src * dcols, LANES), dcols)

    def y_relay(t):
        for rel, d in enumerate(DIRS):
            wires.recv(('y1', t, rel), relay_y.at[t, rel])
            wires.send(('y2', t, rel), relay_y.at[t, rel], y_out.at[t, :, y_cols(place.at(-d, 0))], wg=place.at(d, rel))

    def y_in(t):
        for q in range(4):
            for rel in (0, 1):
                if q == 0 and rel == 0:
                    continue
                wires.recv(('y', t, q, rel) if q < 3 else ('y2', t, rel), y_out.at[t, :, y_cols(place.at(-offsets[q], rel))])

    phase_a(0)
    for t in range(1, steps):
        phase_a(t)
        if t > 1:
            phase_c(t - 2)
        phase_b(t - 1)
        if t == steps - 1:
            u_near(t)
    phase_c(steps - 2)
    for t in range(steps - 2):
        y_relay(t)
    phase_b(steps - 1)
    y_relay(steps - 2)
    phase_c(steps - 1)
    y_relay(steps - 1)
    with jax.named_scope('y_in'):
        for t in range(steps):
            y_in(t)
        for desc in y_open:
            desc.wait()
        wires.finish()


def layer_kernel(n, experts, small, mask, cos_t, sin_t, hidden, wq, wk, wv, wo, gate, up, down,
                 k_out, v_out, small_all, y_out, gq, gk, gv, go, wgu, wd, relay_gu, relay_d, xg, relay_y,
                 u_all, vd, ss_all, send_sems, recv_sems, loc_sems):
    place = Place(n)
    wires = Wires(place, send_sems, recv_sems)
    me = place.me
    prompts, seq = mask.shape[0], mask.shape[1]
    rows, d_model = hidden.shape
    cols, dcols = gate.shape[2] // n, down.shape[2] // n
    q_dim, kv_dim = wq.shape[1], wk.shape[1]
    bf16, f32 = jnp.bfloat16, jnp.float32

    enter(place)
    gather_q = PairGather(wires, 'q', wq, gq, 0)
    gather_k = PairGather(wires, 'k', wk, gk, 1)
    gather_v = PairGather(wires, 'v', wv, gv, 1)
    gather_o = PairGather(wires, 'o', wo, go, 1)
    moving = Reshard(wires, gate, up, down, wgu, wd, relay_gu, relay_d, loc_sems)
    gather_q.start()
    others = [(off, rel) for off in (0, 1, -1, 2) for rel in (0, 1)][1:]
    for off, rel in others:
        wires.send(('small', off, rel), small, small_all.at[me], wg=place.at(off, rel))
    gather_k.start()
    gather_v.start()
    small_all[me] = small[...]
    for off, rel in others:
        wires.recv(('small', off, rel), small_all.at[place.at(-off, rel)])

    def gain(i):
        return jnp.concatenate([small_all[j, pl.ds(experts + i, 1), :] for j in range(n)], axis=1).astype(jnp.float32)

    def norm(values):
        return values * lax.rsqrt(jnp.mean(values * values, axis=-1, keepdims=True) + NORM_EPS)

    h_gathers = [Gather(wires, ('h', t), lambda owner, t=t: xg.at[t, owner],
                        lambda owner, side, t=t: xg.at[t, owner, pl.ds(side * (seq // 2), seq // 2), :]) for t in range(prompts)]
    pl.run_scoped(
        functools.partial(attention_phase, n, place, small_all, mask, cos_t, sin_t, hidden, (wq, wk, wv, wo), (gq, gk, gv, go),
                          (gather_q, gather_k, gather_v, gather_o), moving, gain, norm, k_out, v_out, xg, loc_sems),
        pltpu.VMEM((rows, d_model), bf16),
        pltpu.VMEM((rows, d_model), bf16),
        pltpu.VMEM((rows, q_dim + 2 * kv_dim), f32),
        pltpu.VMEM((rows, q_dim), bf16),
        pltpu.VMEM((2, wq.shape[0], q_dim + 2 * kv_dim), bf16),
        pltpu.SemaphoreType.DMA((2, 3)),
        pltpu.SemaphoreType.DMA((prompts + 1,)),
    )
    h_gathers[0].start(xg.at[0, me])
    with jax.named_scope('services'):
        moving.first_leg(0, 'd')
        moving.first_leg(1, 'd')
        moving.direct_in(1, ('gu',))
    pl.run_scoped(
        functools.partial(moe_phase, n, experts, wires, moving, h_gathers, small, small_all, gain, norm, wgu, wd, xg, y_out, relay_y,
                          u_all, vd, ss_all),
        pltpu.VMEM((experts, d_model, 2 * cols), bf16),
        pltpu.VMEM((2, 4, seq, d_model), bf16),
        pltpu.VMEM((prompts, n // 2, 2 * seq, LANES), f32),
        pltpu.VMEM((2, 4 * seq, cols), f32),
        pltpu.VMEM((4, 2 * seq, dcols), f32),
        pltpu.VMEM((prompts, 4, 2, seq, dcols), bf16),
        pltpu.VMEM((4, 2, seq, dcols), bf16),
        pltpu.VMEM((prompts, n, 2, seq, LANES), bf16),
        pltpu.VMEM((small.shape[0], d_model), bf16),
        pltpu.VMEM((1, d_model), f32),
        pltpu.SemaphoreType.DMA((2, 2)),
        pltpu.SemaphoreType.DMA((experts + 1,)),
        pltpu.SemaphoreType.DMA((4,)),
        pltpu.SemaphoreType.DMA((prompts,)),
    )


def layer(n, experts, prompts, small, mask, cos_t, sin_t, hidden, wq, wk, wv, wo, gate, up, down):
    rows, d_model = hidden.shape
    seq = rows // prompts
    ff = gate.shape[2]
    drows = down.shape[1]
    cols, dcols = ff // n, d_model // n
    bf16, f32 = jnp.bfloat16, jnp.float32
    quarter = experts // 4

    def full(w):
        return jax.ShapeDtypeStruct((n,) + w.shape, bf16)

    outs = pl.pallas_call(
        functools.partial(layer_kernel, n, experts),
        name='layer',
        out_shape=(
            jax.ShapeDtypeStruct((rows, wk.shape[1]), bf16),
            jax.ShapeDtypeStruct((rows, wv.shape[1]), bf16),
            full(small),
            jax.ShapeDtypeStruct((prompts, seq, d_model), bf16),
            full(wq), full(wk), full(wv), full(wo),
            jax.ShapeDtypeStruct((experts, d_model, 2 * cols), bf16),
            jax.ShapeDtypeStruct((experts, ff, dcols), bf16),
            jax.ShapeDtypeStruct((2, 2, quarter, gate.shape[1], 2 * cols), bf16),
            jax.ShapeDtypeStruct((2, 2, quarter, drows, dcols), bf16),
            jax.ShapeDtypeStruct((prompts, n, seq, d_model), bf16),
            jax.ShapeDtypeStruct((prompts, 2, seq, dcols), bf16),
        ),
        in_specs=[VMEM_FULL] * 4 + [ANY] * 8,
        out_specs=(VMEM_FULL,) * 3 + (ANY,) * 11,
        scratch_shapes=[
            pltpu.VMEM((prompts, n // 2, n, 2 * seq, 2 * cols), bf16),
            pltpu.VMEM((experts, ff, dcols), bf16),
            pltpu.VMEM((prompts, n // 2, n, 8, 2 * seq), f32),
            pltpu.SemaphoreType.DMA((416,)),
            pltpu.SemaphoreType.DMA((416,)),
            pltpu.SemaphoreType.DMA((4,)),
        ],
        compiler_params=pltpu.CompilerParams(collective_id=0, has_side_effects=True, vmem_limit_bytes=67_000_000),
        cost_estimate=pl.CostEstimate(flops=110_000_000_000, bytes_accessed=400_000_000, transcendentals=0),
    )(small, mask, cos_t, sin_t, hidden, wq, wk, wv, wo, gate, up, down)
    return outs[3], outs[0], outs[1]


def solution(mesh):
    n = mesh.shape['wg']
    row_spec = P(('dp', 'wg'))
    dim0_spec = P('wg', None)
    dim1_spec = P(None, 'wg', None)

    def device_fn(hidden, seq_lens, route_idx, g_attn_in, w_query, w_key, w_value, w_attn_out, g_attn_out, g_moe_in, w_router, w_gate, w_up, w_down, g_moe_out):
        n_prompts, seq_len, d_model = hidden.shape
        experts = w_router.shape[1]
        rows = n_prompts * seq_len
        depth = w_query.shape[0]
        routes = jnp.pad(route_idx.T.astype(jnp.bfloat16), ((0, 0), (0, depth - rows)))
        small = jnp.concatenate([w_router.T] + [g[None] for g in (g_attn_in, g_attn_out, g_moe_in, g_moe_out)] + [routes], axis=0)
        small = jnp.pad(small, ((0, -small.shape[0] % 16), (0, 0)))
        pos = jnp.arange(seq_len)
        mask = ((pos[None, None, :] <= pos[None, :, None]) & (pos[None, None, :] < seq_lens[:, None, None])).astype(jnp.float32)
        cos_t, sin_t = rope_tables(seq_len)
        tok_rows = hidden.reshape(rows, d_model)
        y_out, k_rope, v_rows = layer(
            n, experts, n_prompts, small, mask, cos_t, sin_t, tok_rows, w_query, w_key, w_value, w_attn_out, w_gate, w_up, w_down)
        cache = (n_prompts, seq_len, w_key.shape[1] // HEAD_DIM, HEAD_DIM)
        return y_out, k_rope.reshape(cache), v_rows.reshape(cache)

    return jax.shard_map(
        device_fn,
        mesh=mesh,
        in_specs=(row_spec, row_spec, row_spec, P('wg'), dim0_spec, dim0_spec, dim0_spec, dim0_spec, P('wg'), P('wg'), dim0_spec, dim1_spec, dim1_spec, dim1_spec, P('wg')),
        out_specs=(row_spec, row_spec, row_spec),
        check_vma=False,
    )
```

```python
import functools
import jax
import jax.numpy as jnp
from jax import lax
from jax.experimental import pallas as pl
from jax.experimental.pallas import tpu as pltpu
from jax.sharding import PartitionSpec as P

HEAD_DIM = 128
LANES = 128
SOFT_CAP = 30.0
NORM_EPS = 1e-5
ROPE_BASE = 10000.0
ATTN_SCALE = HEAD_DIM ** -0.5
MESH = pl.DeviceIdType.MESH
ANY = pl.BlockSpec(memory_space=pl.ANY)
VMEM_FULL = pl.BlockSpec(memory_space=pltpu.VMEM)
DIRS = (1, -1)


def dot_f32(left_op, right_op):
    return jnp.dot(left_op, right_op, preferred_element_type=jnp.float32)


def rms_norm(values, gain_vec):
    values_f32 = values.astype(jnp.float32)
    inv_rms = lax.rsqrt(jnp.mean(values_f32 * values_f32, axis=-1, keepdims=True) + NORM_EPS)
    return values_f32 * inv_rms * gain_vec.astype(jnp.float32)


def rope_tables(seq_len):
    half_dim = HEAD_DIM // 2
    inv_freq = ROPE_BASE ** (-jnp.arange(half_dim, dtype=jnp.float32) * (2.0 / HEAD_DIM))
    angles = jnp.arange(seq_len, dtype=jnp.float32)[:, None] * inv_freq[None, :]
    cos_t, sin_t = jnp.cos(angles), jnp.sin(angles)
    return jnp.concatenate([cos_t, cos_t], axis=1), jnp.concatenate([-sin_t, sin_t], axis=1)


class Place:
    def __init__(self, n):
        self.n = n
        self.chips = n // 2
        self.me = lax.axis_index('wg')
        self.dp = lax.axis_index('dp')
        self.chip = self.me // 2
        self.core = self.me % 2
        self.parity = self.dp % 2
        self.twin = self.dp + 1 - 2 * self.parity

    def at(self, offset, rel):
        return ((self.chip + offset + self.chips) % self.chips) * 2 + (self.core + rel) % 2

    def chip_at(self, offset):
        return (self.chip + offset + self.chips) % self.chips


def still(ref):
    if not hasattr(ref, 'transforms'):
        return ref
    out = ref.ref
    for step in ref.transforms:
        out = out.at[tuple(pl.ds(0, index.size) if hasattr(index, 'start') else pl.ds(0, 1) for index in step.indices)]
    return out


class Wires:
    def __init__(self, place, send_sems, recv_sems):
        self.place, self.send_sems, self.recv_sems = place, send_sems, recv_sems
        self.slots = {}
        self.open = []

    def copy(self, name, src, dst, wg=None, dp=None):
        slot = self.slots.setdefault(name, len(self.slots))
        return pltpu.make_async_remote_copy(
            src_ref=src, dst_ref=dst, send_sem=self.send_sems.at[slot], recv_sem=self.recv_sems.at[slot],
            device_id={'dp': self.place.dp if dp is None else dp, 'wg': self.place.me if wg is None else wg},
            device_id_type=MESH)

    def send(self, name, src, dst, wg=None, dp=None):
        desc = self.copy(name, src, dst, wg, dp)
        desc.start()
        self.open.append((name, still(src)))

    def recv(self, name, dst):
        self.copy(name, dst, dst).wait_recv()

    def finish(self):
        for name, src in self.open:
            self.copy(name, src, src).wait_send()
        self.open = []


def enter(place):
    barrier = pltpu.get_barrier_semaphore()
    peers = [(place.dp, place.at(off, rel)) for off in (1, -1, 2) for rel in (0, 1)] + [(place.dp, place.at(0, 1))]
    peers.append((place.twin, place.me))
    for dp, wg in peers:
        pl.semaphore_signal(barrier, inc=1, device_id={'dp': dp, 'wg': wg}, device_id_type=MESH)
    pl.semaphore_wait(barrier, len(peers))


class Reshard:
    def __init__(self, wires, gate, up, down, wgu, wd, relay_gu, relay_d, loc_sems):
        self.wires, self.place = wires, wires.place
        n = self.place.n
        self.gate, self.up, self.down, self.wgu, self.wd = gate, up, down, wgu, wd
        self.relay_gu, self.relay_d, self.loc_sems = relay_gu, relay_d, loc_sems
        self.experts, self.rows, self.cols = gate.shape[0], gate.shape[1], gate.shape[2] // n
        self.drows, self.dcols = down.shape[1], down.shape[2] // n
        self.half, self.quarter = self.experts // 2, self.experts // 4
        self.mine = self.place.parity * self.half
        self.theirs = self.half - self.mine

    def piece(self, arr, e0, cnt, j):
        if arr == 'd':
            return self.down.at[pl.ds(e0, cnt), :, pl.ds(pl.multiple_of(j * self.dcols, LANES), self.dcols)]
        ref = self.gate if arr == 'g' else self.up
        return ref.at[pl.ds(e0, cnt), :, pl.ds(pl.multiple_of(j * self.cols, LANES), self.cols)]

    def land(self, arr, e0, cnt, src):
        if arr == 'd':
            return self.wd.at[pl.ds(e0, cnt), pl.ds(pl.multiple_of(src * self.drows, self.drows), self.drows), :]
        row = pl.ds(pl.multiple_of(src * self.rows, self.rows), self.rows)
        if arr == 'gu':
            return self.wgu.at[pl.ds(e0, cnt), row, :]
        return self.wgu.at[pl.ds(e0, cnt), row, pl.ds(0 if arr == 'g' else self.cols, self.cols)]

    def relay(self, arr, side, rel):
        if arr == 'd':
            return self.relay_d.at[side, rel]
        if arr == 'gu':
            return self.relay_gu.at[side, rel]
        return self.relay_gu.at[side, rel, :, :, pl.ds(0 if arr == 'g' else self.cols, self.cols)]

    def near(self):
        me, sib = self.place.me, self.place.at(0, 1)
        for i, arr in enumerate('gud'):
            self.wires.send(('sib', arr), self.piece(arr, 0, self.experts, sib), self.land(arr, 0, self.experts, me), wg=sib)
            self.own(i, arr).start()

    def own(self, i, arr):
        me = self.place.me
        return pltpu.make_async_copy(self.piece(arr, 0, self.experts, me), self.land(arr, 0, self.experts, me), self.loc_sems.at[i])

    def direct(self, rel, arrs):
        for arr in arrs:
            for d in DIRS:
                to = self.place.at(d, rel)
                self.wires.send(('direct', d, rel, arr), self.piece(arr, self.mine, self.half, to),
                                self.land(arr, self.mine, self.half, self.place.me), wg=to)

    def first_leg(self, rel, arrs):
        for arr in arrs:
            for side, d in enumerate(DIRS):
                e0 = self.mine + side * self.quarter
                self.wires.send(('leg1', d, rel, arr), self.piece(arr, e0, self.quarter, self.place.at(2 * d, rel)),
                                self.relay(arr, side, rel), wg=self.place.at(d, 0))

    def to_twin(self, name, arr, e0, cnt, src):
        region = self.land(arr, e0, cnt, src)
        self.wires.send(name, region, region, dp=self.place.twin)

    def direct_in(self, rel, arrs):
        for arr in arrs:
            for d in DIRS:
                src = self.place.at(-d, rel)
                for part in arr:
                    self.wires.recv(('direct', d, rel, part), self.land(part, self.mine, self.half, src))
                self.to_twin(('twin', d, rel, arr), arr, self.mine, self.half, src)

    def second_leg(self, rel, arrs):
        for arr in arrs:
            for side, d in enumerate(DIRS):
                for part in arr:
                    self.wires.recv(('leg1', d, rel, part), self.relay(part, side, rel))
                self.wires.send(('leg2', d, rel, arr), self.relay(arr, side, rel),
                                self.land(arr, self.mine + side * self.quarter, self.quarter, self.place.at(-d, 0)),
                                wg=self.place.at(d, rel))

    def far_in(self, arrs):
        for arr in arrs:
            for rel in (0, 1):
                for side, d in enumerate(DIRS):
                    src = self.place.at(2 * d, rel)
                    e0 = self.mine + side * self.quarter
                    self.wires.recv(('leg2', d, rel, arr), self.land(arr, e0, self.quarter, src))
                    self.to_twin(('twin2', d, rel, arr), arr, e0, self.quarter, src)

    def finish_near(self, arr):
        for part in arr:
            self.wires.recv(('sib', part), self.land(part, 0, self.experts, self.place.at(0, 1)))
            self.own('gud'.index(part), part).wait()

    def finish_twin(self, arr):
        for rel in (0, 1):
            for side, d in enumerate(DIRS):
                self.wires.recv(('twin', d, rel, arr), self.land(arr, self.theirs, self.half, self.place.at(-d, rel)))
                self.wires.recv(('twin2', d, rel, arr),
                                self.land(arr, self.theirs + side * self.quarter, self.quarter, self.place.at(2 * d, rel)))


class PairGather:
    def __init__(self, wires, name, src, dst, give_side):
        self.wires, self.place, self.name, self.src, self.dst = wires, wires.place, name, src, dst
        rows = src.shape[0]
        given = rows // 4
        parity = self.place.parity
        last = rows - given
        self.spans = {'give': (parity * last, given), 'both': (given, rows - 2 * given), 'take': (last - parity * last, given)}
        self.far_side = {'give': give_side, 'both': 1 - give_side}

    def part(self, owner, what):
        row, cnt = self.spans[what]
        return self.dst.at[owner, pl.ds(pl.multiple_of(row, 16), cnt), :]

    def start(self):
        place, me = self.place, self.place.me
        for what in ('give', 'both'):
            row, cnt = self.spans[what]
            own = self.src.at[pl.ds(pl.multiple_of(row, 16), cnt), :]
            for d in DIRS:
                self.wires.send((self.name, 'own', what, d), own, self.part(me, what), wg=place.at(d, 0))
        self.wires.send((self.name, 'sib'), self.src, self.dst.at[me], wg=place.at(0, 1))

    def give(self, tag, owner):
        part = self.part(owner, 'give')
        self.wires.send((self.name, 'give', tag), part, part, dp=self.place.twin)

    def near_in(self, *whats):
        place = self.place
        for what in whats:
            for side, d in enumerate(DIRS):
                owner = place.at(-d, 0)
                part = self.part(owner, what)
                self.wires.recv((self.name, 'own', what, d), part)
                if what == 'give':
                    self.give(d, owner)
                if self.far_side[what] == side:
                    self.wires.send((self.name, 'far', what), part, part, wg=place.at(d, 0))
                self.wires.send((self.name, 'across', what, d), part, part, wg=place.at(0, 1))

    def far_in(self, *whats):
        place = self.place
        owner = place.at(2, 0)
        for what in whats:
            part = self.part(owner, what)
            self.wires.recv((self.name, 'far', what), part)
            if what == 'give':
                self.give(2, owner)
            self.wires.send((self.name, 'across', what, 2), part, part, wg=place.at(0, 1))

    def twin_in(self, *tags):
        for tag in tags:
            part = self.part(self.place.at(-tag, 0), 'take')
            self.wires.recv((self.name, 'give', tag), part)
            self.wires.send((self.name, 'across', 'take', tag), part, part, wg=self.place.at(0, 1))

    def sib_in(self):
        place = self.place
        self.wires.recv((self.name, 'sib'), self.dst.at[place.at(0, 1)])
        for tag in (1, -1, 2):
            for what in ('give', 'both', 'take'):
                self.wires.recv((self.name, 'across', what, tag), self.part(place.at(-tag, 1), what))


class Gather:
    def __init__(self, wires, name, region, half_region):
        self.wires, self.place, self.name = wires, wires.place, name
        self.region, self.half_region = region, half_region

    def start(self, src):
        place, dst = self.place, self.region(self.place.me)
        for d in DIRS:
            self.wires.send((self.name, 'own', d), src, dst, wg=place.at(d, 0))
        self.wires.send((self.name, 'own', 0), src, dst, wg=place.at(0, 1))

    def near_in(self, side):
        d, place = DIRS[side], self.place
        owner = place.at(-d, 0)
        block, part = self.region(owner), self.half_region(owner, side)
        self.wires.recv((self.name, 'own', d), block)
        self.wires.send((self.name, 'far', d), part, part, wg=place.at(d, 0))
        self.wires.send((self.name, 'across', d), block, block, wg=place.at(0, 1))

    def far_in(self):
        place = self.place
        owner = place.at(2, 0)
        for side, d in enumerate(DIRS):
            part = self.half_region(owner, side)
            self.wires.recv((self.name, 'far', d), part)
            self.wires.send((self.name, 'across2', d), part, part, wg=place.at(0, 1))

    def sib_own(self):
        self.wires.recv((self.name, 'own', 0), self.region(self.place.at(0, 1)))

    def sib_near(self, side):
        self.wires.recv((self.name, 'across', DIRS[side]), self.region(self.place.at(-DIRS[side], 1)))

    def sib_far(self):
        for side, d in enumerate(DIRS):
            self.wires.recv((self.name, 'across2', d), self.half_region(self.place.at(2, 1), side))


def attention_phase(n, place, small_all, mask, cos_t, sin_t, hidden_hbm, weights, gathered, gathers, moving, gain, norm, k_out, v_out,
                    xg, loc_sems, hidden, h, acc, ctx, wbuf, load_sems, x_sems):
    wq, wk, wv, wo = weights
    gq, gk, gv, go = gathered
    gather_q, gather_k, gather_v, gather_o = gathers
    me = place.me
    prompts, seq = mask.shape[0], mask.shape[1]
    rows, d_model = hidden.shape
    depth = wq.shape[0]
    q_dim, kv_dim = wq.shape[1], wk.shape[1]
    n_kv = kv_dim // HEAD_DIM
    group = q_dim // kv_dim
    tile = 512
    load = pltpu.make_async_copy(hidden_hbm, hidden, x_sems.at[prompts])
    load.start()
    load.wait()

    def norm_in(i, carry):
        r = pl.ds(pl.multiple_of(i * 16, 16), 16)
        h[r, :] = (norm(hidden[r, :].astype(jnp.float32)) * gain(0)).astype(jnp.bfloat16)
        return carry

    with jax.named_scope('norm_in'):
        lax.fori_loop(0, rows // 16, norm_in, 0)
        acc[...] = jnp.zeros_like(acc)

    with jax.named_scope('near'):
        gather_q.near_in('give', 'both')
        gather_k.near_in('give', 'both')
        gather_v.near_in('give', 'both')
        gather_o.start()
        moving.direct(0, 'gu')
        moving.near()
    with jax.named_scope('qkv_far'):
        gather_q.twin_in(1, -1)
        gather_k.twin_in(1, -1)
        gather_v.twin_in(1, -1)
        gather_q.far_in('give', 'both')
        gather_k.far_in('give', 'both')
        gather_v.far_in('give', 'both')
    with jax.named_scope('qkv_last'):
        gather_q.twin_in(2)
        gather_k.twin_in(2)
        gather_v.twin_in(2)
        gather_q.sib_in()
        gather_k.sib_in()
        gather_v.sib_in()
    with jax.named_scope('o_near_give'):
        gather_o.near_in('give')

    def owner_of(i):
        return (me + i) % n

    def product(lhs, weights, first_col):
        def loads(i, slot):
            owner = owner_of(i)

            def start(own):
                col = 0
                for w, (src, gathered) in enumerate(weights):
                    width = src.shape[1]
                    pltpu.make_async_copy(src if own else gathered.at[owner], wbuf.at[slot, :, pl.ds(col, width)],
                                          load_sems.at[slot, w]).start()
                    col += width

            @pl.when(i == 0)
            def _():
                start(True)

            @pl.when(i > 0)
            def _():
                start(False)

        def step(i, carry):
            slot = i % 2
            owner = owner_of(i)

            @pl.when(i + 1 < n)
            def _():
                loads(i + 1, 1 - slot)

            col = 0
            for w, (src, gathered) in enumerate(weights):
                width = src.shape[1]
                pltpu.make_async_copy(gathered.at[owner], wbuf.at[slot, :, pl.ds(col, width)], load_sems.at[slot, w]).wait()
                col += width

            def tiles(j, carry):
                c = pl.ds(pl.multiple_of(j * tile, tile), tile)
                acc[:, c] += dot_f32(lhs[:, pl.ds(pl.multiple_of(owner * depth, depth), depth)], wbuf[slot, :, c])
                return carry

            return lax.fori_loop(0, col // tile, tiles, carry)

        loads(0, 0)
        lax.fori_loop(0, n, step, 0)

    with jax.named_scope('qkv_mm'):
        product(h, ((wq, gq), (wk, gk), (wv, gv)), 0)

    def rope(values):
        values = values.astype(jnp.bfloat16).astype(jnp.float32)
        cos_v, sin_v = cos_t[...], sin_t[...]
        times = values.shape[0] // seq
        if times > 1:
            cos_v, sin_v = jnp.concatenate([cos_v] * times, axis=0), jnp.concatenate([sin_v] * times, axis=0)
        return (values * cos_v + pltpu.roll(values, HEAD_DIM // 2, 1) * sin_v).astype(jnp.bfloat16)

    def attend(i, carry):
        p, g = i // n_kv, i % n_kv
        r = pl.ds(pl.multiple_of(p * seq, seq), seq)
        kv_cols = pl.ds(pl.multiple_of(g * HEAD_DIM, HEAD_DIM), HEAD_DIM)
        q = jnp.concatenate([acc[r, pl.ds(pl.multiple_of((g * group + j) * HEAD_DIM, HEAD_DIM), HEAD_DIM)]
                             for j in range(group)], axis=0)
        q = rope(q)
        k = rope(acc[r, pl.ds(pl.multiple_of(q_dim + g * HEAD_DIM, HEAD_DIM), HEAD_DIM)])
        v = acc[r, pl.ds(pl.multiple_of(q_dim + kv_dim + g * HEAD_DIM, HEAD_DIM), HEAD_DIM)].astype(jnp.bfloat16)
        k_out[r, kv_cols] = k
        v_out[r, kv_cols] = v
        scores = lax.dot_general(q, k, (((1,), (1,)), ((), ())), preferred_element_type=jnp.float32) * ATTN_SCALE
        scores = SOFT_CAP * jnp.tanh(scores / SOFT_CAP)
        allowed = jnp.concatenate([mask[p]] * group, axis=0) > 0.5
        scores = jnp.where(allowed, scores, -1e30)
        ex = jnp.exp(scores - jnp.max(scores, axis=-1, keepdims=True))
        probs = (ex / jnp.sum(ex, axis=-1, keepdims=True)).astype(jnp.bfloat16)
        out = dot_f32(probs, v).astype(jnp.bfloat16)
        for j in range(group):
            ctx[r, pl.ds(pl.multiple_of((g * group + j) * HEAD_DIM, HEAD_DIM), HEAD_DIM)] = out[j * seq:(j + 1) * seq]
        return carry

    with jax.named_scope('attend'):
        lax.fori_loop(0, prompts * n_kv, attend, 0)

    with jax.named_scope('o_near_both'):
        gather_o.near_in('both')
        moving.first_leg(0, 'gu')
        moving.first_leg(1, 'gu')
        moving.direct(1, 'gu')
    with jax.named_scope('o_twin'):
        gather_o.twin_in(1, -1)
    with jax.named_scope('direct_in0'):
        moving.direct_in(0, ('gu',))
    with jax.named_scope('o_far'):
        gather_o.far_in('give', 'both')
    with jax.named_scope('leg2'):
        moving.second_leg(0, ('gu',))
        moving.second_leg(1, ('gu',))
    with jax.named_scope('o_last'):
        gather_o.twin_in(2)
        gather_o.sib_in()
    with jax.named_scope('direct_in1'):
        moving.direct_in(1, ('gu',))
    with jax.named_scope('o_mm'):
        acc[...] = jnp.zeros_like(acc)
        product(ctx, ((wo, go),), 0)

    def finish_rows(i, carry):
        r = pl.ds(pl.multiple_of(i * 16, 16), 16)
        mid = (hidden[r, :].astype(jnp.float32) + norm(acc[r, pl.ds(0, d_model)]) * gain(1)).astype(jnp.bfloat16)
        ctx[r, :] = mid
        return carry

    with jax.named_scope('finish_rows'):
        lax.fori_loop(0, rows // 16, finish_rows, 0)
    stores = []
    for t in range(prompts):
        desc = pltpu.make_async_copy(ctx.at[pl.ds(t * seq, seq), :], xg.at[t, me], x_sems.at[t])
        desc.start()
        stores.append(desc)
    for desc in stores:
        desc.wait()


def moe_phase(n, experts, wires, moving, h_gathers, small, small_all, gain, norm, wgu, wd, xg, y_out, relay_y, u_all, vd, ss_all,
              vgu, hbuf, gates, us, mbuf, ybuf, xcols, route, router, gain_in, load_sems, w_sems, x_sems, out_sems):
    place = wires.place
    steps, seq, d_model = route.shape[0], route.shape[3], hbuf.shape[3]
    chips, me = place.chips, place.me
    rows = 2 * seq
    depth = small.shape[1]
    cols = vgu.shape[2] // 2
    dcols = vd.shape[2]
    offsets = (0, -1, 1, 2)

    with jax.named_scope('tables'):
        gain_in[...] = gain(2)
        for j in range(n):
            router[:, pl.ds(j * depth, depth)] = small_all[j]

        def route_of(j, carry):
            for t in range(steps):
                for i in range(2):
                    line = small_all[j, pl.ds(experts + 4 + i, 1), pl.ds(t * seq, seq)].astype(jnp.float32)
                    route[t, j, i] = jnp.transpose(jnp.broadcast_to(line, (LANES, seq))).astype(jnp.bfloat16)
            return carry

        lax.fori_loop(0, n, route_of, 0)

    own_cols = pl.ds(pl.multiple_of(me * dcols, LANES), dcols)
    half = experts // 2

    def u_owner_chip(owner, q):
        return (owner // 2 + offsets[q] + chips) % chips

    u_gathers = {t: [] for t in range(steps)}
    others = [(off, rel) for off in (0, 1, -1, 2) for rel in (0, 1)][1:]

    pairs = ((0, 1), (2, 3))

    def begin(t, pair):
        loads = []
        for s, q in enumerate(pairs[pair]):
            chip = place.chip_at(offsets[q])
            desc = pltpu.make_async_copy(xg.at[t, pl.ds(2 * chip, 2)], hbuf.at[pair, pl.ds(2 * s, 2)], load_sems.at[pair, s])
            desc.start()
            loads.append(desc)
        return loads

    def routes(t, chips_of):
        def one(i):
            return jnp.concatenate([route[t, pl.ds(2 * chip, 2), i].reshape(rows, LANES) for chip in chips_of], axis=0)

        return one(0), one(1)

    def prepare(t, pair, loads):
        with jax.named_scope('load'):
            for desc in loads:
                desc.wait()
        h = hbuf.at[pair]

        def norm_rows(i, carry):
            r = pl.ds(pl.multiple_of(i % (seq // 32) * 32, 32), 32)
            x = h[i // (seq // 32), r, :].astype(jnp.float32)
            h[i // (seq // 32), r, :] = (norm(x) * gain_in[...]).astype(jnp.bfloat16)
            return carry

        with jax.named_scope('norm'):
            lax.fori_loop(0, 2 * rows // 32, norm_rows, 0)
        logits = lax.dot_general(h[...].reshape(2 * rows, d_model), router[...], (((1,), (1,)), ((), ())),
                                 preferred_element_type=jnp.float32)
        lane = lax.broadcasted_iota(jnp.int32, logits.shape, 1)
        logits = jnp.where(lane < experts, logits, -1e30)
        peak = jnp.max(logits, axis=-1, keepdims=True)
        ex = jnp.where(lane < experts, jnp.exp(logits - peak), 0.0)
        probs = ex / jnp.sum(ex, axis=-1, keepdims=True)
        lane_f = lane.astype(jnp.float32)
        chips_of = [place.chip_at(offsets[q]) for q in pairs[pair]]
        g0, g1 = (jnp.sum(jnp.where(lane_f == r[:, :logits.shape[1]].astype(jnp.float32), probs, 0.0), axis=-1, keepdims=True)
                  for r in routes(t, chips_of))
        both = jnp.where(lax.broadcasted_iota(jnp.int32, (2 * rows, LANES), 1) == 0, g0, g1)
        for s, chip in enumerate(chips_of):
            gates[t, chip] = both[s * rows:(s + 1) * rows]
        us[pair] = jnp.zeros(us.shape[1:], jnp.float32)

    def up_part(t, pair, e0, cnt):
        h = hbuf.at[pair]
        chips_of = [place.chip_at(offsets[q]) for q in pairs[pair]]

        def expert(i, carry):
            e = e0 + i
            act = dot_f32(h[...].reshape(2 * rows, d_model), vgu[e])
            inner = (jax.nn.gelu(act[:, :cols]) * act[:, cols:]).astype(jnp.bfloat16).astype(jnp.float32)
            e_f = e.astype(jnp.float32)
            r0, r1 = routes(t, chips_of)
            us[pair, 0] = jnp.where(r0.astype(jnp.float32) == e_f, inner, us[pair, 0])
            us[pair, 1] = jnp.where(r1.astype(jnp.float32) == e_f, inner, us[pair, 1])
            return carry

        with jax.named_scope('up'):
            lax.fori_loop(0, cnt, expert, 0)

    def emit(t, pair):
        for s, q in enumerate(pairs[pair]):
            chip = place.chip_at(offsets[q])
            for i in range(2):
                u_all[t, chip, me, :, pl.ds(i * cols, cols)] = us[pair, i, s * rows:(s + 1) * rows].astype(jnp.bfloat16)
            if t == steps - 1:
                gather = Gather(wires, ('u', t, q), lambda owner, q=q: u_all.at[t, u_owner_chip(owner, q), owner],
                                lambda owner, side, q=q: u_all.at[t, u_owner_chip(owner, q), owner, pl.ds(side * seq, seq), :])
                gather.start(u_all.at[t, chip, me])
                u_gathers[t].append(gather)
        if t < steps - 1 and pair == 1:
            gather = Gather(wires, ('u', t), lambda owner: u_all.at[t, :, owner],
                            lambda owner, side: u_all.at[t, pl.ds(side * (chips // 2), chips // 2), owner])
            gather.start(u_all.at[t, :, me])
            u_gathers[t].append(gather)

    def chunk_near(t):
        h_gathers[t].near_in(0)
        h_gathers[t].near_in(1)
        if t == 0:
            moving.direct(0, 'd')
            moving.direct(1, 'd')
            moving.first_leg(0, 'd')
            moving.first_leg(1, 'd')
        if t + 1 < steps:
            h_gathers[t + 1].start(xg.at[t + 1, me])

    def load_experts(e0):
        loads = []
        for i in range(half):
            desc = pltpu.make_async_copy(wgu.at[e0 + i], vgu.at[e0 + i], w_sems.at[i])
            desc.start()
            loads.append(desc)
        return loads

    def phase_a(t):
        gather = h_gathers[t]
        mine_loads = []
        if t == 0:
            with jax.named_scope('mine_in'):
                moving.finish_near('gu')
                mine_loads = load_experts(moving.mine)
        with jax.named_scope('near'):
            gather.sib_own()
            chunk_near(t)
            gather.sib_near(0)
            loads = begin(t, 0)
        if t > 0:
            u_near(t - 1)
        prepare(t, 0, loads)
        if t == 0:
            for desc in mine_loads:
                desc.wait()
            up_part(t, 0, moving.mine, half)
        else:
            up_part(t, 0, 0, experts)
            emit(t, 0)
        with jax.named_scope('far'):
            gather.sib_near(1)
            gather.far_in()
            gather.sib_far()
            loads = begin(t, 1)
            if t == 1:
                moving.far_in(('d',))
        prepare(t, 1, loads)
        if t == 0:
            up_part(t, 1, moving.mine, half)
            with jax.named_scope('theirs_in'):
                moving.finish_twin('gu')
                theirs_loads = load_experts(moving.theirs)
                for desc in theirs_loads:
                    desc.wait()
            for pair in (0, 1):
                up_part(t, pair, moving.theirs, half)
                emit(t, pair)
            with jax.named_scope('d_relay'):
                moving.direct_in(0, ('d',))
                moving.direct_in(1, ('d',))
                moving.second_leg(0, ('d',))
                moving.second_leg(1, ('d',))
        else:
            up_part(t, 1, 0, experts)
            emit(t, 1)

    def u_near(t):
        with jax.named_scope('u_near'):
            for gather in u_gathers[t]:
                gather.near_in(0)
                gather.near_in(1)

    def phase_b(t):
        if t == 0:
            with jax.named_scope('d_in'):
                moving.finish_near('d')
                moving.finish_twin('d')
                d_load = pltpu.make_async_copy(wd, vd, w_sems.at[experts])
                d_load.start()
        with jax.named_scope('u_wait'):
            for gather in u_gathers[t]:
                gather.far_in()
                gather.sib_own()
                gather.sib_near(0)
                gather.sib_near(1)
                gather.sib_far()
        if t == 0:
            d_load.wait()
        for first in range(0, chips, 2):
            chips_of = (first, first + 1)
            acc = mbuf.at[pl.ds(first, 2)]
            acc[...] = jnp.zeros_like(acc)

            def expert(e, carry):
                e_b = e.astype(jnp.bfloat16)
                r0, r1 = routes(t, chips_of)
                m0, m1 = r0 == e_b, r1 == e_b
                zero = jnp.zeros((2 * rows, LANES), jnp.bfloat16)
                parts = []
                for j in range(n):
                    u0 = u_all[t, pl.ds(first, 2), j, :, pl.ds(0, cols)].reshape(2 * rows, cols)
                    u1 = u_all[t, pl.ds(first, 2), j, :, pl.ds(cols, cols)].reshape(2 * rows, cols)
                    parts.append(jnp.where(m0, u0, jnp.where(m1, u1, zero)))
                ue = jnp.concatenate(parts, axis=1)
                out = dot_f32(ue, vd[e])
                e_f = e.astype(jnp.float32)
                both = gates[t, pl.ds(first, 2)].reshape(2 * rows, LANES)
                gate = jnp.where(r0.astype(jnp.float32) == e_f, both[:, :1], jnp.where(r1.astype(jnp.float32) == e_f, both[:, 1:2], 0.0))
                acc[...] += (jnp.concatenate([gate] * (dcols // LANES), axis=1) * out).reshape(2, rows, dcols)
                return carry

            with jax.named_scope('down'):
                lax.fori_loop(0, experts, expert, 0)
            for chip in chips_of:
                part = mbuf[chip]
                squares = jnp.sum(part * part, axis=-1, keepdims=True)
                ss_all[t, chip, me] = jnp.transpose(jnp.broadcast_to(squares, (rows, LANES)))[:ss_all.shape[3]]
        for off, rel in others:
            region = ss_all.at[t, :, me]
            wires.send(('ss', t, off, rel), region, region, wg=place.at(off, rel))

    y_open = []

    def phase_c(t):
        loads = []
        for q in range(4):
            chip = place.chip_at(offsets[q])
            desc = pltpu.make_async_copy(xg.at[t, pl.ds(2 * chip, 2), :, own_cols], xcols.at[q], x_sems.at[q])
            desc.start()
            loads.append(desc)
        gain_out = small[pl.ds(experts + 3, 1), :].astype(jnp.float32)
        with jax.named_scope('ss_wait'):
            for off, rel in others:
                wires.recv(('ss', t, off, rel), ss_all.at[t, :, place.at(-off, rel)])
        for q in (3, 1, 2, 0):
            chip = place.chip_at(offsets[q])
            loads[q].wait()
            with jax.named_scope('y'):
                total = ss_all[t, chip, 0]
                for j in range(1, n):
                    total += ss_all[t, chip, j]
                line = jnp.broadcast_to(total[:1], (LANES, rows))
                scale = lax.rsqrt(jnp.transpose(line) * (1.0 / d_model) + NORM_EPS)
                scale = jnp.concatenate([scale] * (dcols // LANES), axis=1)
                x1 = xcols[q].reshape(rows, dcols).astype(jnp.float32)
                ybuf[t, q] = (x1 + mbuf[chip] * scale * gain_out).astype(jnp.bfloat16).reshape(2, seq, dcols)
            dst = y_out.at[t, :, own_cols]
            for rel in (0, 1):
                part = ybuf.at[t, q, (place.core + rel) % 2]
                if q == 0 and rel == 0:
                    desc = pltpu.make_async_copy(part, dst, out_sems.at[t])
                    desc.start()
                    y_open.append(desc)
                elif q < 3:
                    wires.send(('y', t, q, rel), part, dst, wg=place.at(offsets[q], rel))
                else:
                    wires.send(('y1', t, rel), part, relay_y.at[t, rel], wg=place.at(DIRS[rel], 0))

    def y_cols(src):
        return pl.ds(pl.multiple_of(src * dcols, LANES), dcols)

    def y_relay(t):
        for rel, d in enumerate(DIRS):
            wires.recv(('y1', t, rel), relay_y.at[t, rel])
            wires.send(('y2', t, rel), relay_y.at[t, rel], y_out.at[t, :, y_cols(place.at(-d, 0))], wg=place.at(d, rel))

    def y_in(t):
        for q in range(4):
            for rel in (0, 1):
                if q == 0 and rel == 0:
                    continue
                wires.recv(('y', t, q, rel) if q < 3 else ('y2', t, rel), y_out.at[t, :, y_cols(place.at(-offsets[q], rel))])

    phase_a(0)
    for t in range(1, steps):
        phase_a(t)
        if t > 1:
            phase_c(t - 2)
        phase_b(t - 1)
        if t == steps - 1:
            u_near(t)
    phase_c(steps - 2)
    for t in range(steps - 2):
        y_relay(t)
    phase_b(steps - 1)
    y_relay(steps - 2)
    phase_c(steps - 1)
    y_relay(steps - 1)
    with jax.named_scope('y_in'):
        for t in range(steps):
            y_in(t)
        for desc in y_open:
            desc.wait()
        wires.finish()


def layer_kernel(n, experts, small, mask, cos_t, sin_t, hidden, wq, wk, wv, wo, gate, up, down,
                 k_out, v_out, small_all, y_out, gq, gk, gv, go, wgu, wd, relay_gu, relay_d, xg, relay_y,
                 u_all, vd, ss_all, send_sems, recv_sems, loc_sems):
    place = Place(n)
    wires = Wires(place, send_sems, recv_sems)
    me = place.me
    prompts, seq = mask.shape[0], mask.shape[1]
    rows, d_model = hidden.shape
    cols, dcols = gate.shape[2] // n, down.shape[2] // n
    q_dim, kv_dim = wq.shape[1], wk.shape[1]
    bf16, f32 = jnp.bfloat16, jnp.float32

    enter(place)
    gather_q = PairGather(wires, 'q', wq, gq, 0)
    gather_k = PairGather(wires, 'k', wk, gk, 1)
    gather_v = PairGather(wires, 'v', wv, gv, 1)
    gather_o = PairGather(wires, 'o', wo, go, 1)
    moving = Reshard(wires, gate, up, down, wgu, wd, relay_gu, relay_d, loc_sems)
    others = [(off, rel) for off in (0, 1, -1, 2) for rel in (0, 1)][1:]
    for off, rel in others:
        wires.send(('small', off, rel), small, small_all.at[me], wg=place.at(off, rel))
    gather_q.start()
    gather_k.start()
    gather_v.start()
    small_all[me] = small[...]
    for off, rel in others:
        wires.recv(('small', off, rel), small_all.at[place.at(-off, rel)])

    def gain(i):
        return jnp.concatenate([small_all[j, pl.ds(experts + i, 1), :] for j in range(n)], axis=1).astype(jnp.float32)

    def norm(values):
        return values * lax.rsqrt(jnp.mean(values * values, axis=-1, keepdims=True) + NORM_EPS)

    h_gathers = [Gather(wires, ('h', t), lambda owner, t=t: xg.at[t, owner],
                        lambda owner, side, t=t: xg.at[t, owner, pl.ds(side * (seq // 2), seq // 2), :]) for t in range(prompts)]
    pl.run_scoped(
        functools.partial(attention_phase, n, place, small_all, mask, cos_t, sin_t, hidden, (wq, wk, wv, wo), (gq, gk, gv, go),
                          (gather_q, gather_k, gather_v, gather_o), moving, gain, norm, k_out, v_out, xg, loc_sems),
        pltpu.VMEM((rows, d_model), bf16),
        pltpu.VMEM((rows, d_model), bf16),
        pltpu.VMEM((rows, q_dim + 2 * kv_dim), f32),
        pltpu.VMEM((rows, q_dim), bf16),
        pltpu.VMEM((2, wq.shape[0], q_dim + 2 * kv_dim), bf16),
        pltpu.SemaphoreType.DMA((2, 3)),
        pltpu.SemaphoreType.DMA((prompts + 1,)),
    )
    h_gathers[0].start(xg.at[0, me])
    with jax.named_scope('mv_far'):
        moving.far_in(('gu',))
    pl.run_scoped(
        functools.partial(moe_phase, n, experts, wires, moving, h_gathers, small, small_all, gain, norm, wgu, wd, xg, y_out, relay_y,
                          u_all, vd, ss_all),
        pltpu.VMEM((experts, d_model, 2 * cols), bf16),
        pltpu.VMEM((2, 4, seq, d_model), bf16),
        pltpu.VMEM((prompts, n // 2, 2 * seq, LANES), f32),
        pltpu.VMEM((2, 2, 4 * seq, cols), f32),
        pltpu.VMEM((4, 2 * seq, dcols), f32),
        pltpu.VMEM((prompts, 4, 2, seq, dcols), bf16),
        pltpu.VMEM((4, 2, seq, dcols), bf16),
        pltpu.VMEM((prompts, n, 2, seq, LANES), bf16),
        pltpu.VMEM((small.shape[0], d_model), bf16),
        pltpu.VMEM((1, d_model), f32),
        pltpu.SemaphoreType.DMA((2, 2)),
        pltpu.SemaphoreType.DMA((experts + 1,)),
        pltpu.SemaphoreType.DMA((4,)),
        pltpu.SemaphoreType.DMA((prompts,)),
    )


def layer(n, experts, prompts, small, mask, cos_t, sin_t, hidden, wq, wk, wv, wo, gate, up, down):
    rows, d_model = hidden.shape
    seq = rows // prompts
    ff = gate.shape[2]
    drows = down.shape[1]
    cols, dcols = ff // n, d_model // n
    bf16, f32 = jnp.bfloat16, jnp.float32
    quarter = experts // 4

    def full(w):
        return jax.ShapeDtypeStruct((n,) + w.shape, bf16)

    outs = pl.pallas_call(
        functools.partial(layer_kernel, n, experts),
        name='layer',
        out_shape=(
            jax.ShapeDtypeStruct((rows, wk.shape[1]), bf16),
            jax.ShapeDtypeStruct((rows, wv.shape[1]), bf16),
            full(small),
            jax.ShapeDtypeStruct((prompts, seq, d_model), bf16),
            full(wq), full(wk), full(wv), full(wo),
            jax.ShapeDtypeStruct((experts, d_model, 2 * cols), bf16),
            jax.ShapeDtypeStruct((experts, ff, dcols), bf16),
            jax.ShapeDtypeStruct((2, 2, quarter, gate.shape[1], 2 * cols), bf16),
            jax.ShapeDtypeStruct((2, 2, quarter, drows, dcols), bf16),
            jax.ShapeDtypeStruct((prompts, n, seq, d_model), bf16),
            jax.ShapeDtypeStruct((prompts, 2, seq, dcols), bf16),
        ),
        in_specs=[VMEM_FULL] * 4 + [ANY] * 8,
        out_specs=(VMEM_FULL,) * 3 + (ANY,) * 11,
        scratch_shapes=[
            pltpu.VMEM((prompts, n // 2, n, 2 * seq, 2 * cols), bf16),
            pltpu.VMEM((experts, ff, dcols), bf16),
            pltpu.VMEM((prompts, n // 2, n, 8, 2 * seq), f32),
            pltpu.SemaphoreType.DMA((416,)),
            pltpu.SemaphoreType.DMA((416,)),
            pltpu.SemaphoreType.DMA((4,)),
        ],
        compiler_params=pltpu.CompilerParams(collective_id=0, has_side_effects=True, vmem_limit_bytes=67_000_000),
        cost_estimate=pl.CostEstimate(flops=110_000_000_000, bytes_accessed=400_000_000, transcendentals=0),
    )(small, mask, cos_t, sin_t, hidden, wq, wk, wv, wo, gate, up, down)
    return outs[3], outs[0], outs[1]


def solution(mesh):
    n = mesh.shape['wg']
    row_spec = P(('dp', 'wg'))
    dim0_spec = P('wg', None)
    dim1_spec = P(None, 'wg', None)

    def device_fn(hidden, seq_lens, route_idx, g_attn_in, w_query, w_key, w_value, w_attn_out, g_attn_out, g_moe_in, w_router, w_gate, w_up, w_down, g_moe_out):
        n_prompts, seq_len, d_model = hidden.shape
        experts = w_router.shape[1]
        rows = n_prompts * seq_len
        depth = w_query.shape[0]
        routes = jnp.pad(route_idx.T.astype(jnp.bfloat16), ((0, 0), (0, depth - rows)))
        small = jnp.concatenate([w_router.T] + [g[None] for g in (g_attn_in, g_attn_out, g_moe_in, g_moe_out)] + [routes], axis=0)
        small = jnp.pad(small, ((0, -small.shape[0] % 16), (0, 0)))
        pos = jnp.arange(seq_len)
        mask = ((pos[None, None, :] <= pos[None, :, None]) & (pos[None, None, :] < seq_lens[:, None, None])).astype(jnp.float32)
        cos_t, sin_t = rope_tables(seq_len)
        tok_rows = hidden.reshape(rows, d_model)
        y_out, k_rope, v_rows = layer(
            n, experts, n_prompts, small, mask, cos_t, sin_t, tok_rows, w_query, w_key, w_value, w_attn_out, w_gate, w_up, w_down)
        cache = (n_prompts, seq_len, w_key.shape[1] // HEAD_DIM, HEAD_DIM)
        return y_out, k_rope.reshape(cache), v_rows.reshape(cache)

    return jax.shard_map(
        device_fn,
        mesh=mesh,
        in_specs=(row_spec, row_spec, row_spec, P('wg'), dim0_spec, dim0_spec, dim0_spec, dim0_spec, P('wg'), P('wg'), dim0_spec, dim1_spec, dim1_spec, dim1_spec, P('wg')),
        out_specs=(row_spec, row_spec, row_spec),
        check_vma=False,
    )
```

```python
import functools
import jax
import jax.numpy as jnp
from jax import lax
from jax.experimental import pallas as pl
from jax.experimental.pallas import tpu as pltpu
from jax.sharding import PartitionSpec as P

HEAD_DIM = 128
LANES = 128
SOFT_CAP = 30.0
NORM_EPS = 1e-5
ROPE_BASE = 10000.0
ATTN_SCALE = HEAD_DIM ** -0.5
MESH = pl.DeviceIdType.MESH
ANY = pl.BlockSpec(memory_space=pl.ANY)
VMEM_FULL = pl.BlockSpec(memory_space=pltpu.VMEM)
DIRS = (1, -1)


def dot_f32(left_op, right_op):
    return jnp.dot(left_op, right_op, preferred_element_type=jnp.float32)


def rms_norm(values, gain_vec):
    values_f32 = values.astype(jnp.float32)
    inv_rms = lax.rsqrt(jnp.mean(values_f32 * values_f32, axis=-1, keepdims=True) + NORM_EPS)
    return values_f32 * inv_rms * gain_vec.astype(jnp.float32)


def rope_tables(seq_len):
    half_dim = HEAD_DIM // 2
    inv_freq = ROPE_BASE ** (-jnp.arange(half_dim, dtype=jnp.float32) * (2.0 / HEAD_DIM))
    angles = jnp.arange(seq_len, dtype=jnp.float32)[:, None] * inv_freq[None, :]
    cos_t, sin_t = jnp.cos(angles), jnp.sin(angles)
    return jnp.concatenate([cos_t, cos_t], axis=1), jnp.concatenate([-sin_t, sin_t], axis=1)


class Place:
    def __init__(self, n):
        self.n = n
        self.chips = n // 2
        self.me = lax.axis_index('wg')
        self.dp = lax.axis_index('dp')
        self.chip = self.me // 2
        self.core = self.me % 2
        self.parity = self.dp % 2
        self.twin = self.dp + 1 - 2 * self.parity

    def at(self, offset, rel):
        return ((self.chip + offset + self.chips) % self.chips) * 2 + (self.core + rel) % 2

    def chip_at(self, offset):
        return (self.chip + offset + self.chips) % self.chips


def still(ref):
    if not hasattr(ref, 'transforms'):
        return ref
    out = ref.ref
    for step in ref.transforms:
        out = out.at[tuple(pl.ds(0, index.size) if hasattr(index, 'start') else pl.ds(0, 1) for index in step.indices)]
    return out


class Wires:
    def __init__(self, place, send_sems, recv_sems):
        self.place, self.send_sems, self.recv_sems = place, send_sems, recv_sems
        self.slots = {}
        self.open = []

    def copy(self, name, src, dst, wg=None, dp=None):
        slot = self.slots.setdefault(name, len(self.slots))
        return pltpu.make_async_remote_copy(
            src_ref=src, dst_ref=dst, send_sem=self.send_sems.at[slot], recv_sem=self.recv_sems.at[slot],
            device_id={'dp': self.place.dp if dp is None else dp, 'wg': self.place.me if wg is None else wg},
            device_id_type=MESH)

    def send(self, name, src, dst, wg=None, dp=None):
        desc = self.copy(name, src, dst, wg, dp)
        desc.start()
        self.open.append((name, still(src)))

    def recv(self, name, dst):
        self.copy(name, dst, dst).wait_recv()

    def finish(self):
        for name, src in self.open:
            self.copy(name, src, src).wait_send()
        self.open = []


def enter(place):
    barrier = pltpu.get_barrier_semaphore()
    peers = [(place.dp, place.at(off, rel)) for off in (1, -1, 2) for rel in (0, 1)] + [(place.dp, place.at(0, 1))]
    peers.append((place.twin, place.me))
    for dp, wg in peers:
        pl.semaphore_signal(barrier, inc=1, device_id={'dp': dp, 'wg': wg}, device_id_type=MESH)
    pl.semaphore_wait(barrier, len(peers))


class Reshard:
    def __init__(self, wires, gate, up, down, wgu, wd, relay_gu, relay_d, loc_sems):
        self.wires, self.place = wires, wires.place
        n = self.place.n
        self.gate, self.up, self.down, self.wgu, self.wd = gate, up, down, wgu, wd
        self.relay_gu, self.relay_d, self.loc_sems = relay_gu, relay_d, loc_sems
        self.experts, self.rows, self.cols = gate.shape[0], gate.shape[1], gate.shape[2] // n
        self.drows, self.dcols = down.shape[1], down.shape[2] // n
        self.half, self.quarter = self.experts // 2, self.experts // 4
        self.mine = self.place.parity * self.half
        self.theirs = self.half - self.mine

    def piece(self, arr, e0, cnt, j):
        if arr == 'd':
            return self.down.at[pl.ds(e0, cnt), :, pl.ds(pl.multiple_of(j * self.dcols, LANES), self.dcols)]
        ref = self.gate if arr == 'g' else self.up
        return ref.at[pl.ds(e0, cnt), :, pl.ds(pl.multiple_of(j * self.cols, LANES), self.cols)]

    def land(self, arr, e0, cnt, src):
        if arr == 'd':
            return self.wd.at[pl.ds(e0, cnt), pl.ds(pl.multiple_of(src * self.drows, self.drows), self.drows), :]
        row = pl.ds(pl.multiple_of(src * self.rows, self.rows), self.rows)
        if arr == 'gu':
            return self.wgu.at[pl.ds(e0, cnt), row, :]
        return self.wgu.at[pl.ds(e0, cnt), row, pl.ds(0 if arr == 'g' else self.cols, self.cols)]

    def relay(self, arr, side, rel):
        if arr == 'd':
            return self.relay_d.at[side, rel]
        if arr == 'gu':
            return self.relay_gu.at[side, rel]
        return self.relay_gu.at[side, rel, :, :, pl.ds(0 if arr == 'g' else self.cols, self.cols)]

    def near(self):
        me, sib = self.place.me, self.place.at(0, 1)
        for i, arr in enumerate('gud'):
            self.wires.send(('sib', arr), self.piece(arr, 0, self.experts, sib), self.land(arr, 0, self.experts, me), wg=sib)
            self.own(i, arr).start()

    def own(self, i, arr):
        me = self.place.me
        return pltpu.make_async_copy(self.piece(arr, 0, self.experts, me), self.land(arr, 0, self.experts, me), self.loc_sems.at[i])

    def direct(self, rel, arrs):
        for arr in arrs:
            for d in DIRS:
                to = self.place.at(d, rel)
                self.wires.send(('direct', d, rel, arr), self.piece(arr, self.mine, self.half, to),
                                self.land(arr, self.mine, self.half, self.place.me), wg=to)

    def first_leg(self, rel, arrs):
        for arr in arrs:
            for side, d in enumerate(DIRS):
                e0 = self.mine + side * self.quarter
                self.wires.send(('leg1', d, rel, arr), self.piece(arr, e0, self.quarter, self.place.at(2 * d, rel)),
                                self.relay(arr, side, rel), wg=self.place.at(d, 0))

    def to_twin(self, name, arr, e0, cnt, src):
        region = self.land(arr, e0, cnt, src)
        self.wires.send(name, region, region, dp=self.place.twin)

    def direct_in(self, rel, arrs):
        for arr in arrs:
            for d in DIRS:
                src = self.place.at(-d, rel)
                for part in arr:
                    self.wires.recv(('direct', d, rel, part), self.land(part, self.mine, self.half, src))
                self.to_twin(('twin', d, rel, arr), arr, self.mine, self.half, src)

    def second_leg(self, rel, arrs):
        for arr in arrs:
            for side, d in enumerate(DIRS):
                for part in arr:
                    self.wires.recv(('leg1', d, rel, part), self.relay(part, side, rel))
                self.wires.send(('leg2', d, rel, arr), self.relay(arr, side, rel),
                                self.land(arr, self.mine + side * self.quarter, self.quarter, self.place.at(-d, 0)),
                                wg=self.place.at(d, rel))

    def far_in(self, arrs):
        for arr in arrs:
            for rel in (0, 1):
                for side, d in enumerate(DIRS):
                    src = self.place.at(2 * d, rel)
                    e0 = self.mine + side * self.quarter
                    self.wires.recv(('leg2', d, rel, arr), self.land(arr, e0, self.quarter, src))
                    self.to_twin(('twin2', d, rel, arr), arr, e0, self.quarter, src)

    def finish_near(self, arr):
        for part in arr:
            self.wires.recv(('sib', part), self.land(part, 0, self.experts, self.place.at(0, 1)))
            self.own('gud'.index(part), part).wait()

    def finish_twin(self, arr):
        for rel in (0, 1):
            for side, d in enumerate(DIRS):
                self.wires.recv(('twin', d, rel, arr), self.land(arr, self.theirs, self.half, self.place.at(-d, rel)))
                self.wires.recv(('twin2', d, rel, arr),
                                self.land(arr, self.theirs + side * self.quarter, self.quarter, self.place.at(2 * d, rel)))


class PairGather:
    def __init__(self, wires, name, src, dst, give_side):
        self.wires, self.place, self.name, self.src, self.dst = wires, wires.place, name, src, dst
        rows = src.shape[0]
        given = rows * 5 // 16
        parity = self.place.parity
        last = rows - given
        self.spans = {'give': (parity * last, given), 'both': (given, rows - 2 * given), 'take': (last - parity * last, given)}
        self.far_side = {'give': give_side, 'both': 1 - give_side}

    def part(self, owner, what):
        row, cnt = self.spans[what]
        return self.dst.at[owner, pl.ds(pl.multiple_of(row, 16), cnt), :]

    def start(self):
        place, me = self.place, self.place.me
        for what in ('give', 'both'):
            row, cnt = self.spans[what]
            own = self.src.at[pl.ds(pl.multiple_of(row, 16), cnt), :]
            for d in DIRS:
                self.wires.send((self.name, 'own', what, d), own, self.part(me, what), wg=place.at(d, 0))
        self.wires.send((self.name, 'sib'), self.src, self.dst.at[me], wg=place.at(0, 1))

    def give(self, tag, owner):
        part = self.part(owner, 'give')
        self.wires.send((self.name, 'give', tag), part, part, dp=self.place.twin)

    def near_in(self, *whats):
        place = self.place
        for what in whats:
            for side, d in enumerate(DIRS):
                owner = place.at(-d, 0)
                part = self.part(owner, what)
                self.wires.recv((self.name, 'own', what, d), part)
                if what == 'give':
                    self.give(d, owner)
                if self.far_side[what] == side:
                    self.wires.send((self.name, 'far', what), part, part, wg=place.at(d, 0))
                self.wires.send((self.name, 'across', what, d), part, part, wg=place.at(0, 1))

    def far_in(self, *whats):
        place = self.place
        owner = place.at(2, 0)
        for what in whats:
            part = self.part(owner, what)
            self.wires.recv((self.name, 'far', what), part)
            if what == 'give':
                self.give(2, owner)
            self.wires.send((self.name, 'across', what, 2), part, part, wg=place.at(0, 1))

    def twin_in(self, *tags):
        for tag in tags:
            part = self.part(self.place.at(-tag, 0), 'take')
            self.wires.recv((self.name, 'give', tag), part)
            self.wires.send((self.name, 'across', 'take', tag), part, part, wg=self.place.at(0, 1))

    def sib_in(self):
        place = self.place
        self.wires.recv((self.name, 'sib'), self.dst.at[place.at(0, 1)])
        for tag in (1, -1, 2):
            for what in ('give', 'both', 'take'):
                self.wires.recv((self.name, 'across', what, tag), self.part(place.at(-tag, 1), what))


class Gather:
    def __init__(self, wires, name, region, half_region):
        self.wires, self.place, self.name = wires, wires.place, name
        self.region, self.half_region = region, half_region

    def start(self, src):
        place, dst = self.place, self.region(self.place.me)
        for d in DIRS:
            self.wires.send((self.name, 'own', d), src, dst, wg=place.at(d, 0))
        self.wires.send((self.name, 'own', 0), src, dst, wg=place.at(0, 1))

    def near_in(self, side):
        d, place = DIRS[side], self.place
        owner = place.at(-d, 0)
        block, part = self.region(owner), self.half_region(owner, side)
        self.wires.recv((self.name, 'own', d), block)
        self.wires.send((self.name, 'far', d), part, part, wg=place.at(d, 0))
        self.wires.send((self.name, 'across', d), block, block, wg=place.at(0, 1))

    def far_in(self):
        place = self.place
        owner = place.at(2, 0)
        for side, d in enumerate(DIRS):
            part = self.half_region(owner, side)
            self.wires.recv((self.name, 'far', d), part)
            self.wires.send((self.name, 'across2', d), part, part, wg=place.at(0, 1))

    def sib_own(self):
        self.wires.recv((self.name, 'own', 0), self.region(self.place.at(0, 1)))

    def sib_near(self, side):
        self.wires.recv((self.name, 'across', DIRS[side]), self.region(self.place.at(-DIRS[side], 1)))

    def sib_far(self):
        for side, d in enumerate(DIRS):
            self.wires.recv((self.name, 'across2', d), self.half_region(self.place.at(2, 1), side))


def attention_phase(n, place, small_all, mask, cos_t, sin_t, hidden_hbm, weights, gathered, gathers, moving, gain, norm, k_out, v_out,
                    xg, loc_sems, hidden, h, acc, ctx, wbuf, load_sems, x_sems):
    wq, wk, wv, wo = weights
    gq, gk, gv, go = gathered
    gather_q, gather_k, gather_v, gather_o = gathers
    me = place.me
    prompts, seq = mask.shape[0], mask.shape[1]
    rows, d_model = hidden.shape
    depth = wq.shape[0]
    q_dim, kv_dim = wq.shape[1], wk.shape[1]
    n_kv = kv_dim // HEAD_DIM
    group = q_dim // kv_dim
    tile = 512
    load = pltpu.make_async_copy(hidden_hbm, hidden, x_sems.at[prompts])
    load.start()
    load.wait()

    def norm_in(i, carry):
        r = pl.ds(pl.multiple_of(i * 16, 16), 16)
        h[r, :] = (norm(hidden[r, :].astype(jnp.float32)) * gain(0)).astype(jnp.bfloat16)
        return carry

    with jax.named_scope('norm_in'):
        lax.fori_loop(0, rows // 16, norm_in, 0)
        acc[...] = jnp.zeros_like(acc)

    with jax.named_scope('near'):
        gather_q.near_in('give', 'both')
        gather_k.near_in('give', 'both')
        gather_v.near_in('give', 'both')
        gather_o.start()
        moving.direct(0, 'gu')
        moving.first_leg(0, 'gu')
        moving.first_leg(1, 'gu')
        moving.near()
    with jax.named_scope('qkv_far'):
        gather_q.twin_in(1, -1)
        gather_k.twin_in(1, -1)
        gather_v.twin_in(1, -1)
        gather_q.far_in('give', 'both')
        gather_k.far_in('give', 'both')
        gather_v.far_in('give', 'both')
    with jax.named_scope('qkv_last'):
        gather_q.twin_in(2)
        gather_k.twin_in(2)
        gather_v.twin_in(2)
        gather_q.sib_in()
        gather_k.sib_in()
        gather_v.sib_in()
    with jax.named_scope('o_near_give'):
        gather_o.near_in('give')

    def owner_of(i):
        return (me + i) % n

    def product(lhs, weights, first_col):
        def loads(i, slot):
            owner = owner_of(i)

            def start(own):
                col = 0
                for w, (src, gathered) in enumerate(weights):
                    width = src.shape[1]
                    pltpu.make_async_copy(src if own else gathered.at[owner], wbuf.at[slot, :, pl.ds(col, width)],
                                          load_sems.at[slot, w]).start()
                    col += width

            @pl.when(i == 0)
            def _():
                start(True)

            @pl.when(i > 0)
            def _():
                start(False)

        def step(i, carry):
            slot = i % 2
            owner = owner_of(i)

            @pl.when(i + 1 < n)
            def _():
                loads(i + 1, 1 - slot)

            col = 0
            for w, (src, gathered) in enumerate(weights):
                width = src.shape[1]
                pltpu.make_async_copy(gathered.at[owner], wbuf.at[slot, :, pl.ds(col, width)], load_sems.at[slot, w]).wait()
                col += width

            def tiles(j, carry):
                c = pl.ds(pl.multiple_of(j * tile, tile), tile)
                acc[:, c] += dot_f32(lhs[:, pl.ds(pl.multiple_of(owner * depth, depth), depth)], wbuf[slot, :, c])
                return carry

            return lax.fori_loop(0, col // tile, tiles, carry)

        loads(0, 0)
        lax.fori_loop(0, n, step, 0)

    with jax.named_scope('qkv_mm'):
        product(h, ((wq, gq), (wk, gk), (wv, gv)), 0)

    def rope(values):
        values = values.astype(jnp.bfloat16).astype(jnp.float32)
        cos_v, sin_v = cos_t[...], sin_t[...]
        times = values.shape[0] // seq
        if times > 1:
            cos_v, sin_v = jnp.concatenate([cos_v] * times, axis=0), jnp.concatenate([sin_v] * times, axis=0)
        return (values * cos_v + pltpu.roll(values, HEAD_DIM // 2, 1) * sin_v).astype(jnp.bfloat16)

    def attend(i, carry):
        p, g = i // n_kv, i % n_kv
        r = pl.ds(pl.multiple_of(p * seq, seq), seq)
        kv_cols = pl.ds(pl.multiple_of(g * HEAD_DIM, HEAD_DIM), HEAD_DIM)
        q = jnp.concatenate([acc[r, pl.ds(pl.multiple_of((g * group + j) * HEAD_DIM, HEAD_DIM), HEAD_DIM)]
                             for j in range(group)], axis=0)
        q = rope(q)
        k = rope(acc[r, pl.ds(pl.multiple_of(q_dim + g * HEAD_DIM, HEAD_DIM), HEAD_DIM)])
        v = acc[r, pl.ds(pl.multiple_of(q_dim + kv_dim + g * HEAD_DIM, HEAD_DIM), HEAD_DIM)].astype(jnp.bfloat16)
        k_out[r, kv_cols] = k
        v_out[r, kv_cols] = v
        scores = lax.dot_general(q, k, (((1,), (1,)), ((), ())), preferred_element_type=jnp.float32) * ATTN_SCALE
        scores = SOFT_CAP * jnp.tanh(scores / SOFT_CAP)
        allowed = jnp.concatenate([mask[p]] * group, axis=0) > 0.5
        scores = jnp.where(allowed, scores, -1e30)
        ex = jnp.exp(scores - jnp.max(scores, axis=-1, keepdims=True))
        probs = (ex / jnp.sum(ex, axis=-1, keepdims=True)).astype(jnp.bfloat16)
        out = dot_f32(probs, v).astype(jnp.bfloat16)
        for j in range(group):
            ctx[r, pl.ds(pl.multiple_of((g * group + j) * HEAD_DIM, HEAD_DIM), HEAD_DIM)] = out[j * seq:(j + 1) * seq]
        return carry

    with jax.named_scope('attend'):
        lax.fori_loop(0, prompts * n_kv, attend, 0)

    with jax.named_scope('o_near_both'):
        gather_o.near_in('both')
    with jax.named_scope('direct_in0'):
        moving.direct_in(0, ('gu',))
    with jax.named_scope('leg2'):
        moving.second_leg(0, ('gu',))
        moving.second_leg(1, ('gu',))
        moving.direct(1, 'gu')
        moving.direct(0, 'd')
        moving.direct(1, 'd')
    with jax.named_scope('o_far'):
        gather_o.twin_in(1, -1)
        gather_o.far_in('give', 'both')
    with jax.named_scope('mv_far'):
        moving.far_in(('gu',))
    with jax.named_scope('o_last'):
        gather_o.twin_in(2)
        gather_o.sib_in()
    with jax.named_scope('o_mm'):
        acc[...] = jnp.zeros_like(acc)
        product(ctx, ((wo, go),), 0)

    def finish_rows(i, carry):
        r = pl.ds(pl.multiple_of(i * 16, 16), 16)
        mid = (hidden[r, :].astype(jnp.float32) + norm(acc[r, pl.ds(0, d_model)]) * gain(1)).astype(jnp.bfloat16)
        ctx[r, :] = mid
        return carry

    with jax.named_scope('finish_rows'):
        lax.fori_loop(0, rows // 16, finish_rows, 0)
    stores = []
    for t in range(prompts):
        desc = pltpu.make_async_copy(ctx.at[pl.ds(t * seq, seq), :], xg.at[t, me], x_sems.at[t])
        desc.start()
        stores.append(desc)
    for desc in stores:
        desc.wait()


def moe_phase(n, experts, wires, moving, h_gathers, small, small_all, gain, norm, wgu, wd, xg, y_out, relay_y, u_all, vd, ss_all,
              vgu, hbuf, gates, us, mbuf, ybuf, xcols, route, router, gain_in, load_sems, w_sems, x_sems, out_sems):
    place = wires.place
    steps, seq, d_model = route.shape[0], route.shape[3], hbuf.shape[3]
    chips, me = place.chips, place.me
    rows = 2 * seq
    depth = small.shape[1]
    cols = vgu.shape[2] // 2
    dcols = vd.shape[2]
    offsets = (0, -1, 1, 2)

    with jax.named_scope('tables'):
        gain_in[...] = gain(2)
        for j in range(n):
            router[:, pl.ds(j * depth, depth)] = small_all[j]

        def route_of(j, carry):
            for t in range(steps):
                for i in range(2):
                    line = small_all[j, pl.ds(experts + 4 + i, 1), pl.ds(t * seq, seq)].astype(jnp.float32)
                    route[t, j, i] = jnp.transpose(jnp.broadcast_to(line, (LANES, seq))).astype(jnp.bfloat16)
            return carry

        lax.fori_loop(0, n, route_of, 0)

    own_cols = pl.ds(pl.multiple_of(me * dcols, LANES), dcols)
    half = experts // 2

    def u_owner_chip(owner, q):
        return (owner // 2 + offsets[q] + chips) % chips

    u_gathers = {t: [] for t in range(steps)}
    others = [(off, rel) for off in (0, 1, -1, 2) for rel in (0, 1)][1:]

    pairs = ((0, 1), (2, 3))

    def begin(t, pair):
        loads = []
        for s, q in enumerate(pairs[pair]):
            chip = place.chip_at(offsets[q])
            desc = pltpu.make_async_copy(xg.at[t, pl.ds(2 * chip, 2)], hbuf.at[pair, pl.ds(2 * s, 2)], load_sems.at[pair, s])
            desc.start()
            loads.append(desc)
        return loads

    def routes(t, chips_of):
        def one(i):
            return jnp.concatenate([route[t, pl.ds(2 * chip, 2), i].reshape(rows, LANES) for chip in chips_of], axis=0)

        return one(0), one(1)

    def prepare(t, pair, loads):
        with jax.named_scope('load'):
            for desc in loads:
                desc.wait()
        h = hbuf.at[pair]

        def norm_rows(i, carry):
            r = pl.ds(pl.multiple_of(i % (seq // 32) * 32, 32), 32)
            x = h[i // (seq // 32), r, :].astype(jnp.float32)
            h[i // (seq // 32), r, :] = (norm(x) * gain_in[...]).astype(jnp.bfloat16)
            return carry

        with jax.named_scope('norm'):
            lax.fori_loop(0, 2 * rows // 32, norm_rows, 0)
        logits = lax.dot_general(h[...].reshape(2 * rows, d_model), router[...], (((1,), (1,)), ((), ())),
                                 preferred_element_type=jnp.float32)
        lane = lax.broadcasted_iota(jnp.int32, logits.shape, 1)
        logits = jnp.where(lane < experts, logits, -1e30)
        peak = jnp.max(logits, axis=-1, keepdims=True)
        ex = jnp.where(lane < experts, jnp.exp(logits - peak), 0.0)
        probs = ex / jnp.sum(ex, axis=-1, keepdims=True)
        lane_f = lane.astype(jnp.float32)
        chips_of = [place.chip_at(offsets[q]) for q in pairs[pair]]
        g0, g1 = (jnp.sum(jnp.where(lane_f == r[:, :logits.shape[1]].astype(jnp.float32), probs, 0.0), axis=-1, keepdims=True)
                  for r in routes(t, chips_of))
        both = jnp.where(lax.broadcasted_iota(jnp.int32, (2 * rows, LANES), 1) == 0, g0, g1)
        for s, chip in enumerate(chips_of):
            gates[t, chip] = both[s * rows:(s + 1) * rows]
        us[pair] = jnp.zeros(us.shape[1:], jnp.float32)

    def up_part(t, pair, e0, cnt):
        h = hbuf.at[pair]
        chips_of = [place.chip_at(offsets[q]) for q in pairs[pair]]

        def expert(i, carry):
            e = e0 + i
            act = dot_f32(h[...].reshape(2 * rows, d_model), vgu[e])
            inner = (jax.nn.gelu(act[:, :cols]) * act[:, cols:]).astype(jnp.bfloat16).astype(jnp.float32)
            e_f = e.astype(jnp.float32)
            r0, r1 = routes(t, chips_of)
            us[pair, 0] = jnp.where(r0.astype(jnp.float32) == e_f, inner, us[pair, 0])
            us[pair, 1] = jnp.where(r1.astype(jnp.float32) == e_f, inner, us[pair, 1])
            return carry

        with jax.named_scope('up'):
            lax.fori_loop(0, cnt, expert, 0)

    def emit(t, pair):
        for s, q in enumerate(pairs[pair]):
            chip = place.chip_at(offsets[q])
            for i in range(2):
                u_all[t, chip, me, :, pl.ds(i * cols, cols)] = us[pair, i, s * rows:(s + 1) * rows].astype(jnp.bfloat16)
            if t == steps - 1:
                gather = Gather(wires, ('u', t, q), lambda owner, q=q: u_all.at[t, u_owner_chip(owner, q), owner],
                                lambda owner, side, q=q: u_all.at[t, u_owner_chip(owner, q), owner, pl.ds(side * seq, seq), :])
                gather.start(u_all.at[t, chip, me])
                u_gathers[t].append(gather)
        if t < steps - 1 and pair == 1:
            gather = Gather(wires, ('u', t), lambda owner: u_all.at[t, :, owner],
                            lambda owner, side: u_all.at[t, pl.ds(side * (chips // 2), chips // 2), owner])
            gather.start(u_all.at[t, :, me])
            u_gathers[t].append(gather)

    def chunk_near(t):
        h_gathers[t].near_in(0)
        h_gathers[t].near_in(1)
        if t + 1 < steps:
            h_gathers[t + 1].start(xg.at[t + 1, me])

    def load_experts(e0):
        loads = []
        for i in range(half):
            desc = pltpu.make_async_copy(wgu.at[e0 + i], vgu.at[e0 + i], w_sems.at[i])
            desc.start()
            loads.append(desc)
        return loads

    def phase_a(t):
        gather = h_gathers[t]
        mine_loads = []
        if t == 0:
            with jax.named_scope('mine_in'):
                moving.finish_near('gu')
                mine_loads = load_experts(moving.mine)
        with jax.named_scope('near'):
            gather.sib_own()
            chunk_near(t)
            gather.sib_near(0)
            loads = begin(t, 0)
        if t > 0:
            u_near(t - 1)
        prepare(t, 0, loads)
        if t == 0:
            for desc in mine_loads:
                desc.wait()
            up_part(t, 0, moving.mine, half)
        else:
            up_part(t, 0, 0, experts)
            emit(t, 0)
        with jax.named_scope('far'):
            gather.sib_near(1)
            gather.far_in()
            gather.sib_far()
            loads = begin(t, 1)
            if t == 1:
                moving.far_in(('d',))
        prepare(t, 1, loads)
        if t == 0:
            up_part(t, 1, moving.mine, half)
            with jax.named_scope('theirs_in'):
                moving.finish_twin('gu')
                theirs_loads = load_experts(moving.theirs)
                for desc in theirs_loads:
                    desc.wait()
            for pair in (0, 1):
                up_part(t, pair, moving.theirs, half)
                emit(t, pair)
            with jax.named_scope('d_relay'):
                moving.direct_in(0, ('d',))
                moving.direct_in(1, ('d',))
                moving.second_leg(0, ('d',))
                moving.second_leg(1, ('d',))
        else:
            up_part(t, 1, 0, experts)
            emit(t, 1)

    def u_near(t):
        with jax.named_scope('u_near'):
            for gather in u_gathers[t]:
                gather.near_in(0)
                gather.near_in(1)

    def phase_b(t):
        if t == 0:
            with jax.named_scope('d_in'):
                moving.finish_near('d')
                moving.finish_twin('d')
                d_load = pltpu.make_async_copy(wd, vd, w_sems.at[experts])
                d_load.start()
        with jax.named_scope('u_wait'):
            for gather in u_gathers[t]:
                gather.far_in()
                gather.sib_own()
                gather.sib_near(0)
                gather.sib_near(1)
                gather.sib_far()
        if t == 0:
            d_load.wait()
        for first in range(0, chips, 2):
            chips_of = (first, first + 1)
            acc = mbuf.at[pl.ds(first, 2)]
            acc[...] = jnp.zeros_like(acc)

            def expert(e, carry):
                e_b = e.astype(jnp.bfloat16)
                r0, r1 = routes(t, chips_of)
                m0, m1 = r0 == e_b, r1 == e_b
                zero = jnp.zeros((2 * rows, LANES), jnp.bfloat16)
                parts = []
                for j in range(n):
                    u0 = u_all[t, pl.ds(first, 2), j, :, pl.ds(0, cols)].reshape(2 * rows, cols)
                    u1 = u_all[t, pl.ds(first, 2), j, :, pl.ds(cols, cols)].reshape(2 * rows, cols)
                    parts.append(jnp.where(m0, u0, jnp.where(m1, u1, zero)))
                ue = jnp.concatenate(parts, axis=1)
                out = dot_f32(ue, vd[e])
                e_f = e.astype(jnp.float32)
                both = gates[t, pl.ds(first, 2)].reshape(2 * rows, LANES)
                gate = jnp.where(r0.astype(jnp.float32) == e_f, both[:, :1], jnp.where(r1.astype(jnp.float32) == e_f, both[:, 1:2], 0.0))
                acc[...] += (jnp.concatenate([gate] * (dcols // LANES), axis=1) * out).reshape(2, rows, dcols)
                return carry

            with jax.named_scope('down'):
                lax.fori_loop(0, experts, expert, 0)
            for chip in chips_of:
                part = mbuf[chip]
                squares = jnp.sum(part * part, axis=-1, keepdims=True)
                ss_all[t, chip, me] = jnp.transpose(jnp.broadcast_to(squares, (rows, LANES)))[:ss_all.shape[3]]
        for off, rel in others:
            region = ss_all.at[t, :, me]
            wires.send(('ss', t, off, rel), region, region, wg=place.at(off, rel))

    y_open = []

    def phase_c(t):
        loads = []
        for q in range(4):
            chip = place.chip_at(offsets[q])
            desc = pltpu.make_async_copy(xg.at[t, pl.ds(2 * chip, 2), :, own_cols], xcols.at[q], x_sems.at[q])
            desc.start()
            loads.append(desc)
        gain_out = small[pl.ds(experts + 3, 1), :].astype(jnp.float32)
        with jax.named_scope('ss_wait'):
            for off, rel in others:
                wires.recv(('ss', t, off, rel), ss_all.at[t, :, place.at(-off, rel)])
        for q in (3, 1, 2, 0):
            chip = place.chip_at(offsets[q])
            loads[q].wait()
            with jax.named_scope('y'):
                total = ss_all[t, chip, 0]
                for j in range(1, n):
                    total += ss_all[t, chip, j]
                line = jnp.broadcast_to(total[:1], (LANES, rows))
                scale = lax.rsqrt(jnp.transpose(line) * (1.0 / d_model) + NORM_EPS)
                scale = jnp.concatenate([scale] * (dcols // LANES), axis=1)
                x1 = xcols[q].reshape(rows, dcols).astype(jnp.float32)
                ybuf[t, q] = (x1 + mbuf[chip] * scale * gain_out).astype(jnp.bfloat16).reshape(2, seq, dcols)
            dst = y_out.at[t, :, own_cols]
            for rel in (0, 1):
                part = ybuf.at[t, q, (place.core + rel) % 2]
                if q == 0 and rel == 0:
                    desc = pltpu.make_async_copy(part, dst, out_sems.at[t])
                    desc.start()
                    y_open.append(desc)
                elif q < 3:
                    wires.send(('y', t, q, rel), part, dst, wg=place.at(offsets[q], rel))
                else:
                    wires.send(('y1', t, rel), part, relay_y.at[t, rel], wg=place.at(DIRS[rel], 0))

    def y_cols(src):
        return pl.ds(pl.multiple_of(src * dcols, LANES), dcols)

    def y_relay(t):
        for rel, d in enumerate(DIRS):
            wires.recv(('y1', t, rel), relay_y.at[t, rel])
            wires.send(('y2', t, rel), relay_y.at[t, rel], y_out.at[t, :, y_cols(place.at(-d, 0))], wg=place.at(d, rel))

    def y_in(t):
        for q in range(4):
            for rel in (0, 1):
                if q == 0 and rel == 0:
                    continue
                wires.recv(('y', t, q, rel) if q < 3 else ('y2', t, rel), y_out.at[t, :, y_cols(place.at(-offsets[q], rel))])

    phase_a(0)
    for t in range(1, steps):
        phase_a(t)
        if t > 1:
            phase_c(t - 2)
        phase_b(t - 1)
        if t == steps - 1:
            u_near(t)
    phase_c(steps - 2)
    for t in range(steps - 2):
        y_relay(t)
    phase_b(steps - 1)
    y_relay(steps - 2)
    phase_c(steps - 1)
    y_relay(steps - 1)
    with jax.named_scope('y_in'):
        for t in range(steps):
            y_in(t)
        for desc in y_open:
            desc.wait()
        wires.finish()


def layer_kernel(n, experts, small, mask, cos_t, sin_t, hidden, wq, wk, wv, wo, gate, up, down,
                 k_out, v_out, small_all, y_out, gq, gk, gv, go, wgu, wd, relay_gu, relay_d, xg, relay_y,
                 u_all, vd, ss_all, send_sems, recv_sems, loc_sems):
    place = Place(n)
    wires = Wires(place, send_sems, recv_sems)
    me = place.me
    prompts, seq = mask.shape[0], mask.shape[1]
    rows, d_model = hidden.shape
    cols, dcols = gate.shape[2] // n, down.shape[2] // n
    q_dim, kv_dim = wq.shape[1], wk.shape[1]
    bf16, f32 = jnp.bfloat16, jnp.float32

    enter(place)
    gather_q = PairGather(wires, 'q', wq, gq, 0)
    gather_k = PairGather(wires, 'k', wk, gk, 1)
    gather_v = PairGather(wires, 'v', wv, gv, 1)
    gather_o = PairGather(wires, 'o', wo, go, 1)
    moving = Reshard(wires, gate, up, down, wgu, wd, relay_gu, relay_d, loc_sems)
    others = [(off, rel) for off in (0, 1, -1, 2) for rel in (0, 1)][1:]
    for off, rel in others:
        wires.send(('small', off, rel), small, small_all.at[me], wg=place.at(off, rel))
    gather_q.start()
    gather_k.start()
    gather_v.start()
    small_all[me] = small[...]
    for off, rel in others:
        wires.recv(('small', off, rel), small_all.at[place.at(-off, rel)])

    def gain(i):
        return jnp.concatenate([small_all[j, pl.ds(experts + i, 1), :] for j in range(n)], axis=1).astype(jnp.float32)

    def norm(values):
        return values * lax.rsqrt(jnp.mean(values * values, axis=-1, keepdims=True) + NORM_EPS)

    h_gathers = [Gather(wires, ('h', t), lambda owner, t=t: xg.at[t, owner],
                        lambda owner, side, t=t: xg.at[t, owner, pl.ds(side * (seq // 2), seq // 2), :]) for t in range(prompts)]
    pl.run_scoped(
        functools.partial(attention_phase, n, place, small_all, mask, cos_t, sin_t, hidden, (wq, wk, wv, wo), (gq, gk, gv, go),
                          (gather_q, gather_k, gather_v, gather_o), moving, gain, norm, k_out, v_out, xg, loc_sems),
        pltpu.VMEM((rows, d_model), bf16),
        pltpu.VMEM((rows, d_model), bf16),
        pltpu.VMEM((rows, q_dim + 2 * kv_dim), f32),
        pltpu.VMEM((rows, q_dim), bf16),
        pltpu.VMEM((2, wq.shape[0], q_dim + 2 * kv_dim), bf16),
        pltpu.SemaphoreType.DMA((2, 3)),
        pltpu.SemaphoreType.DMA((prompts + 1,)),
    )
    h_gathers[0].start(xg.at[0, me])
    with jax.named_scope('services'):
        moving.first_leg(0, 'd')
        moving.first_leg(1, 'd')
        moving.direct_in(1, ('gu',))
    pl.run_scoped(
        functools.partial(moe_phase, n, experts, wires, moving, h_gathers, small, small_all, gain, norm, wgu, wd, xg, y_out, relay_y,
                          u_all, vd, ss_all),
        pltpu.VMEM((experts, d_model, 2 * cols), bf16),
        pltpu.VMEM((2, 4, seq, d_model), bf16),
        pltpu.VMEM((prompts, n // 2, 2 * seq, LANES), f32),
        pltpu.VMEM((2, 2, 4 * seq, cols), f32),
        pltpu.VMEM((4, 2 * seq, dcols), f32),
        pltpu.VMEM((prompts, 4, 2, seq, dcols), bf16),
        pltpu.VMEM((4, 2, seq, dcols), bf16),
        pltpu.VMEM((prompts, n, 2, seq, LANES), bf16),
        pltpu.VMEM((small.shape[0], d_model), bf16),
        pltpu.VMEM((1, d_model), f32),
        pltpu.SemaphoreType.DMA((2, 2)),
        pltpu.SemaphoreType.DMA((experts + 1,)),
        pltpu.SemaphoreType.DMA((4,)),
        pltpu.SemaphoreType.DMA((prompts,)),
    )


def layer(n, experts, prompts, small, mask, cos_t, sin_t, hidden, wq, wk, wv, wo, gate, up, down):
    rows, d_model = hidden.shape
    seq = rows // prompts
    ff = gate.shape[2]
    drows = down.shape[1]
    cols, dcols = ff // n, d_model // n
    bf16, f32 = jnp.bfloat16, jnp.float32
    quarter = experts // 4

    def full(w):
        return jax.ShapeDtypeStruct((n,) + w.shape, bf16)

    outs = pl.pallas_call(
        functools.partial(layer_kernel, n, experts),
        name='layer',
        out_shape=(
            jax.ShapeDtypeStruct((rows, wk.shape[1]), bf16),
            jax.ShapeDtypeStruct((rows, wv.shape[1]), bf16),
            full(small),
            jax.ShapeDtypeStruct((prompts, seq, d_model), bf16),
            full(wq), full(wk), full(wv), full(wo),
            jax.ShapeDtypeStruct((experts, d_model, 2 * cols), bf16),
            jax.ShapeDtypeStruct((experts, ff, dcols), bf16),
            jax.ShapeDtypeStruct((2, 2, quarter, gate.shape[1], 2 * cols), bf16),
            jax.ShapeDtypeStruct((2, 2, quarter, drows, dcols), bf16),
            jax.ShapeDtypeStruct((prompts, n, seq, d_model), bf16),
            jax.ShapeDtypeStruct((prompts, 2, seq, dcols), bf16),
        ),
        in_specs=[VMEM_FULL] * 4 + [ANY] * 8,
        out_specs=(VMEM_FULL,) * 3 + (ANY,) * 11,
        scratch_shapes=[
            pltpu.VMEM((prompts, n // 2, n, 2 * seq, 2 * cols), bf16),
            pltpu.VMEM((experts, ff, dcols), bf16),
            pltpu.VMEM((prompts, n // 2, n, 8, 2 * seq), f32),
            pltpu.SemaphoreType.DMA((416,)),
            pltpu.SemaphoreType.DMA((416,)),
            pltpu.SemaphoreType.DMA((4,)),
        ],
        compiler_params=pltpu.CompilerParams(collective_id=0, has_side_effects=True, vmem_limit_bytes=67_000_000),
        cost_estimate=pl.CostEstimate(flops=110_000_000_000, bytes_accessed=400_000_000, transcendentals=0),
    )(small, mask, cos_t, sin_t, hidden, wq, wk, wv, wo, gate, up, down)
    return outs[3], outs[0], outs[1]


def solution(mesh):
    n = mesh.shape['wg']
    row_spec = P(('dp', 'wg'))
    dim0_spec = P('wg', None)
    dim1_spec = P(None, 'wg', None)

    def device_fn(hidden, seq_lens, route_idx, g_attn_in, w_query, w_key, w_value, w_attn_out, g_attn_out, g_moe_in, w_router, w_gate, w_up, w_down, g_moe_out):
        n_prompts, seq_len, d_model = hidden.shape
        experts = w_router.shape[1]
        rows = n_prompts * seq_len
        depth = w_query.shape[0]
        routes = jnp.pad(route_idx.T.astype(jnp.bfloat16), ((0, 0), (0, depth - rows)))
        small = jnp.concatenate([w_router.T] + [g[None] for g in (g_attn_in, g_attn_out, g_moe_in, g_moe_out)] + [routes], axis=0)
        small = jnp.pad(small, ((0, -small.shape[0] % 16), (0, 0)))
        pos = jnp.arange(seq_len)
        mask = ((pos[None, None, :] <= pos[None, :, None]) & (pos[None, None, :] < seq_lens[:, None, None])).astype(jnp.float32)
        cos_t, sin_t = rope_tables(seq_len)
        tok_rows = hidden.reshape(rows, d_model)
        y_out, k_rope, v_rows = layer(
            n, experts, n_prompts, small, mask, cos_t, sin_t, tok_rows, w_query, w_key, w_value, w_attn_out, w_gate, w_up, w_down)
        cache = (n_prompts, seq_len, w_key.shape[1] // HEAD_DIM, HEAD_DIM)
        return y_out, k_rope.reshape(cache), v_rows.reshape(cache)

    return jax.shard_map(
        device_fn,
        mesh=mesh,
        in_specs=(row_spec, row_spec, row_spec, P('wg'), dim0_spec, dim0_spec, dim0_spec, dim0_spec, P('wg'), P('wg'), dim0_spec, dim1_spec, dim1_spec, dim1_spec, P('wg')),
        out_specs=(row_spec, row_spec, row_spec),
        check_vma=False,
    )
```

```python
import functools
import jax
import jax.numpy as jnp
from jax import lax
from jax.experimental import pallas as pl
from jax.experimental.pallas import tpu as pltpu
from jax.sharding import PartitionSpec as P

HEAD_DIM = 128
LANES = 128
SOFT_CAP = 30.0
NORM_EPS = 1e-5
ROPE_BASE = 10000.0
ATTN_SCALE = HEAD_DIM ** -0.5
MESH = pl.DeviceIdType.MESH
ANY = pl.BlockSpec(memory_space=pl.ANY)
VMEM_FULL = pl.BlockSpec(memory_space=pltpu.VMEM)
DIRS = (1, -1)


def dot_f32(left_op, right_op):
    return jnp.dot(left_op, right_op, preferred_element_type=jnp.float32)


def rms_norm(values, gain_vec):
    values_f32 = values.astype(jnp.float32)
    inv_rms = lax.rsqrt(jnp.mean(values_f32 * values_f32, axis=-1, keepdims=True) + NORM_EPS)
    return values_f32 * inv_rms * gain_vec.astype(jnp.float32)


def rope_tables(seq_len):
    half_dim = HEAD_DIM // 2
    inv_freq = ROPE_BASE ** (-jnp.arange(half_dim, dtype=jnp.float32) * (2.0 / HEAD_DIM))
    angles = jnp.arange(seq_len, dtype=jnp.float32)[:, None] * inv_freq[None, :]
    cos_t, sin_t = jnp.cos(angles), jnp.sin(angles)
    return jnp.concatenate([cos_t, cos_t], axis=1), jnp.concatenate([-sin_t, sin_t], axis=1)


class Place:
    def __init__(self, n):
        self.n = n
        self.chips = n // 2
        self.me = lax.axis_index('wg')
        self.dp = lax.axis_index('dp')
        self.chip = self.me // 2
        self.core = self.me % 2
        self.parity = self.dp % 2
        self.twin = self.dp + 1 - 2 * self.parity

    def at(self, offset, rel):
        return ((self.chip + offset + self.chips) % self.chips) * 2 + (self.core + rel) % 2

    def chip_at(self, offset):
        return (self.chip + offset + self.chips) % self.chips


def still(ref):
    if not hasattr(ref, 'transforms'):
        return ref
    out = ref.ref
    for step in ref.transforms:
        out = out.at[tuple(pl.ds(0, index.size) if hasattr(index, 'start') else pl.ds(0, 1) for index in step.indices)]
    return out


class Wires:
    def __init__(self, place, send_sems, recv_sems):
        self.place, self.send_sems, self.recv_sems = place, send_sems, recv_sems
        self.slots = {}
        self.open = []

    def copy(self, name, src, dst, wg=None, dp=None):
        slot = self.slots.setdefault(name, len(self.slots))
        return pltpu.make_async_remote_copy(
            src_ref=src, dst_ref=dst, send_sem=self.send_sems.at[slot], recv_sem=self.recv_sems.at[slot],
            device_id={'dp': self.place.dp if dp is None else dp, 'wg': self.place.me if wg is None else wg},
            device_id_type=MESH)

    def send(self, name, src, dst, wg=None, dp=None):
        desc = self.copy(name, src, dst, wg, dp)
        desc.start()
        self.open.append((name, still(src)))

    def recv(self, name, dst):
        self.copy(name, dst, dst).wait_recv()

    def finish(self):
        for name, src in self.open:
            self.copy(name, src, src).wait_send()
        self.open = []


def enter(place):
    barrier = pltpu.get_barrier_semaphore()
    peers = [(place.dp, place.at(off, rel)) for off in (1, -1, 2) for rel in (0, 1)] + [(place.dp, place.at(0, 1))]
    peers.append((place.twin, place.me))
    for dp, wg in peers:
        pl.semaphore_signal(barrier, inc=1, device_id={'dp': dp, 'wg': wg}, device_id_type=MESH)
    pl.semaphore_wait(barrier, len(peers))


class Reshard:
    def __init__(self, wires, gate, up, down, wgu, wd, relay_gu, relay_d, loc_sems):
        self.wires, self.place = wires, wires.place
        n = self.place.n
        self.gate, self.up, self.down, self.wgu, self.wd = gate, up, down, wgu, wd
        self.relay_gu, self.relay_d, self.loc_sems = relay_gu, relay_d, loc_sems
        self.experts, self.rows, self.cols = gate.shape[0], gate.shape[1], gate.shape[2] // n
        self.drows, self.dcols = down.shape[1], down.shape[2] // n
        self.half, self.quarter = self.experts // 2, self.experts // 4
        self.mine = self.place.parity * self.half
        self.theirs = self.half - self.mine

    def piece(self, arr, e0, cnt, j):
        if arr == 'd':
            return self.down.at[pl.ds(e0, cnt), :, pl.ds(pl.multiple_of(j * self.dcols, LANES), self.dcols)]
        ref = self.gate if arr == 'g' else self.up
        return ref.at[pl.ds(e0, cnt), :, pl.ds(pl.multiple_of(j * self.cols, LANES), self.cols)]

    def land(self, arr, e0, cnt, src):
        if arr == 'd':
            return self.wd.at[pl.ds(e0, cnt), pl.ds(pl.multiple_of(src * self.drows, self.drows), self.drows), :]
        row = pl.ds(pl.multiple_of(src * self.rows, self.rows), self.rows)
        if arr == 'gu':
            return self.wgu.at[pl.ds(e0, cnt), row, :]
        return self.wgu.at[pl.ds(e0, cnt), row, pl.ds(0 if arr == 'g' else self.cols, self.cols)]

    def relay(self, arr, side, rel):
        if arr == 'd':
            return self.relay_d.at[side, rel]
        if arr == 'gu':
            return self.relay_gu.at[side, rel]
        return self.relay_gu.at[side, rel, :, :, pl.ds(0 if arr == 'g' else self.cols, self.cols)]

    def near(self):
        me, sib = self.place.me, self.place.at(0, 1)
        for i, arr in enumerate('gud'):
            self.wires.send(('sib', arr), self.piece(arr, 0, self.experts, sib), self.land(arr, 0, self.experts, me), wg=sib)
            self.own(i, arr).start()

    def own(self, i, arr):
        me = self.place.me
        return pltpu.make_async_copy(self.piece(arr, 0, self.experts, me), self.land(arr, 0, self.experts, me), self.loc_sems.at[i])

    def direct(self, rel, arrs):
        for arr in arrs:
            for d in DIRS:
                to = self.place.at(d, rel)
                self.wires.send(('direct', d, rel, arr), self.piece(arr, self.mine, self.half, to),
                                self.land(arr, self.mine, self.half, self.place.me), wg=to)

    def first_leg(self, rel, arrs):
        for arr in arrs:
            for side, d in enumerate(DIRS):
                e0 = self.mine + side * self.quarter
                self.wires.send(('leg1', d, rel, arr), self.piece(arr, e0, self.quarter, self.place.at(2 * d, rel)),
                                self.relay(arr, side, rel), wg=self.place.at(d, 0))

    def to_twin(self, name, arr, e0, cnt, src):
        region = self.land(arr, e0, cnt, src)
        self.wires.send(name, region, region, dp=self.place.twin)

    def direct_in(self, rel, arrs):
        for arr in arrs:
            for d in DIRS:
                src = self.place.at(-d, rel)
                for part in arr:
                    self.wires.recv(('direct', d, rel, part), self.land(part, self.mine, self.half, src))
                self.to_twin(('twin', d, rel, arr), arr, self.mine, self.half, src)

    def second_leg(self, rel, arrs):
        for arr in arrs:
            for side, d in enumerate(DIRS):
                for part in arr:
                    self.wires.recv(('leg1', d, rel, part), self.relay(part, side, rel))
                self.wires.send(('leg2', d, rel, arr), self.relay(arr, side, rel),
                                self.land(arr, self.mine + side * self.quarter, self.quarter, self.place.at(-d, 0)),
                                wg=self.place.at(d, rel))

    def far_in(self, arrs):
        for arr in arrs:
            for rel in (0, 1):
                for side, d in enumerate(DIRS):
                    src = self.place.at(2 * d, rel)
                    e0 = self.mine + side * self.quarter
                    self.wires.recv(('leg2', d, rel, arr), self.land(arr, e0, self.quarter, src))
                    self.to_twin(('twin2', d, rel, arr), arr, e0, self.quarter, src)

    def finish_near(self, arr):
        for part in arr:
            self.wires.recv(('sib', part), self.land(part, 0, self.experts, self.place.at(0, 1)))
            self.own('gud'.index(part), part).wait()

    def finish_twin(self, arr):
        for rel in (0, 1):
            for side, d in enumerate(DIRS):
                self.wires.recv(('twin', d, rel, arr), self.land(arr, self.theirs, self.half, self.place.at(-d, rel)))
                self.wires.recv(('twin2', d, rel, arr),
                                self.land(arr, self.theirs + side * self.quarter, self.quarter, self.place.at(2 * d, rel)))


class PairGather:
    def __init__(self, wires, name, src, dst, give_side):
        self.wires, self.place, self.name, self.src, self.dst = wires, wires.place, name, src, dst
        rows = src.shape[0]
        given = rows * 5 // 16
        parity = self.place.parity
        last = rows - given
        self.spans = {'give': (parity * last, given), 'both': (given, rows - 2 * given), 'take': (last - parity * last, given)}
        self.far_side = {'give': give_side, 'both': 1 - give_side}

    def part(self, owner, what):
        row, cnt = self.spans[what]
        return self.dst.at[owner, pl.ds(pl.multiple_of(row, 16), cnt), :]

    def start(self):
        place, me = self.place, self.place.me
        for what in ('give', 'both'):
            row, cnt = self.spans[what]
            own = self.src.at[pl.ds(pl.multiple_of(row, 16), cnt), :]
            for d in DIRS:
                self.wires.send((self.name, 'own', what, d), own, self.part(me, what), wg=place.at(d, 0))
        self.wires.send((self.name, 'sib'), self.src, self.dst.at[me], wg=place.at(0, 1))

    def give(self, tag, owner):
        part = self.part(owner, 'give')
        self.wires.send((self.name, 'give', tag), part, part, dp=self.place.twin)

    def near_in(self, *whats):
        place = self.place
        for what in whats:
            for side, d in enumerate(DIRS):
                owner = place.at(-d, 0)
                part = self.part(owner, what)
                self.wires.recv((self.name, 'own', what, d), part)
                if what == 'give':
                    self.give(d, owner)
                if self.far_side[what] == side:
                    self.wires.send((self.name, 'far', what), part, part, wg=place.at(d, 0))
                self.wires.send((self.name, 'across', what, d), part, part, wg=place.at(0, 1))

    def far_in(self, *whats):
        place = self.place
        owner = place.at(2, 0)
        for what in whats:
            part = self.part(owner, what)
            self.wires.recv((self.name, 'far', what), part)
            if what == 'give':
                self.give(2, owner)
            self.wires.send((self.name, 'across', what, 2), part, part, wg=place.at(0, 1))

    def twin_in(self, *tags):
        for tag in tags:
            part = self.part(self.place.at(-tag, 0), 'take')
            self.wires.recv((self.name, 'give', tag), part)
            self.wires.send((self.name, 'across', 'take', tag), part, part, wg=self.place.at(0, 1))

    def sib_in(self):
        place = self.place
        self.wires.recv((self.name, 'sib'), self.dst.at[place.at(0, 1)])
        for tag in (1, -1, 2):
            for what in ('give', 'both', 'take'):
                self.wires.recv((self.name, 'across', what, tag), self.part(place.at(-tag, 1), what))


class Gather:
    def __init__(self, wires, name, region, half_region):
        self.wires, self.place, self.name = wires, wires.place, name
        self.region, self.half_region = region, half_region

    def start(self, src):
        place, dst = self.place, self.region(self.place.me)
        for d in DIRS:
            self.wires.send((self.name, 'own', d), src, dst, wg=place.at(d, 0))
        self.wires.send((self.name, 'own', 0), src, dst, wg=place.at(0, 1))

    def near_in(self, side):
        d, place = DIRS[side], self.place
        owner = place.at(-d, 0)
        block, part = self.region(owner), self.half_region(owner, side)
        self.wires.recv((self.name, 'own', d), block)
        self.wires.send((self.name, 'far', d), part, part, wg=place.at(d, 0))
        self.wires.send((self.name, 'across', d), block, block, wg=place.at(0, 1))

    def far_in(self):
        place = self.place
        owner = place.at(2, 0)
        for side, d in enumerate(DIRS):
            part = self.half_region(owner, side)
            self.wires.recv((self.name, 'far', d), part)
            self.wires.send((self.name, 'across2', d), part, part, wg=place.at(0, 1))

    def sib_own(self):
        self.wires.recv((self.name, 'own', 0), self.region(self.place.at(0, 1)))

    def sib_near(self, side):
        self.wires.recv((self.name, 'across', DIRS[side]), self.region(self.place.at(-DIRS[side], 1)))

    def sib_far(self):
        for side, d in enumerate(DIRS):
            self.wires.recv((self.name, 'across2', d), self.half_region(self.place.at(2, 1), side))


def attention_phase(n, place, small_all, mask, cos_t, sin_t, hidden_hbm, weights, gathered, gathers, moving, gain, norm, k_out, v_out,
                    xg, loc_sems, hidden, h, acc, ctx, wbuf, load_sems, x_sems):
    wq, wk, wv, wo = weights
    gq, gk, gv, go = gathered
    gather_q, gather_k, gather_v, gather_o = gathers
    me = place.me
    prompts, seq = mask.shape[0], mask.shape[1]
    rows, d_model = hidden.shape
    depth = wq.shape[0]
    q_dim, kv_dim = wq.shape[1], wk.shape[1]
    n_kv = kv_dim // HEAD_DIM
    group = q_dim // kv_dim
    tile = 512
    load = pltpu.make_async_copy(hidden_hbm, hidden, x_sems.at[prompts])
    load.start()
    load.wait()

    def norm_in(i, carry):
        r = pl.ds(pl.multiple_of(i * 16, 16), 16)
        h[r, :] = (norm(hidden[r, :].astype(jnp.float32)) * gain(0)).astype(jnp.bfloat16)
        return carry

    with jax.named_scope('norm_in'):
        lax.fori_loop(0, rows // 16, norm_in, 0)
        acc[...] = jnp.zeros_like(acc)

    with jax.named_scope('near'):
        gather_q.near_in('give', 'both')
        gather_k.near_in('give', 'both')
        gather_v.near_in('give', 'both')
        gather_o.start()
        moving.direct(0, 'gu')
        moving.first_leg(0, 'gu')
        moving.first_leg(1, 'gu')
        moving.near()
    with jax.named_scope('qkv_far'):
        gather_q.twin_in(1, -1)
        gather_k.twin_in(1, -1)
        gather_v.twin_in(1, -1)
        gather_q.far_in('give', 'both')
        gather_k.far_in('give', 'both')
        gather_v.far_in('give', 'both')
    with jax.named_scope('qkv_last'):
        gather_q.twin_in(2)
        gather_k.twin_in(2)
        gather_v.twin_in(2)
        gather_q.sib_in()
        gather_k.sib_in()
        gather_v.sib_in()
    with jax.named_scope('o_near_give'):
        gather_o.near_in('give')

    def owner_of(i):
        return (me + i) % n

    def product(lhs, weights, first_col):
        def loads(i, slot):
            owner = owner_of(i)

            def start(own):
                col = 0
                for w, (src, gathered) in enumerate(weights):
                    width = src.shape[1]
                    pltpu.make_async_copy(src if own else gathered.at[owner], wbuf.at[slot, :, pl.ds(col, width)],
                                          load_sems.at[slot, w]).start()
                    col += width

            @pl.when(i == 0)
            def _():
                start(True)

            @pl.when(i > 0)
            def _():
                start(False)

        def step(i, carry):
            slot = i % 2
            owner = owner_of(i)

            @pl.when(i + 1 < n)
            def _():
                loads(i + 1, 1 - slot)

            col = 0
            for w, (src, gathered) in enumerate(weights):
                width = src.shape[1]
                pltpu.make_async_copy(gathered.at[owner], wbuf.at[slot, :, pl.ds(col, width)], load_sems.at[slot, w]).wait()
                col += width

            def tiles(j, carry):
                c = pl.ds(pl.multiple_of(j * tile, tile), tile)
                acc[:, c] += dot_f32(lhs[:, pl.ds(pl.multiple_of(owner * depth, depth), depth)], wbuf[slot, :, c])
                return carry

            return lax.fori_loop(0, col // tile, tiles, carry)

        loads(0, 0)
        lax.fori_loop(0, n, step, 0)

    with jax.named_scope('qkv_mm'):
        product(h, ((wq, gq), (wk, gk), (wv, gv)), 0)

    def rope(values):
        values = values.astype(jnp.bfloat16).astype(jnp.float32)
        cos_v, sin_v = cos_t[...], sin_t[...]
        times = values.shape[0] // seq
        if times > 1:
            cos_v, sin_v = jnp.concatenate([cos_v] * times, axis=0), jnp.concatenate([sin_v] * times, axis=0)
        return (values * cos_v + pltpu.roll(values, HEAD_DIM // 2, 1) * sin_v).astype(jnp.bfloat16)

    def attend(i, carry):
        p, g = i // n_kv, i % n_kv
        r = pl.ds(pl.multiple_of(p * seq, seq), seq)
        kv_cols = pl.ds(pl.multiple_of(g * HEAD_DIM, HEAD_DIM), HEAD_DIM)
        q = jnp.concatenate([acc[r, pl.ds(pl.multiple_of((g * group + j) * HEAD_DIM, HEAD_DIM), HEAD_DIM)]
                             for j in range(group)], axis=0)
        q = rope(q)
        k = rope(acc[r, pl.ds(pl.multiple_of(q_dim + g * HEAD_DIM, HEAD_DIM), HEAD_DIM)])
        v = acc[r, pl.ds(pl.multiple_of(q_dim + kv_dim + g * HEAD_DIM, HEAD_DIM), HEAD_DIM)].astype(jnp.bfloat16)
        k_out[r, kv_cols] = k
        v_out[r, kv_cols] = v
        scores = lax.dot_general(q, k, (((1,), (1,)), ((), ())), preferred_element_type=jnp.float32) * ATTN_SCALE
        scores = SOFT_CAP * jnp.tanh(scores / SOFT_CAP)
        allowed = jnp.concatenate([mask[p]] * group, axis=0) > 0.5
        scores = jnp.where(allowed, scores, -1e30)
        ex = jnp.exp(scores - jnp.max(scores, axis=-1, keepdims=True))
        probs = (ex / jnp.sum(ex, axis=-1, keepdims=True)).astype(jnp.bfloat16)
        out = dot_f32(probs, v).astype(jnp.bfloat16)
        for j in range(group):
            ctx[r, pl.ds(pl.multiple_of((g * group + j) * HEAD_DIM, HEAD_DIM), HEAD_DIM)] = out[j * seq:(j + 1) * seq]
        return carry

    with jax.named_scope('attend'):
        lax.fori_loop(0, prompts * n_kv, attend, 0)

    with jax.named_scope('o_near_both'):
        gather_o.near_in('both')
    with jax.named_scope('direct_in0'):
        moving.direct_in(0, ('gu',))
    with jax.named_scope('leg2'):
        moving.second_leg(0, ('gu',))
        moving.second_leg(1, ('gu',))
        moving.direct(1, 'gu')
        moving.direct(0, 'd')
        moving.direct(1, 'd')
    with jax.named_scope('o_far'):
        gather_o.twin_in(1, -1)
        gather_o.far_in('give', 'both')
    with jax.named_scope('mv_far'):
        moving.far_in(('gu',))
    with jax.named_scope('o_last'):
        gather_o.twin_in(2)
        gather_o.sib_in()
    with jax.named_scope('o_mm'):
        acc[...] = jnp.zeros_like(acc)
        product(ctx, ((wo, go),), 0)

    def finish_rows(i, carry):
        r = pl.ds(pl.multiple_of(i * 16, 16), 16)
        mid = (hidden[r, :].astype(jnp.float32) + norm(acc[r, pl.ds(0, d_model)]) * gain(1)).astype(jnp.bfloat16)
        ctx[r, :] = mid
        return carry

    with jax.named_scope('finish_rows'):
        lax.fori_loop(0, rows // 16, finish_rows, 0)
    stores = []
    for t in range(prompts):
        desc = pltpu.make_async_copy(ctx.at[pl.ds(t * seq, seq), :], xg.at[t, me], x_sems.at[t])
        desc.start()
        stores.append(desc)
    for desc in stores:
        desc.wait()


def moe_phase(n, experts, wires, moving, h_gathers, small, small_all, gain, norm, wgu, wd, xg, y_out, relay_y, u_all, vd, ss_all,
              vgu, hbuf, gates, us, mbuf, ybuf, xcols, route, router, gain_in, load_sems, w_sems, x_sems, out_sems):
    place = wires.place
    steps, seq, d_model = route.shape[0], route.shape[3], hbuf.shape[3]
    chips, me = place.chips, place.me
    rows = 2 * seq
    depth = small.shape[1]
    cols = vgu.shape[2] // 2
    dcols = vd.shape[2]
    offsets = (0, -1, 1, 2)

    with jax.named_scope('tables'):
        gain_in[...] = gain(2)
        for j in range(n):
            router[:, pl.ds(j * depth, depth)] = small_all[j]

        def route_of(j, carry):
            for t in range(steps):
                for i in range(2):
                    line = small_all[j, pl.ds(experts + 4 + i, 1), pl.ds(t * seq, seq)].astype(jnp.float32)
                    route[t, j, i] = jnp.transpose(jnp.broadcast_to(line, (LANES, seq))).astype(jnp.bfloat16)
            return carry

        lax.fori_loop(0, n, route_of, 0)

    own_cols = pl.ds(pl.multiple_of(me * dcols, LANES), dcols)
    half = experts // 2

    def u_owner_chip(owner, q):
        return (owner // 2 + offsets[q] + chips) % chips

    u_gathers = {t: [] for t in range(steps)}
    others = [(off, rel) for off in (0, 1, -1, 2) for rel in (0, 1)][1:]

    pairs = ((0, 1), (2, 3))

    def begin(t, pair):
        loads = []
        for s, q in enumerate(pairs[pair]):
            chip = place.chip_at(offsets[q])
            desc = pltpu.make_async_copy(xg.at[t, pl.ds(2 * chip, 2)], hbuf.at[pair, pl.ds(2 * s, 2)], load_sems.at[pair, s])
            desc.start()
            loads.append(desc)
        return loads

    def routes(t, chips_of):
        def one(i):
            return jnp.concatenate([route[t, pl.ds(2 * chip, 2), i].reshape(rows, LANES) for chip in chips_of], axis=0)

        return one(0), one(1)

    def prepare(t, pair, loads):
        with jax.named_scope('load'):
            for desc in loads:
                desc.wait()
        h = hbuf.at[pair]

        def norm_rows(i, carry):
            r = pl.ds(pl.multiple_of(i % (seq // 32) * 32, 32), 32)
            x = h[i // (seq // 32), r, :].astype(jnp.float32)
            h[i // (seq // 32), r, :] = (norm(x) * gain_in[...]).astype(jnp.bfloat16)
            return carry

        with jax.named_scope('norm'):
            lax.fori_loop(0, 2 * rows // 32, norm_rows, 0)
        logits = lax.dot_general(h[...].reshape(2 * rows, d_model), router[...], (((1,), (1,)), ((), ())),
                                 preferred_element_type=jnp.float32)
        lane = lax.broadcasted_iota(jnp.int32, logits.shape, 1)
        logits = jnp.where(lane < experts, logits, -1e30)
        peak = jnp.max(logits, axis=-1, keepdims=True)
        ex = jnp.where(lane < experts, jnp.exp(logits - peak), 0.0)
        probs = ex / jnp.sum(ex, axis=-1, keepdims=True)
        lane_f = lane.astype(jnp.float32)
        chips_of = [place.chip_at(offsets[q]) for q in pairs[pair]]
        g0, g1 = (jnp.sum(jnp.where(lane_f == r[:, :logits.shape[1]].astype(jnp.float32), probs, 0.0), axis=-1, keepdims=True)
                  for r in routes(t, chips_of))
        both = jnp.where(lax.broadcasted_iota(jnp.int32, (2 * rows, LANES), 1) == 0, g0, g1)
        for s, chip in enumerate(chips_of):
            gates[t % 2, chip] = both[s * rows:(s + 1) * rows]
        us[pair] = jnp.zeros(us.shape[1:], jnp.float32)

    def up_part(t, pair, e0, cnt):
        h = hbuf.at[pair]
        chips_of = [place.chip_at(offsets[q]) for q in pairs[pair]]

        def expert(i, carry):
            e = e0 + i
            act = dot_f32(h[...].reshape(2 * rows, d_model), vgu[e])
            inner = (jax.nn.gelu(act[:, :cols]) * act[:, cols:]).astype(jnp.bfloat16).astype(jnp.float32)
            e_f = e.astype(jnp.float32)
            r0, r1 = routes(t, chips_of)
            us[pair, 0] = jnp.where(r0.astype(jnp.float32) == e_f, inner, us[pair, 0])
            us[pair, 1] = jnp.where(r1.astype(jnp.float32) == e_f, inner, us[pair, 1])
            return carry

        with jax.named_scope('up'):
            lax.fori_loop(0, cnt, expert, 0)

    def emit(t, pair):
        for s, q in enumerate(pairs[pair]):
            chip = place.chip_at(offsets[q])
            for i in range(2):
                u_all[t, chip, me, :, pl.ds(i * cols, cols)] = us[pair, i, s * rows:(s + 1) * rows].astype(jnp.bfloat16)
            if t == steps - 1:
                gather = Gather(wires, ('u', t, q), lambda owner, q=q: u_all.at[t, u_owner_chip(owner, q), owner],
                                lambda owner, side, q=q: u_all.at[t, u_owner_chip(owner, q), owner, pl.ds(side * seq, seq), :])
                gather.start(u_all.at[t, chip, me])
                u_gathers[t].append(gather)
        if t < steps - 1 and pair == 1:
            gather = Gather(wires, ('u', t), lambda owner: u_all.at[t, :, owner],
                            lambda owner, side: u_all.at[t, pl.ds(side * (chips // 2), chips // 2), owner])
            gather.start(u_all.at[t, :, me])
            u_gathers[t].append(gather)

    def chunk_near(t):
        h_gathers[t].near_in(0)
        h_gathers[t].near_in(1)
        if t + 1 < steps:
            h_gathers[t + 1].start(xg.at[t + 1, me])

    def load_experts(e0):
        loads = []
        for i in range(half):
            desc = pltpu.make_async_copy(wgu.at[e0 + i], vgu.at[e0 + i], w_sems.at[i])
            desc.start()
            loads.append(desc)
        return loads

    def phase_a(t):
        gather = h_gathers[t]
        mine_loads = []
        if t == 0:
            with jax.named_scope('mine_in'):
                moving.finish_near('gu')
                mine_loads = load_experts(moving.mine)
        with jax.named_scope('near'):
            gather.sib_own()
            chunk_near(t)
            gather.sib_near(0)
            loads = begin(t, 0)
        if t > 0:
            u_near(t - 1)
        prepare(t, 0, loads)
        if t == 0:
            for desc in mine_loads:
                desc.wait()
            up_part(t, 0, moving.mine, half)
        else:
            up_part(t, 0, 0, experts)
            emit(t, 0)
        with jax.named_scope('far'):
            gather.sib_near(1)
            gather.far_in()
            gather.sib_far()
            loads = begin(t, 1)
            if t == 1:
                moving.far_in(('d',))
        prepare(t, 1, loads)
        if t == 0:
            with jax.named_scope('d_direct'):
                moving.direct_in(0, ('d',))
                moving.direct_in(1, ('d',))
            up_part(t, 1, moving.mine, half)
            with jax.named_scope('theirs_in'):
                moving.finish_twin('gu')
                theirs_loads = load_experts(moving.theirs)
                for desc in theirs_loads:
                    desc.wait()
            for pair in (0, 1):
                up_part(t, pair, moving.theirs, half)
                emit(t, pair)
            with jax.named_scope('d_relay'):
                moving.second_leg(0, ('d',))
                moving.second_leg(1, ('d',))
        else:
            up_part(t, 1, 0, experts)
            emit(t, 1)

    def u_near(t):
        with jax.named_scope('u_near'):
            for gather in u_gathers[t]:
                gather.near_in(0)
                gather.near_in(1)

    def phase_b(t, between):
        if t == 0:
            with jax.named_scope('d_in'):
                moving.finish_near('d')
                moving.finish_twin('d')
                d_load = pltpu.make_async_copy(wd, vd, w_sems.at[experts])
                d_load.start()
        with jax.named_scope('u_wait'):
            for gather in u_gathers[t]:
                gather.far_in()
                gather.sib_own()
                gather.sib_near(0)
                gather.sib_near(1)
                gather.sib_far()
        if t == 0:
            d_load.wait()
        for first in range(0, chips, 2):
            chips_of = (first, first + 1)
            acc = mbuf.at[pl.ds((chips * t + first) % mbuf.shape[0], 2)]
            acc[...] = jnp.zeros_like(acc)

            def expert(e, carry):
                e_b = e.astype(jnp.bfloat16)
                r0, r1 = routes(t, chips_of)
                m0, m1 = r0 == e_b, r1 == e_b
                zero = jnp.zeros((2 * rows, LANES), jnp.bfloat16)
                parts = []
                for j in range(n):
                    u0 = u_all[t, pl.ds(first, 2), j, :, pl.ds(0, cols)].reshape(2 * rows, cols)
                    u1 = u_all[t, pl.ds(first, 2), j, :, pl.ds(cols, cols)].reshape(2 * rows, cols)
                    parts.append(jnp.where(m0, u0, jnp.where(m1, u1, zero)))
                ue = jnp.concatenate(parts, axis=1)
                out = dot_f32(ue, vd[e])
                e_f = e.astype(jnp.float32)
                both = gates[t % 2, pl.ds(first, 2)].reshape(2 * rows, LANES)
                gate = jnp.where(r0.astype(jnp.float32) == e_f, both[:, :1], jnp.where(r1.astype(jnp.float32) == e_f, both[:, 1:2], 0.0))
                acc[...] += (jnp.concatenate([gate] * (dcols // LANES), axis=1) * out).reshape(2, rows, dcols)
                return carry

            with jax.named_scope('down'):
                lax.fori_loop(0, experts, expert, 0)
            for chip in chips_of:
                part = mbuf[(chips * t + chip) % mbuf.shape[0]]
                squares = jnp.sum(part * part, axis=-1, keepdims=True)
                ss_all[t, chip, me] = jnp.transpose(jnp.broadcast_to(squares, (rows, LANES)))[:ss_all.shape[3]]
            if first == 0:
                between()
        for off, rel in others:
            region = ss_all.at[t, :, me]
            wires.send(('ss', t, off, rel), region, region, wg=place.at(off, rel))

    y_open = []

    def phase_c(t):
        loads = []
        for q in range(4):
            chip = place.chip_at(offsets[q])
            desc = pltpu.make_async_copy(xg.at[t, pl.ds(2 * chip, 2), :, own_cols], xcols.at[q], x_sems.at[q])
            desc.start()
            loads.append(desc)
        gain_out = small[pl.ds(experts + 3, 1), :].astype(jnp.float32)
        with jax.named_scope('ss_wait'):
            for off, rel in others:
                wires.recv(('ss', t, off, rel), ss_all.at[t, :, place.at(-off, rel)])
        for q in (3, 1, 2, 0):
            chip = place.chip_at(offsets[q])
            loads[q].wait()
            with jax.named_scope('y'):
                total = ss_all[t, chip, 0]
                for j in range(1, n):
                    total += ss_all[t, chip, j]
                line = jnp.broadcast_to(total[:1], (LANES, rows))
                scale = lax.rsqrt(jnp.transpose(line) * (1.0 / d_model) + NORM_EPS)
                scale = jnp.concatenate([scale] * (dcols // LANES), axis=1)
                x1 = xcols[q].reshape(rows, dcols).astype(jnp.float32)
                ybuf[t, q] = (x1 + mbuf[(chips * t + chip) % mbuf.shape[0]] * scale * gain_out).astype(jnp.bfloat16).reshape(2, seq, dcols)
            dst = y_out.at[t, :, own_cols]
            for rel in (0, 1):
                part = ybuf.at[t, q, (place.core + rel) % 2]
                if q == 0 and rel == 0:
                    desc = pltpu.make_async_copy(part, dst, out_sems.at[t])
                    desc.start()
                    y_open.append(desc)
                elif q < 3:
                    wires.send(('y', t, q, rel), part, dst, wg=place.at(offsets[q], rel))
                else:
                    wires.send(('y1', t, rel), part, relay_y.at[t, rel], wg=place.at(DIRS[rel], 0))

    def y_cols(src):
        return pl.ds(pl.multiple_of(src * dcols, LANES), dcols)

    def y_relay(t):
        for rel, d in enumerate(DIRS):
            wires.recv(('y1', t, rel), relay_y.at[t, rel])
            wires.send(('y2', t, rel), relay_y.at[t, rel], y_out.at[t, :, y_cols(place.at(-d, 0))], wg=place.at(d, rel))

    def y_in(t):
        for q in range(4):
            for rel in (0, 1):
                if q == 0 and rel == 0:
                    continue
                wires.recv(('y', t, q, rel) if q < 3 else ('y2', t, rel), y_out.at[t, :, y_cols(place.at(-offsets[q], rel))])

    phase_a(0)
    for t in range(1, steps):
        phase_a(t)
        if t > 1:
            phase_c(t - 2)
        phase_b(t - 1, functools.partial(u_near, t) if t == steps - 1 else lambda: None)
    for t in range(steps - 2):
        y_relay(t)
    phase_b(steps - 1, functools.partial(phase_c, steps - 2))
    y_relay(steps - 2)
    phase_c(steps - 1)
    y_relay(steps - 1)
    with jax.named_scope('y_in'):
        for t in range(steps):
            y_in(t)
        for desc in y_open:
            desc.wait()
        wires.finish()


def layer_kernel(n, experts, small, mask, cos_t, sin_t, hidden, wq, wk, wv, wo, gate, up, down,
                 k_out, v_out, small_all, y_out, gq, gk, gv, go, wgu, wd, relay_gu, relay_d, xg, relay_y,
                 u_all, vd, ss_all, send_sems, recv_sems, loc_sems):
    place = Place(n)
    wires = Wires(place, send_sems, recv_sems)
    me = place.me
    prompts, seq = mask.shape[0], mask.shape[1]
    rows, d_model = hidden.shape
    cols, dcols = gate.shape[2] // n, down.shape[2] // n
    q_dim, kv_dim = wq.shape[1], wk.shape[1]
    bf16, f32 = jnp.bfloat16, jnp.float32

    enter(place)
    gather_q = PairGather(wires, 'q', wq, gq, 0)
    gather_k = PairGather(wires, 'k', wk, gk, 1)
    gather_v = PairGather(wires, 'v', wv, gv, 1)
    gather_o = PairGather(wires, 'o', wo, go, 1)
    moving = Reshard(wires, gate, up, down, wgu, wd, relay_gu, relay_d, loc_sems)
    others = [(off, rel) for off in (0, 1, -1, 2) for rel in (0, 1)][1:]
    for off, rel in others:
        wires.send(('small', off, rel), small, small_all.at[me], wg=place.at(off, rel))
    gather_q.start()
    gather_k.start()
    gather_v.start()
    small_all[me] = small[...]
    for off, rel in others:
        wires.recv(('small', off, rel), small_all.at[place.at(-off, rel)])

    def gain(i):
        return jnp.concatenate([small_all[j, pl.ds(experts + i, 1), :] for j in range(n)], axis=1).astype(jnp.float32)

    def norm(values):
        return values * lax.rsqrt(jnp.mean(values * values, axis=-1, keepdims=True) + NORM_EPS)

    h_gathers = [Gather(wires, ('h', t), lambda owner, t=t: xg.at[t, owner],
                        lambda owner, side, t=t: xg.at[t, owner, pl.ds(side * (seq // 2), seq // 2), :]) for t in range(prompts)]
    pl.run_scoped(
        functools.partial(attention_phase, n, place, small_all, mask, cos_t, sin_t, hidden, (wq, wk, wv, wo), (gq, gk, gv, go),
                          (gather_q, gather_k, gather_v, gather_o), moving, gain, norm, k_out, v_out, xg, loc_sems),
        pltpu.VMEM((rows, d_model), bf16),
        pltpu.VMEM((rows, d_model), bf16),
        pltpu.VMEM((rows, q_dim + 2 * kv_dim), f32),
        pltpu.VMEM((rows, q_dim), bf16),
        pltpu.VMEM((2, wq.shape[0], q_dim + 2 * kv_dim), bf16),
        pltpu.SemaphoreType.DMA((2, 3)),
        pltpu.SemaphoreType.DMA((prompts + 1,)),
    )
    h_gathers[0].start(xg.at[0, me])
    with jax.named_scope('services'):
        moving.first_leg(0, 'd')
        moving.first_leg(1, 'd')
        moving.direct_in(1, ('gu',))
    pl.run_scoped(
        functools.partial(moe_phase, n, experts, wires, moving, h_gathers, small, small_all, gain, norm, wgu, wd, xg, y_out, relay_y,
                          u_all, vd, ss_all),
        pltpu.VMEM((experts, d_model, 2 * cols), bf16),
        pltpu.VMEM((2, 4, seq, d_model), bf16),
        pltpu.VMEM((2, n // 2, 2 * seq, LANES), f32),
        pltpu.VMEM((2, 2, 4 * seq, cols), f32),
        pltpu.VMEM((6, 2 * seq, dcols), f32),
        pltpu.VMEM((prompts, 4, 2, seq, dcols), bf16),
        pltpu.VMEM((4, 2, seq, dcols), bf16),
        pltpu.VMEM((prompts, n, 2, seq, LANES), bf16),
        pltpu.VMEM((small.shape[0], d_model), bf16),
        pltpu.VMEM((1, d_model), f32),
        pltpu.SemaphoreType.DMA((2, 2)),
        pltpu.SemaphoreType.DMA((experts + 1,)),
        pltpu.SemaphoreType.DMA((4,)),
        pltpu.SemaphoreType.DMA((prompts,)),
    )


def layer(n, experts, prompts, small, mask, cos_t, sin_t, hidden, wq, wk, wv, wo, gate, up, down):
    rows, d_model = hidden.shape
    seq = rows // prompts
    ff = gate.shape[2]
    drows = down.shape[1]
    cols, dcols = ff // n, d_model // n
    bf16, f32 = jnp.bfloat16, jnp.float32
    quarter = experts // 4

    def full(w):
        return jax.ShapeDtypeStruct((n,) + w.shape, bf16)

    outs = pl.pallas_call(
        functools.partial(layer_kernel, n, experts),
        name='layer',
        out_shape=(
            jax.ShapeDtypeStruct((rows, wk.shape[1]), bf16),
            jax.ShapeDtypeStruct((rows, wv.shape[1]), bf16),
            full(small),
            jax.ShapeDtypeStruct((prompts, seq, d_model), bf16),
            full(wq), full(wk), full(wv), full(wo),
            jax.ShapeDtypeStruct((experts, d_model, 2 * cols), bf16),
            jax.ShapeDtypeStruct((experts, ff, dcols), bf16),
            jax.ShapeDtypeStruct((2, 2, quarter, gate.shape[1], 2 * cols), bf16),
            jax.ShapeDtypeStruct((2, 2, quarter, drows, dcols), bf16),
            jax.ShapeDtypeStruct((prompts, n, seq, d_model), bf16),
            jax.ShapeDtypeStruct((prompts, 2, seq, dcols), bf16),
        ),
        in_specs=[VMEM_FULL] * 4 + [ANY] * 8,
        out_specs=(VMEM_FULL,) * 3 + (ANY,) * 11,
        scratch_shapes=[
            pltpu.VMEM((prompts, n // 2, n, 2 * seq, 2 * cols), bf16),
            pltpu.VMEM((experts, ff, dcols), bf16),
            pltpu.VMEM((prompts, n // 2, n, 8, 2 * seq), f32),
            pltpu.SemaphoreType.DMA((416,)),
            pltpu.SemaphoreType.DMA((416,)),
            pltpu.SemaphoreType.DMA((4,)),
        ],
        compiler_params=pltpu.CompilerParams(collective_id=0, has_side_effects=True, vmem_limit_bytes=67_000_000),
        cost_estimate=pl.CostEstimate(flops=110_000_000_000, bytes_accessed=400_000_000, transcendentals=0),
    )(small, mask, cos_t, sin_t, hidden, wq, wk, wv, wo, gate, up, down)
    return outs[3], outs[0], outs[1]


def solution(mesh):
    n = mesh.shape['wg']
    row_spec = P(('dp', 'wg'))
    dim0_spec = P('wg', None)
    dim1_spec = P(None, 'wg', None)

    def device_fn(hidden, seq_lens, route_idx, g_attn_in, w_query, w_key, w_value, w_attn_out, g_attn_out, g_moe_in, w_router, w_gate, w_up, w_down, g_moe_out):
        n_prompts, seq_len, d_model = hidden.shape
        experts = w_router.shape[1]
        rows = n_prompts * seq_len
        depth = w_query.shape[0]
        lines = -(-(experts + 4 + route_idx.shape[1]) // 16) * 16
        line = lax.broadcasted_iota(jnp.int32, (lines, depth), 0)
        small = jnp.pad(w_router.T, ((0, lines - experts), (0, 0)))
        for i, g in enumerate((g_attn_in, g_attn_out, g_moe_in, g_moe_out)):
            small = jnp.where(line == experts + i, g[None], small)
        first = experts + 4
        routes = jnp.pad(route_idx.T.astype(jnp.bfloat16), ((first, lines - first - route_idx.shape[1]), (0, depth - rows)))
        small = jnp.where(line >= first, routes, small)
        pos = jnp.arange(seq_len)
        mask = ((pos[None, None, :] <= pos[None, :, None]) & (pos[None, None, :] < seq_lens[:, None, None])).astype(jnp.float32)
        cos_t, sin_t = rope_tables(seq_len)
        tok_rows = hidden.reshape(rows, d_model)
        y_out, k_rope, v_rows = layer(
            n, experts, n_prompts, small, mask, cos_t, sin_t, tok_rows, w_query, w_key, w_value, w_attn_out, w_gate, w_up, w_down)
        cache = (n_prompts, seq_len, w_key.shape[1] // HEAD_DIM, HEAD_DIM)
        return y_out, k_rope.reshape(cache), v_rows.reshape(cache)

    return jax.shard_map(
        device_fn,
        mesh=mesh,
        in_specs=(row_spec, row_spec, row_spec, P('wg'), dim0_spec, dim0_spec, dim0_spec, dim0_spec, P('wg'), P('wg'), dim0_spec, dim1_spec, dim1_spec, dim1_spec, P('wg')),
        out_specs=(row_spec, row_spec, row_spec),
        check_vma=False,
    )
```

```python
import functools
import jax
import jax.numpy as jnp
from jax import lax
from jax.experimental import pallas as pl
from jax.experimental.pallas import tpu as pltpu
from jax.sharding import PartitionSpec as P

HEAD_DIM = 128
LANES = 128
SOFT_CAP = 30.0
NORM_EPS = 1e-5
ROPE_BASE = 10000.0
ATTN_SCALE = HEAD_DIM ** -0.5
MESH = pl.DeviceIdType.MESH
ANY = pl.BlockSpec(memory_space=pl.ANY)
VMEM_FULL = pl.BlockSpec(memory_space=pltpu.VMEM)
DIRS = (1, -1)


def dot_f32(left_op, right_op):
    return jnp.dot(left_op, right_op, preferred_element_type=jnp.float32)


def rms_norm(values, gain_vec):
    values_f32 = values.astype(jnp.float32)
    inv_rms = lax.rsqrt(jnp.mean(values_f32 * values_f32, axis=-1, keepdims=True) + NORM_EPS)
    return values_f32 * inv_rms * gain_vec.astype(jnp.float32)


def rope_tables(seq_len):
    half_dim = HEAD_DIM // 2
    inv_freq = ROPE_BASE ** (-jnp.arange(half_dim, dtype=jnp.float32) * (2.0 / HEAD_DIM))
    angles = jnp.arange(seq_len, dtype=jnp.float32)[:, None] * inv_freq[None, :]
    cos_t, sin_t = jnp.cos(angles), jnp.sin(angles)
    return jnp.concatenate([cos_t, cos_t], axis=1), jnp.concatenate([-sin_t, sin_t], axis=1)


class Place:
    def __init__(self, n):
        self.n = n
        self.chips = n // 2
        self.me = lax.axis_index('wg')
        self.dp = lax.axis_index('dp')
        self.chip = self.me // 2
        self.core = self.me % 2
        self.parity = self.dp % 2
        self.twin = self.dp + 1 - 2 * self.parity

    def at(self, offset, rel):
        return ((self.chip + offset + self.chips) % self.chips) * 2 + (self.core + rel) % 2

    def chip_at(self, offset):
        return (self.chip + offset + self.chips) % self.chips


def still(ref):
    if not hasattr(ref, 'transforms'):
        return ref
    out = ref.ref
    for step in ref.transforms:
        out = out.at[tuple(pl.ds(0, index.size) if hasattr(index, 'start') else pl.ds(0, 1) for index in step.indices)]
    return out


class Wires:
    def __init__(self, place, send_sems, recv_sems):
        self.place, self.send_sems, self.recv_sems = place, send_sems, recv_sems
        self.slots = {}
        self.open = []

    def copy(self, name, src, dst, wg=None, dp=None):
        slot = self.slots.setdefault(name, len(self.slots))
        return pltpu.make_async_remote_copy(
            src_ref=src, dst_ref=dst, send_sem=self.send_sems.at[slot], recv_sem=self.recv_sems.at[slot],
            device_id={'dp': self.place.dp if dp is None else dp, 'wg': self.place.me if wg is None else wg},
            device_id_type=MESH)

    def send(self, name, src, dst, wg=None, dp=None):
        desc = self.copy(name, src, dst, wg, dp)
        desc.start()
        self.open.append((name, still(src)))

    def recv(self, name, dst):
        self.copy(name, dst, dst).wait_recv()

    def finish(self):
        for name, src in self.open:
            self.copy(name, src, src).wait_send()
        self.open = []


def enter(place):
    barrier = pltpu.get_barrier_semaphore()
    peers = [(place.dp, place.at(off, rel)) for off in (1, -1, 2) for rel in (0, 1)] + [(place.dp, place.at(0, 1))]
    peers.append((place.twin, place.me))
    for dp, wg in peers:
        pl.semaphore_signal(barrier, inc=1, device_id={'dp': dp, 'wg': wg}, device_id_type=MESH)
    pl.semaphore_wait(barrier, len(peers))


class Reshard:
    def __init__(self, wires, gate, up, down, wgu, wd, relay_gu, relay_d, loc_sems):
        self.wires, self.place = wires, wires.place
        n = self.place.n
        self.gate, self.up, self.down, self.wgu, self.wd = gate, up, down, wgu, wd
        self.relay_gu, self.relay_d, self.loc_sems = relay_gu, relay_d, loc_sems
        self.experts, self.rows, self.cols = gate.shape[0], gate.shape[1], gate.shape[2] // n
        self.drows, self.dcols = down.shape[1], down.shape[2] // n
        self.half, self.quarter = self.experts // 2, self.experts // 4
        self.mine = self.place.parity * self.half
        self.theirs = self.half - self.mine

    def piece(self, arr, e0, cnt, j):
        if arr == 'd':
            return self.down.at[pl.ds(e0, cnt), :, pl.ds(pl.multiple_of(j * self.dcols, LANES), self.dcols)]
        ref = self.gate if arr == 'g' else self.up
        return ref.at[pl.ds(e0, cnt), :, pl.ds(pl.multiple_of(j * self.cols, LANES), self.cols)]

    def land(self, arr, e0, cnt, src):
        if arr == 'd':
            return self.wd.at[pl.ds(e0, cnt), pl.ds(pl.multiple_of(src * self.drows, self.drows), self.drows), :]
        row = pl.ds(pl.multiple_of(src * self.rows, self.rows), self.rows)
        if arr == 'gu':
            return self.wgu.at[pl.ds(e0, cnt), row, :]
        return self.wgu.at[pl.ds(e0, cnt), row, pl.ds(0 if arr == 'g' else self.cols, self.cols)]

    def relay(self, arr, side, rel):
        if arr == 'd':
            return self.relay_d.at[side, rel]
        if arr == 'gu':
            return self.relay_gu.at[side, rel]
        return self.relay_gu.at[side, rel, :, :, pl.ds(0 if arr == 'g' else self.cols, self.cols)]

    def near(self):
        me, sib = self.place.me, self.place.at(0, 1)
        for i, arr in enumerate('gud'):
            self.wires.send(('sib', arr), self.piece(arr, 0, self.experts, sib), self.land(arr, 0, self.experts, me), wg=sib)
            self.own(i, arr).start()

    def own(self, i, arr):
        me = self.place.me
        return pltpu.make_async_copy(self.piece(arr, 0, self.experts, me), self.land(arr, 0, self.experts, me), self.loc_sems.at[i])

    def direct(self, rel, arrs):
        for arr in arrs:
            for d in DIRS:
                to = self.place.at(d, rel)
                self.wires.send(('direct', d, rel, arr), self.piece(arr, self.mine, self.half, to),
                                self.land(arr, self.mine, self.half, self.place.me), wg=to)

    def first_leg(self, rel, arrs):
        for arr in arrs:
            for side, d in enumerate(DIRS):
                e0 = self.mine + side * self.quarter
                self.wires.send(('leg1', d, rel, arr), self.piece(arr, e0, self.quarter, self.place.at(2 * d, rel)),
                                self.relay(arr, side, rel), wg=self.place.at(d, 0))

    def to_twin(self, name, arr, e0, cnt, src):
        region = self.land(arr, e0, cnt, src)
        self.wires.send(name, region, region, dp=self.place.twin)

    def direct_in(self, rel, arrs):
        for arr in arrs:
            for d in DIRS:
                src = self.place.at(-d, rel)
                for part in arr:
                    self.wires.recv(('direct', d, rel, part), self.land(part, self.mine, self.half, src))
                self.to_twin(('twin', d, rel, arr), arr, self.mine, self.half, src)

    def second_leg(self, rel, arrs):
        for arr in arrs:
            for side, d in enumerate(DIRS):
                for part in arr:
                    self.wires.recv(('leg1', d, rel, part), self.relay(part, side, rel))
                self.wires.send(('leg2', d, rel, arr), self.relay(arr, side, rel),
                                self.land(arr, self.mine + side * self.quarter, self.quarter, self.place.at(-d, 0)),
                                wg=self.place.at(d, rel))

    def far_in(self, arrs):
        for arr in arrs:
            for rel in (0, 1):
                for side, d in enumerate(DIRS):
                    src = self.place.at(2 * d, rel)
                    e0 = self.mine + side * self.quarter
                    self.wires.recv(('leg2', d, rel, arr), self.land(arr, e0, self.quarter, src))
                    self.to_twin(('twin2', d, rel, arr), arr, e0, self.quarter, src)

    def finish_near(self, arr):
        for part in arr:
            self.wires.recv(('sib', part), self.land(part, 0, self.experts, self.place.at(0, 1)))
            self.own('gud'.index(part), part).wait()

    def finish_twin(self, arr):
        for rel in (0, 1):
            for side, d in enumerate(DIRS):
                self.wires.recv(('twin', d, rel, arr), self.land(arr, self.theirs, self.half, self.place.at(-d, rel)))
                self.wires.recv(('twin2', d, rel, arr),
                                self.land(arr, self.theirs + side * self.quarter, self.quarter, self.place.at(2 * d, rel)))


class PairGather:
    def __init__(self, wires, name, src, dst, give_side):
        self.wires, self.place, self.name, self.src, self.dst = wires, wires.place, name, src, dst
        rows = src.shape[0]
        given = rows * 5 // 16
        parity = self.place.parity
        last = rows - given
        self.spans = {'give': (parity * last, given), 'both': (given, rows - 2 * given), 'take': (last - parity * last, given)}
        self.far_side = {'give': give_side, 'both': 1 - give_side}

    def part(self, owner, what):
        row, cnt = self.spans[what]
        return self.dst.at[owner, pl.ds(pl.multiple_of(row, 16), cnt), :]

    def start(self):
        place, me = self.place, self.place.me
        for what in ('give', 'both'):
            row, cnt = self.spans[what]
            own = self.src.at[pl.ds(pl.multiple_of(row, 16), cnt), :]
            for d in DIRS:
                self.wires.send((self.name, 'own', what, d), own, self.part(me, what), wg=place.at(d, 0))
        self.wires.send((self.name, 'sib'), self.src, self.dst.at[me], wg=place.at(0, 1))

    def give(self, tag, owner):
        part = self.part(owner, 'give')
        self.wires.send((self.name, 'give', tag), part, part, dp=self.place.twin)

    def near_in(self, *whats):
        place = self.place
        for what in whats:
            for side, d in enumerate(DIRS):
                owner = place.at(-d, 0)
                part = self.part(owner, what)
                self.wires.recv((self.name, 'own', what, d), part)
                if what == 'give':
                    self.give(d, owner)
                if self.far_side[what] == side:
                    self.wires.send((self.name, 'far', what), part, part, wg=place.at(d, 0))
                self.wires.send((self.name, 'across', what, d), part, part, wg=place.at(0, 1))

    def far_in(self, *whats):
        place = self.place
        owner = place.at(2, 0)
        for what in whats:
            part = self.part(owner, what)
            self.wires.recv((self.name, 'far', what), part)
            if what == 'give':
                self.give(2, owner)
            self.wires.send((self.name, 'across', what, 2), part, part, wg=place.at(0, 1))

    def twin_in(self, *tags):
        for tag in tags:
            part = self.part(self.place.at(-tag, 0), 'take')
            self.wires.recv((self.name, 'give', tag), part)
            self.wires.send((self.name, 'across', 'take', tag), part, part, wg=self.place.at(0, 1))

    def sib_in(self):
        place = self.place
        self.wires.recv((self.name, 'sib'), self.dst.at[place.at(0, 1)])
        for tag in (1, -1, 2):
            for what in ('give', 'both', 'take'):
                self.wires.recv((self.name, 'across', what, tag), self.part(place.at(-tag, 1), what))


class Gather:
    def __init__(self, wires, name, region, half_region):
        self.wires, self.place, self.name = wires, wires.place, name
        self.region, self.half_region = region, half_region

    def start(self, src):
        place, dst = self.place, self.region(self.place.me)
        for d in DIRS:
            self.wires.send((self.name, 'own', d), src, dst, wg=place.at(d, 0))
        self.wires.send((self.name, 'own', 0), src, dst, wg=place.at(0, 1))

    def near_in(self, side):
        d, place = DIRS[side], self.place
        owner = place.at(-d, 0)
        block, part = self.region(owner), self.half_region(owner, side)
        self.wires.recv((self.name, 'own', d), block)
        self.wires.send((self.name, 'far', d), part, part, wg=place.at(d, 0))
        self.wires.send((self.name, 'across', d), block, block, wg=place.at(0, 1))

    def far_in(self):
        place = self.place
        owner = place.at(2, 0)
        for side, d in enumerate(DIRS):
            part = self.half_region(owner, side)
            self.wires.recv((self.name, 'far', d), part)
            self.wires.send((self.name, 'across2', d), part, part, wg=place.at(0, 1))

    def sib_own(self):
        self.wires.recv((self.name, 'own', 0), self.region(self.place.at(0, 1)))

    def sib_near(self, side):
        self.wires.recv((self.name, 'across', DIRS[side]), self.region(self.place.at(-DIRS[side], 1)))

    def sib_far(self):
        for side, d in enumerate(DIRS):
            self.wires.recv((self.name, 'across2', d), self.half_region(self.place.at(2, 1), side))


def attention_phase(n, place, small_all, mask, cos_t, sin_t, hidden_hbm, weights, gathered, gathers, moving, gain, norm, k_out, v_out,
                    xg, loc_sems, hidden, h, acc, ctx, wbuf, load_sems, x_sems):
    wq, wk, wv, wo = weights
    gq, gk, gv, go = gathered
    gather_q, gather_k, gather_v, gather_o = gathers
    me = place.me
    prompts, seq = mask.shape[0], mask.shape[1]
    rows, d_model = hidden.shape
    depth = wq.shape[0]
    q_dim, kv_dim = wq.shape[1], wk.shape[1]
    n_kv = kv_dim // HEAD_DIM
    group = q_dim // kv_dim
    tile = 512
    load = pltpu.make_async_copy(hidden_hbm, hidden, x_sems.at[prompts])
    load.start()
    load.wait()

    def norm_in(i, carry):
        r = pl.ds(pl.multiple_of(i * 16, 16), 16)
        h[r, :] = (norm(hidden[r, :].astype(jnp.float32)) * gain(0)).astype(jnp.bfloat16)
        return carry

    with jax.named_scope('norm_in'):
        lax.fori_loop(0, rows // 16, norm_in, 0)
        acc[...] = jnp.zeros_like(acc)

    with jax.named_scope('near'):
        gather_q.near_in('give', 'both')
        gather_k.near_in('give', 'both')
        gather_v.near_in('give', 'both')
        gather_o.start()
        moving.direct(0, 'gu')
        moving.first_leg(0, 'gu')
        moving.first_leg(1, 'gu')
        moving.near()
    with jax.named_scope('qkv_far'):
        gather_q.twin_in(1, -1)
        gather_k.twin_in(1, -1)
        gather_v.twin_in(1, -1)
        gather_q.far_in('give', 'both')
        gather_k.far_in('give', 'both')
        gather_v.far_in('give', 'both')
    with jax.named_scope('qkv_last'):
        gather_q.twin_in(2)
        gather_k.twin_in(2)
        gather_v.twin_in(2)
        gather_q.sib_in()
        gather_k.sib_in()
        gather_v.sib_in()
    with jax.named_scope('o_near_give'):
        gather_o.near_in('give')

    def owner_of(i):
        return (me + i) % n

    def product(lhs, weights, first_col):
        def loads(i, slot):
            owner = owner_of(i)

            def start(own):
                col = 0
                for w, (src, gathered) in enumerate(weights):
                    width = src.shape[1]
                    pltpu.make_async_copy(src if own else gathered.at[owner], wbuf.at[slot, :, pl.ds(col, width)],
                                          load_sems.at[slot, w]).start()
                    col += width

            @pl.when(i == 0)
            def _():
                start(True)

            @pl.when(i > 0)
            def _():
                start(False)

        def step(i, carry):
            slot = i % 2
            owner = owner_of(i)

            @pl.when(i + 1 < n)
            def _():
                loads(i + 1, 1 - slot)

            col = 0
            for w, (src, gathered) in enumerate(weights):
                width = src.shape[1]
                pltpu.make_async_copy(gathered.at[owner], wbuf.at[slot, :, pl.ds(col, width)], load_sems.at[slot, w]).wait()
                col += width

            def tiles(j, carry):
                c = pl.ds(pl.multiple_of(j * tile, tile), tile)
                acc[:, c] += dot_f32(lhs[:, pl.ds(pl.multiple_of(owner * depth, depth), depth)], wbuf[slot, :, c])
                return carry

            return lax.fori_loop(0, col // tile, tiles, carry)

        loads(0, 0)
        lax.fori_loop(0, n, step, 0)

    with jax.named_scope('qkv_mm'):
        product(h, ((wq, gq), (wk, gk), (wv, gv)), 0)

    def rope(values):
        values = values.astype(jnp.bfloat16).astype(jnp.float32)
        cos_v, sin_v = cos_t[...], sin_t[...]
        times = values.shape[0] // seq
        if times > 1:
            cos_v, sin_v = jnp.concatenate([cos_v] * times, axis=0), jnp.concatenate([sin_v] * times, axis=0)
        return (values * cos_v + pltpu.roll(values, HEAD_DIM // 2, 1) * sin_v).astype(jnp.bfloat16)

    def attend(i, carry):
        p, g = i // n_kv, i % n_kv
        r = pl.ds(pl.multiple_of(p * seq, seq), seq)
        kv_cols = pl.ds(pl.multiple_of(g * HEAD_DIM, HEAD_DIM), HEAD_DIM)
        q = jnp.concatenate([acc[r, pl.ds(pl.multiple_of((g * group + j) * HEAD_DIM, HEAD_DIM), HEAD_DIM)]
                             for j in range(group)], axis=0)
        q = rope(q)
        k = rope(acc[r, pl.ds(pl.multiple_of(q_dim + g * HEAD_DIM, HEAD_DIM), HEAD_DIM)])
        v = acc[r, pl.ds(pl.multiple_of(q_dim + kv_dim + g * HEAD_DIM, HEAD_DIM), HEAD_DIM)].astype(jnp.bfloat16)
        k_out[r, kv_cols] = k
        v_out[r, kv_cols] = v
        scores = lax.dot_general(q, k, (((1,), (1,)), ((), ())), preferred_element_type=jnp.float32) * ATTN_SCALE
        scores = SOFT_CAP * jnp.tanh(scores / SOFT_CAP)
        allowed = jnp.concatenate([mask[p]] * group, axis=0) > 0.5
        scores = jnp.where(allowed, scores, -1e30)
        ex = jnp.exp(scores - jnp.max(scores, axis=-1, keepdims=True))
        probs = (ex / jnp.sum(ex, axis=-1, keepdims=True)).astype(jnp.bfloat16)
        out = dot_f32(probs, v).astype(jnp.bfloat16)
        for j in range(group):
            ctx[r, pl.ds(pl.multiple_of((g * group + j) * HEAD_DIM, HEAD_DIM), HEAD_DIM)] = out[j * seq:(j + 1) * seq]
        return carry

    with jax.named_scope('attend'):
        lax.fori_loop(0, prompts * n_kv, attend, 0)

    with jax.named_scope('o_near_both'):
        gather_o.near_in('both')
    with jax.named_scope('direct_in0'):
        moving.direct_in(0, ('gu',))
    with jax.named_scope('leg2'):
        moving.second_leg(0, ('gu',))
        moving.second_leg(1, ('gu',))
        moving.direct(1, 'gu')
        moving.direct(0, 'd')
        moving.direct(1, 'd')
    with jax.named_scope('o_far'):
        gather_o.twin_in(1, -1)
        gather_o.far_in('give', 'both')
    with jax.named_scope('mv_far'):
        moving.far_in(('gu',))
    with jax.named_scope('o_last'):
        gather_o.twin_in(2)
        gather_o.sib_in()
    with jax.named_scope('o_mm'):
        acc[...] = jnp.zeros_like(acc)
        product(ctx, ((wo, go),), 0)

    def finish_rows(i, carry):
        r = pl.ds(pl.multiple_of(i * 16, 16), 16)
        mid = (hidden[r, :].astype(jnp.float32) + norm(acc[r, pl.ds(0, d_model)]) * gain(1)).astype(jnp.bfloat16)
        ctx[r, :] = mid
        return carry

    with jax.named_scope('finish_rows'):
        lax.fori_loop(0, rows // 16, finish_rows, 0)
    stores = []
    for t in range(prompts):
        desc = pltpu.make_async_copy(ctx.at[pl.ds(t * seq, seq), :], xg.at[t, me], x_sems.at[t])
        desc.start()
        stores.append(desc)
    for desc in stores:
        desc.wait()


def moe_phase(n, experts, wires, moving, h_gathers, small, small_all, gain, norm, wgu, wd, xg, y_out, relay_y, u_all, vd, ss_all,
              vgu, hbuf, gates, us, mbuf, ybuf, xcols, route, router, gain_in, load_sems, w_sems, x_sems, out_sems):
    place = wires.place
    steps, seq, d_model = route.shape[0], route.shape[3], hbuf.shape[3]
    chips, me = place.chips, place.me
    rows = 2 * seq
    depth = small.shape[1]
    cols = vgu.shape[2] // 2
    dcols = vd.shape[2]
    offsets = (0, -1, 1, 2)

    with jax.named_scope('tables'):
        gain_in[...] = gain(2)
        for j in range(n):
            router[:, pl.ds(j * depth, depth)] = small_all[j]

        def route_of(j, carry):
            for t in range(steps):
                for i in range(2):
                    line = small_all[j, pl.ds(experts + 4 + i, 1), pl.ds(t * seq, seq)].astype(jnp.float32)
                    route[t, j, i] = jnp.transpose(jnp.broadcast_to(line, (LANES, seq))).astype(jnp.bfloat16)
            return carry

        lax.fori_loop(0, n, route_of, 0)

    own_cols = pl.ds(pl.multiple_of(me * dcols, LANES), dcols)
    half = experts // 2

    def u_owner_chip(owner, q):
        return (owner // 2 + offsets[q] + chips) % chips

    u_gathers = {t: [] for t in range(steps)}
    others = [(off, rel) for off in (0, 1, -1, 2) for rel in (0, 1)][1:]

    pairs = ((0, 1), (2, 3))

    def begin(t, pair):
        loads = []
        for s, q in enumerate(pairs[pair]):
            chip = place.chip_at(offsets[q])
            desc = pltpu.make_async_copy(xg.at[t, pl.ds(2 * chip, 2)], hbuf.at[pair, pl.ds(2 * s, 2)], load_sems.at[pair, s])
            desc.start()
            loads.append(desc)
        return loads

    def routes(t, chips_of):
        def one(i):
            return jnp.concatenate([route[t, pl.ds(2 * chip, 2), i].reshape(rows, LANES) for chip in chips_of], axis=0)

        return one(0), one(1)

    def prepare(t, pair, loads):
        with jax.named_scope('load'):
            for desc in loads:
                desc.wait()
        h = hbuf.at[pair]

        def norm_rows(i, carry):
            r = pl.ds(pl.multiple_of(i % (seq // 32) * 32, 32), 32)
            x = h[i // (seq // 32), r, :].astype(jnp.float32)
            h[i // (seq // 32), r, :] = (norm(x) * gain_in[...]).astype(jnp.bfloat16)
            return carry

        with jax.named_scope('norm'):
            lax.fori_loop(0, 2 * rows // 32, norm_rows, 0)
        logits = lax.dot_general(h[...].reshape(2 * rows, d_model), router[...], (((1,), (1,)), ((), ())),
                                 preferred_element_type=jnp.float32)
        lane = lax.broadcasted_iota(jnp.int32, logits.shape, 1)
        logits = jnp.where(lane < experts, logits, -1e30)
        peak = jnp.max(logits, axis=-1, keepdims=True)
        ex = jnp.where(lane < experts, jnp.exp(logits - peak), 0.0)
        probs = ex / jnp.sum(ex, axis=-1, keepdims=True)
        lane_f = lane.astype(jnp.float32)
        chips_of = [place.chip_at(offsets[q]) for q in pairs[pair]]
        g0, g1 = (jnp.sum(jnp.where(lane_f == r[:, :logits.shape[1]].astype(jnp.float32), probs, 0.0), axis=-1, keepdims=True)
                  for r in routes(t, chips_of))
        both = jnp.where(lax.broadcasted_iota(jnp.int32, (2 * rows, LANES), 1) == 0, g0, g1)
        for s, chip in enumerate(chips_of):
            gates[t % 2, chip] = both[s * rows:(s + 1) * rows]
        us[pair] = jnp.zeros(us.shape[1:], jnp.float32)

    def up_part(t, pair, e0, cnt):
        h = hbuf.at[pair]
        chips_of = [place.chip_at(offsets[q]) for q in pairs[pair]]

        def expert(i, carry):
            e = e0 + i
            act = dot_f32(h[...].reshape(2 * rows, d_model), vgu[e])
            inner = (jax.nn.gelu(act[:, :cols]) * act[:, cols:]).astype(jnp.bfloat16).astype(jnp.float32)
            e_f = e.astype(jnp.float32)
            r0, r1 = routes(t, chips_of)
            us[pair, 0] = jnp.where(r0.astype(jnp.float32) == e_f, inner, us[pair, 0])
            us[pair, 1] = jnp.where(r1.astype(jnp.float32) == e_f, inner, us[pair, 1])
            return carry

        with jax.named_scope('up'):
            lax.fori_loop(0, cnt, expert, 0)

    def emit(t, pair):
        for s, q in enumerate(pairs[pair]):
            chip = place.chip_at(offsets[q])
            for i in range(2):
                u_all[t, chip, me, :, pl.ds(i * cols, cols)] = us[pair, i, s * rows:(s + 1) * rows].astype(jnp.bfloat16)
            if t == steps - 1:
                gather = Gather(wires, ('u', t, q), lambda owner, q=q: u_all.at[t, u_owner_chip(owner, q), owner],
                                lambda owner, side, q=q: u_all.at[t, u_owner_chip(owner, q), owner, pl.ds(side * seq, seq), :])
                gather.start(u_all.at[t, chip, me])
                u_gathers[t].append(gather)
        if t < steps - 1 and pair == 1:
            gather = Gather(wires, ('u', t), lambda owner: u_all.at[t, :, owner],
                            lambda owner, side: u_all.at[t, pl.ds(side * (chips // 2), chips // 2), owner])
            gather.start(u_all.at[t, :, me])
            u_gathers[t].append(gather)

    def chunk_near(t):
        h_gathers[t].near_in(0)
        h_gathers[t].near_in(1)
        if t == 1:
            u_near(0, u_gathers[0])
        if t + 1 < steps:
            h_gathers[t + 1].start(xg.at[t + 1, me])

    def load_experts(e0):
        loads = []
        for i in range(half):
            desc = pltpu.make_async_copy(wgu.at[e0 + i], vgu.at[e0 + i], w_sems.at[i])
            desc.start()
            loads.append(desc)
        return loads

    first_loads = {}

    def enter_chunk(t):
        with jax.named_scope('near'):
            h_gathers[t].sib_own()
            chunk_near(t)
            h_gathers[t].sib_near(0)
            first_loads[t] = begin(t, 0)

    def phase_a(t):
        gather = h_gathers[t]
        mine_loads = []
        if t == 0:
            with jax.named_scope('mine_in'):
                moving.finish_near('gu')
                mine_loads = load_experts(moving.mine)
        if t < 2:
            enter_chunk(t)
        if t > 1:
            u_near(t - 1, u_gathers[t - 1])
        prepare(t, 0, first_loads.pop(t))
        if t == 0:
            for desc in mine_loads:
                desc.wait()
            up_part(t, 0, moving.mine, half)
        else:
            up_part(t, 0, 0, experts)
            emit(t, 0)
        with jax.named_scope('far'):
            if t == 1:
                moving.far_in(('d',))
            gather.sib_near(1)
            gather.far_in()
            gather.sib_far()
            loads = begin(t, 1)
        prepare(t, 1, loads)
        if t == steps - 1:
            u_near(t, u_gathers[t])
        if t == 0:
            with jax.named_scope('d_direct'):
                moving.direct_in(0, ('d',))
                moving.direct_in(1, ('d',))
                moving.second_leg(0, ('d',))
                moving.second_leg(1, ('d',))
            up_part(t, 1, moving.mine, half)
            with jax.named_scope('theirs_in'):
                moving.finish_twin('gu')
                theirs_loads = load_experts(moving.theirs)
                for desc in theirs_loads:
                    desc.wait()
            for pair in (0, 1):
                up_part(t, pair, moving.theirs, half)
                emit(t, pair)
        else:
            up_part(t, 1, 0, experts)
            emit(t, 1)

    def u_near(t, gathers):
        with jax.named_scope('u_near'):
            for gather in gathers:
                gather.near_in(0)
                gather.near_in(1)

    def phase_b(t, between):
        if t == 0:
            with jax.named_scope('d_in'):
                moving.finish_near('d')
                moving.finish_twin('d')
                d_load = pltpu.make_async_copy(wd, vd, w_sems.at[experts])
                d_load.start()
        with jax.named_scope('u_wait'):
            for gather in u_gathers[t]:
                gather.far_in()
                gather.sib_own()
                gather.sib_near(0)
                gather.sib_near(1)
                gather.sib_far()
        if t == 0:
            d_load.wait()
        for first in range(0, chips, 2):
            chips_of = (first, first + 1)
            acc = mbuf.at[pl.ds((chips * t + first) % mbuf.shape[0], 2)]
            acc[...] = jnp.zeros_like(acc)

            def expert(e, carry):
                e_b = e.astype(jnp.bfloat16)
                r0, r1 = routes(t, chips_of)
                m0, m1 = r0 == e_b, r1 == e_b
                zero = jnp.zeros((2 * rows, LANES), jnp.bfloat16)
                parts = []
                for j in range(n):
                    u0 = u_all[t, pl.ds(first, 2), j, :, pl.ds(0, cols)].reshape(2 * rows, cols)
                    u1 = u_all[t, pl.ds(first, 2), j, :, pl.ds(cols, cols)].reshape(2 * rows, cols)
                    parts.append(jnp.where(m0, u0, jnp.where(m1, u1, zero)))
                ue = jnp.concatenate(parts, axis=1)
                out = dot_f32(ue, vd[e])
                e_f = e.astype(jnp.float32)
                both = gates[t % 2, pl.ds(first, 2)].reshape(2 * rows, LANES)
                gate = jnp.where(r0.astype(jnp.float32) == e_f, both[:, :1], jnp.where(r1.astype(jnp.float32) == e_f, both[:, 1:2], 0.0))
                acc[...] += (jnp.concatenate([gate] * (dcols // LANES), axis=1) * out).reshape(2, rows, dcols)
                return carry

            with jax.named_scope('down'):
                lax.fori_loop(0, experts, expert, 0)
            for chip in chips_of:
                part = mbuf[(chips * t + chip) % mbuf.shape[0]]
                squares = jnp.sum(part * part, axis=-1, keepdims=True)
                ss_all[t, chip, me] = jnp.transpose(jnp.broadcast_to(squares, (rows, LANES)))[:ss_all.shape[3]]
            if first == 0:
                between()
        for off, rel in others:
            region = ss_all.at[t, :, me]
            wires.send(('ss', t, off, rel), region, region, wg=place.at(off, rel))

    y_open = []

    def phase_c(t):
        loads = []
        for q in range(4):
            chip = place.chip_at(offsets[q])
            desc = pltpu.make_async_copy(xg.at[t, pl.ds(2 * chip, 2), :, own_cols], xcols.at[q], x_sems.at[q])
            desc.start()
            loads.append(desc)
        gain_out = small[pl.ds(experts + 3, 1), :].astype(jnp.float32)
        with jax.named_scope('ss_wait'):
            for off, rel in others:
                wires.recv(('ss', t, off, rel), ss_all.at[t, :, place.at(-off, rel)])
        for q in (3, 1, 2, 0):
            chip = place.chip_at(offsets[q])
            loads[q].wait()
            with jax.named_scope('y'):
                total = ss_all[t, chip, 0]
                for j in range(1, n):
                    total += ss_all[t, chip, j]
                line = jnp.broadcast_to(total[:1], (LANES, rows))
                scale = lax.rsqrt(jnp.transpose(line) * (1.0 / d_model) + NORM_EPS)
                scale = jnp.concatenate([scale] * (dcols // LANES), axis=1)
                x1 = xcols[q].reshape(rows, dcols).astype(jnp.float32)
                ybuf[t, q] = (x1 + mbuf[(chips * t + chip) % mbuf.shape[0]] * scale * gain_out).astype(jnp.bfloat16).reshape(2, seq, dcols)
            dst = y_out.at[t, :, own_cols]
            for rel in (0, 1):
                part = ybuf.at[t, q, (place.core + rel) % 2]
                if q == 0 and rel == 0:
                    desc = pltpu.make_async_copy(part, dst, out_sems.at[t])
                    desc.start()
                    y_open.append(desc)
                elif q < 3:
                    wires.send(('y', t, q, rel), part, dst, wg=place.at(offsets[q], rel))
                else:
                    wires.send(('y1', t, rel), part, relay_y.at[t, rel], wg=place.at(DIRS[rel], 0))

    def y_cols(src):
        return pl.ds(pl.multiple_of(src * dcols, LANES), dcols)

    def y_relay(t):
        for rel, d in enumerate(DIRS):
            wires.recv(('y1', t, rel), relay_y.at[t, rel])
            wires.send(('y2', t, rel), relay_y.at[t, rel], y_out.at[t, :, y_cols(place.at(-d, 0))], wg=place.at(d, rel))

    def y_in(t):
        for q in range(4):
            for rel in (0, 1):
                if q == 0 and rel == 0:
                    continue
                wires.recv(('y', t, q, rel) if q < 3 else ('y2', t, rel), y_out.at[t, :, y_cols(place.at(-offsets[q], rel))])

    phase_a(0)
    for t in range(1, steps):
        phase_a(t)

        def between(t=t):
            if t + 1 < steps:
                enter_chunk(t + 1)
            else:
                u_near(t, u_gathers[t][2:])
            if t > 1:
                phase_c(t - 2)

        phase_b(t - 1, between)
    for t in range(steps - 2):
        y_relay(t)
    phase_b(steps - 1, functools.partial(phase_c, steps - 2))
    y_relay(steps - 2)
    phase_c(steps - 1)
    y_relay(steps - 1)
    with jax.named_scope('y_in'):
        for t in range(steps):
            y_in(t)
        for desc in y_open:
            desc.wait()
        wires.finish()


def layer_kernel(n, experts, small, mask, cos_t, sin_t, hidden, wq, wk, wv, wo, gate, up, down,
                 k_out, v_out, small_all, y_out, gq, gk, gv, go, wgu, wd, relay_gu, relay_d, xg, relay_y,
                 u_all, vd, ss_all, send_sems, recv_sems, loc_sems):
    place = Place(n)
    wires = Wires(place, send_sems, recv_sems)
    me = place.me
    prompts, seq = mask.shape[0], mask.shape[1]
    rows, d_model = hidden.shape
    cols, dcols = gate.shape[2] // n, down.shape[2] // n
    q_dim, kv_dim = wq.shape[1], wk.shape[1]
    bf16, f32 = jnp.bfloat16, jnp.float32

    enter(place)
    gather_q = PairGather(wires, 'q', wq, gq, 0)
    gather_k = PairGather(wires, 'k', wk, gk, 1)
    gather_v = PairGather(wires, 'v', wv, gv, 1)
    gather_o = PairGather(wires, 'o', wo, go, 1)
    moving = Reshard(wires, gate, up, down, wgu, wd, relay_gu, relay_d, loc_sems)
    others = [(off, rel) for off in (0, 1, -1, 2) for rel in (0, 1)][1:]
    for off, rel in others:
        wires.send(('small', off, rel), small, small_all.at[me], wg=place.at(off, rel))
    gather_q.start()
    gather_k.start()
    gather_v.start()
    small_all[me] = small[...]
    for off, rel in others:
        wires.recv(('small', off, rel), small_all.at[place.at(-off, rel)])

    def gain(i):
        return jnp.concatenate([small_all[j, pl.ds(experts + i, 1), :] for j in range(n)], axis=1).astype(jnp.float32)

    def norm(values):
        return values * lax.rsqrt(jnp.mean(values * values, axis=-1, keepdims=True) + NORM_EPS)

    h_gathers = [Gather(wires, ('h', t), lambda owner, t=t: xg.at[t, owner],
                        lambda owner, side, t=t: xg.at[t, owner, pl.ds(side * (seq // 2), seq // 2), :]) for t in range(prompts)]
    pl.run_scoped(
        functools.partial(attention_phase, n, place, small_all, mask, cos_t, sin_t, hidden, (wq, wk, wv, wo), (gq, gk, gv, go),
                          (gather_q, gather_k, gather_v, gather_o), moving, gain, norm, k_out, v_out, xg, loc_sems),
        pltpu.VMEM((rows, d_model), bf16),
        pltpu.VMEM((rows, d_model), bf16),
        pltpu.VMEM((rows, q_dim + 2 * kv_dim), f32),
        pltpu.VMEM((rows, q_dim), bf16),
        pltpu.VMEM((2, wq.shape[0], q_dim + 2 * kv_dim), bf16),
        pltpu.SemaphoreType.DMA((2, 3)),
        pltpu.SemaphoreType.DMA((prompts + 1,)),
    )
    h_gathers[0].start(xg.at[0, me])
    with jax.named_scope('services'):
        moving.first_leg(0, 'd')
        moving.first_leg(1, 'd')
        moving.direct_in(1, ('gu',))
    pl.run_scoped(
        functools.partial(moe_phase, n, experts, wires, moving, h_gathers, small, small_all, gain, norm, wgu, wd, xg, y_out, relay_y,
                          u_all, vd, ss_all),
        pltpu.VMEM((experts, d_model, 2 * cols), bf16),
        pltpu.VMEM((2, 4, seq, d_model), bf16),
        pltpu.VMEM((2, n // 2, 2 * seq, LANES), f32),
        pltpu.VMEM((2, 2, 4 * seq, cols), f32),
        pltpu.VMEM((6, 2 * seq, dcols), f32),
        pltpu.VMEM((prompts, 4, 2, seq, dcols), bf16),
        pltpu.VMEM((4, 2, seq, dcols), bf16),
        pltpu.VMEM((prompts, n, 2, seq, LANES), bf16),
        pltpu.VMEM((small.shape[0], d_model), bf16),
        pltpu.VMEM((1, d_model), f32),
        pltpu.SemaphoreType.DMA((2, 2)),
        pltpu.SemaphoreType.DMA((experts + 1,)),
        pltpu.SemaphoreType.DMA((4,)),
        pltpu.SemaphoreType.DMA((prompts,)),
    )


def layer(n, experts, prompts, small, mask, cos_t, sin_t, hidden, wq, wk, wv, wo, gate, up, down):
    rows, d_model = hidden.shape
    seq = rows // prompts
    ff = gate.shape[2]
    drows = down.shape[1]
    cols, dcols = ff // n, d_model // n
    bf16, f32 = jnp.bfloat16, jnp.float32
    quarter = experts // 4

    def full(w):
        return jax.ShapeDtypeStruct((n,) + w.shape, bf16)

    outs = pl.pallas_call(
        functools.partial(layer_kernel, n, experts),
        name='layer',
        out_shape=(
            jax.ShapeDtypeStruct((rows, wk.shape[1]), bf16),
            jax.ShapeDtypeStruct((rows, wv.shape[1]), bf16),
            full(small),
            jax.ShapeDtypeStruct((prompts, seq, d_model), bf16),
            full(wq), full(wk), full(wv), full(wo),
            jax.ShapeDtypeStruct((experts, d_model, 2 * cols), bf16),
            jax.ShapeDtypeStruct((experts, ff, dcols), bf16),
            jax.ShapeDtypeStruct((2, 2, quarter, gate.shape[1], 2 * cols), bf16),
            jax.ShapeDtypeStruct((2, 2, quarter, drows, dcols), bf16),
            jax.ShapeDtypeStruct((prompts, n, seq, d_model), bf16),
            jax.ShapeDtypeStruct((prompts, 2, seq, dcols), bf16),
        ),
        in_specs=[VMEM_FULL] * 4 + [ANY] * 8,
        out_specs=(VMEM_FULL,) * 3 + (ANY,) * 11,
        scratch_shapes=[
            pltpu.VMEM((prompts, n // 2, n, 2 * seq, 2 * cols), bf16),
            pltpu.VMEM((experts, ff, dcols), bf16),
            pltpu.VMEM((prompts, n // 2, n, 8, 2 * seq), f32),
            pltpu.SemaphoreType.DMA((416,)),
            pltpu.SemaphoreType.DMA((416,)),
            pltpu.SemaphoreType.DMA((4,)),
        ],
        compiler_params=pltpu.CompilerParams(collective_id=0, has_side_effects=True, vmem_limit_bytes=67_000_000),
        cost_estimate=pl.CostEstimate(flops=110_000_000_000, bytes_accessed=400_000_000, transcendentals=0),
    )(small, mask, cos_t, sin_t, hidden, wq, wk, wv, wo, gate, up, down)
    return outs[3], outs[0], outs[1]


def solution(mesh):
    n = mesh.shape['wg']
    row_spec = P(('dp', 'wg'))
    dim0_spec = P('wg', None)
    dim1_spec = P(None, 'wg', None)

    def device_fn(hidden, seq_lens, route_idx, g_attn_in, w_query, w_key, w_value, w_attn_out, g_attn_out, g_moe_in, w_router, w_gate, w_up, w_down, g_moe_out):
        n_prompts, seq_len, d_model = hidden.shape
        experts = w_router.shape[1]
        rows = n_prompts * seq_len
        depth = w_query.shape[0]
        lines = -(-(experts + 4 + route_idx.shape[1]) // 16) * 16
        line = lax.broadcasted_iota(jnp.int32, (lines, depth), 0)
        small = jnp.pad(w_router.T, ((0, lines - experts), (0, 0)))
        for i, g in enumerate((g_attn_in, g_attn_out, g_moe_in, g_moe_out)):
            small = jnp.where(line == experts + i, g[None], small)
        first = experts + 4
        routes = jnp.pad(route_idx.T.astype(jnp.bfloat16), ((first, lines - first - route_idx.shape[1]), (0, depth - rows)))
        small = jnp.where(line >= first, routes, small)
        pos = jnp.arange(seq_len)
        mask = ((pos[None, None, :] <= pos[None, :, None]) & (pos[None, None, :] < seq_lens[:, None, None])).astype(jnp.float32)
        cos_t, sin_t = rope_tables(seq_len)
        tok_rows = hidden.reshape(rows, d_model)
        y_out, k_rope, v_rows = layer(
            n, experts, n_prompts, small, mask, cos_t, sin_t, tok_rows, w_query, w_key, w_value, w_attn_out, w_gate, w_up, w_down)
        cache = (n_prompts, seq_len, w_key.shape[1] // HEAD_DIM, HEAD_DIM)
        return y_out, k_rope.reshape(cache), v_rows.reshape(cache)

    return jax.shard_map(
        device_fn,
        mesh=mesh,
        in_specs=(row_spec, row_spec, row_spec, P('wg'), dim0_spec, dim0_spec, dim0_spec, dim0_spec, P('wg'), P('wg'), dim0_spec, dim1_spec, dim1_spec, dim1_spec, P('wg')),
        out_specs=(row_spec, row_spec, row_spec),
        check_vma=False,
    )
```

```python
import functools
import jax
import jax.numpy as jnp
from jax import lax
from jax.experimental import pallas as pl
from jax.experimental.pallas import tpu as pltpu
from jax.sharding import PartitionSpec as P

HEAD_DIM = 128
LANES = 128
SOFT_CAP = 30.0
NORM_EPS = 1e-5
ROPE_BASE = 10000.0
ATTN_SCALE = HEAD_DIM ** -0.5
MESH = pl.DeviceIdType.MESH
ANY = pl.BlockSpec(memory_space=pl.ANY)
VMEM_FULL = pl.BlockSpec(memory_space=pltpu.VMEM)
DIRS = (1, -1)
CORES = (0, 1)
LAST_DIMS = (((1,), (1,)), ((), ()))


def dot_f32(left_op, right_op):
    return jnp.dot(left_op, right_op, preferred_element_type=jnp.float32)


def rope_tables(seq_len):
    half_dim = HEAD_DIM // 2
    inv_freq = ROPE_BASE ** (-jnp.arange(half_dim, dtype=jnp.float32) * (2.0 / HEAD_DIM))
    angles = jnp.arange(seq_len, dtype=jnp.float32)[:, None] * inv_freq[None, :]
    cos_t, sin_t = jnp.cos(angles), jnp.sin(angles)
    return jnp.concatenate([cos_t, cos_t], axis=1), jnp.concatenate([-sin_t, sin_t], axis=1)


class Place:
    def __init__(self, n):
        self.n = n
        self.chips = n // 2
        self.me = lax.axis_index('wg')
        self.dp = lax.axis_index('dp')
        self.chip = self.me // 2
        self.core = self.me % 2
        self.parity = self.dp % 2
        self.twin = self.dp + 1 - 2 * self.parity

    def at(self, offset, rel):
        return ((self.chip + offset + self.chips) % self.chips) * 2 + (self.core + rel) % 2

    def chip_at(self, offset):
        return (self.chip + offset + self.chips) % self.chips


def still(ref):
    if not hasattr(ref, 'transforms'):
        return ref
    out = ref.ref
    for step in ref.transforms:
        out = out.at[tuple(pl.ds(0, index.size) if hasattr(index, 'start') else pl.ds(0, 1) for index in step.indices)]
    return out


class Wires:
    def __init__(self, place, send_sems, recv_sems):
        self.place, self.send_sems, self.recv_sems = place, send_sems, recv_sems
        self.slots = {}
        self.open = []

    def copy(self, name, src, dst, wg=None, dp=None):
        slot = self.slots.setdefault(name, len(self.slots))
        return pltpu.make_async_remote_copy(
            src_ref=src, dst_ref=dst, send_sem=self.send_sems.at[slot], recv_sem=self.recv_sems.at[slot],
            device_id={'dp': self.place.dp if dp is None else dp, 'wg': self.place.me if wg is None else wg},
            device_id_type=MESH)

    def send(self, name, src, dst, wg=None, dp=None):
        desc = self.copy(name, src, dst, wg, dp)
        desc.start()
        self.open.append((name, still(src)))

    def recv(self, name, dst):
        self.copy(name, dst, dst).wait_recv()

    def finish(self):
        for name, src in self.open:
            self.copy(name, src, src).wait_send()
        self.open = []


def enter(place):
    barrier = pltpu.get_barrier_semaphore()
    peers = [(place.dp, place.at(off, rel)) for off in (1, -1, 2) for rel in CORES] + [(place.dp, place.at(0, 1))]
    peers.append((place.twin, place.me))
    for dp, wg in peers:
        pl.semaphore_signal(barrier, inc=1, device_id={'dp': dp, 'wg': wg}, device_id_type=MESH)
    pl.semaphore_wait(barrier, len(peers))


class Reshard:
    def __init__(self, wires, gate, up, down, wgu, wd, relay_gu, relay_d, loc_sems):
        self.wires, self.place = wires, wires.place
        n = self.place.n
        self.gate, self.up, self.down, self.wgu, self.wd = gate, up, down, wgu, wd
        self.relay_gu, self.relay_d, self.loc_sems = relay_gu, relay_d, loc_sems
        self.experts, self.rows, self.cols = gate.shape[0], gate.shape[1], gate.shape[2] // n
        self.drows, self.dcols = down.shape[1], down.shape[2] // n
        self.half, self.quarter = self.experts // 2, self.experts // 4
        self.mine = self.place.parity * self.half
        self.theirs = self.half - self.mine

    def piece(self, arr, e0, cnt, j):
        if arr == 'd':
            return self.down.at[pl.ds(e0, cnt), :, pl.ds(pl.multiple_of(j * self.dcols, LANES), self.dcols)]
        ref = self.gate if arr == 'g' else self.up
        return ref.at[pl.ds(e0, cnt), :, pl.ds(pl.multiple_of(j * self.cols, LANES), self.cols)]

    def land(self, arr, e0, cnt, src):
        if arr == 'd':
            return self.wd.at[pl.ds(e0, cnt), pl.ds(pl.multiple_of(src * self.drows, self.drows), self.drows), :]
        row = pl.ds(pl.multiple_of(src * self.rows, self.rows), self.rows)
        if arr == 'gu':
            return self.wgu.at[pl.ds(e0, cnt), row, :]
        return self.wgu.at[pl.ds(e0, cnt), row, pl.ds(0 if arr == 'g' else self.cols, self.cols)]

    def relay(self, arr, side, rel):
        if arr == 'd':
            return self.relay_d.at[side, rel]
        if arr == 'gu':
            return self.relay_gu.at[side, rel]
        return self.relay_gu.at[side, rel, :, :, pl.ds(0 if arr == 'g' else self.cols, self.cols)]

    def near(self):
        me, sib = self.place.me, self.place.at(0, 1)
        for i, arr in enumerate('gud'):
            self.wires.send(('sib', arr), self.piece(arr, 0, self.experts, sib), self.land(arr, 0, self.experts, me), wg=sib)
            self.own(i, arr).start()

    def own(self, i, arr):
        me = self.place.me
        return pltpu.make_async_copy(self.piece(arr, 0, self.experts, me), self.land(arr, 0, self.experts, me), self.loc_sems.at[i])

    def direct(self, rel, arrs):
        for arr in arrs:
            for d in DIRS:
                to = self.place.at(d, rel)
                self.wires.send(('direct', d, rel, arr), self.piece(arr, self.mine, self.half, to),
                                self.land(arr, self.mine, self.half, self.place.me), wg=to)

    def first_leg(self, rel, arrs):
        for arr in arrs:
            for side, d in enumerate(DIRS):
                e0 = self.mine + side * self.quarter
                self.wires.send(('leg1', d, rel, arr), self.piece(arr, e0, self.quarter, self.place.at(2 * d, rel)),
                                self.relay(arr, side, rel), wg=self.place.at(d, 0))

    def to_twin(self, name, arr, e0, cnt, src):
        region = self.land(arr, e0, cnt, src)
        self.wires.send(name, region, region, dp=self.place.twin)

    def direct_in(self, rel, arrs):
        for arr in arrs:
            for d in DIRS:
                src = self.place.at(-d, rel)
                for part in arr:
                    self.wires.recv(('direct', d, rel, part), self.land(part, self.mine, self.half, src))
                self.to_twin(('twin', d, rel, arr), arr, self.mine, self.half, src)

    def second_leg(self, rel, arrs):
        for arr in arrs:
            for side, d in enumerate(DIRS):
                for part in arr:
                    self.wires.recv(('leg1', d, rel, part), self.relay(part, side, rel))
                self.wires.send(('leg2', d, rel, arr), self.relay(arr, side, rel),
                                self.land(arr, self.mine + side * self.quarter, self.quarter, self.place.at(-d, 0)),
                                wg=self.place.at(d, rel))

    def far_in(self, arrs):
        for arr in arrs:
            for rel in CORES:
                for side, d in enumerate(DIRS):
                    src = self.place.at(2 * d, rel)
                    e0 = self.mine + side * self.quarter
                    self.wires.recv(('leg2', d, rel, arr), self.land(arr, e0, self.quarter, src))
                    self.to_twin(('twin2', d, rel, arr), arr, e0, self.quarter, src)

    def finish_near(self, arr):
        for part in arr:
            self.wires.recv(('sib', part), self.land(part, 0, self.experts, self.place.at(0, 1)))
            self.own('gud'.index(part), part).wait()

    def finish_twin(self, arr):
        for rel in CORES:
            for side, d in enumerate(DIRS):
                self.wires.recv(('twin', d, rel, arr), self.land(arr, self.theirs, self.half, self.place.at(-d, rel)))
                self.wires.recv(('twin2', d, rel, arr),
                                self.land(arr, self.theirs + side * self.quarter, self.quarter, self.place.at(2 * d, rel)))


class PairGather:
    def __init__(self, wires, name, src, dst, give_side):
        self.wires, self.place, self.name, self.src, self.dst = wires, wires.place, name, src, dst
        rows = src.shape[0]
        given = rows * 5 // 16
        parity = self.place.parity
        last = rows - given
        self.spans = {'give': (parity * last, given), 'both': (given, rows - 2 * given), 'take': (last - parity * last, given)}
        self.far_side = {'give': give_side, 'both': 1 - give_side}

    def part(self, owner, what):
        row, cnt = self.spans[what]
        return self.dst.at[owner, pl.ds(pl.multiple_of(row, 16), cnt), :]

    def start(self):
        place, me = self.place, self.place.me
        for what in ('give', 'both'):
            row, cnt = self.spans[what]
            own = self.src.at[pl.ds(pl.multiple_of(row, 16), cnt), :]
            for d in DIRS:
                self.wires.send((self.name, 'own', what, d), own, self.part(me, what), wg=place.at(d, 0))
        self.wires.send((self.name, 'sib'), self.src, self.dst.at[me], wg=place.at(0, 1))

    def give(self, tag, owner):
        part = self.part(owner, 'give')
        self.wires.send((self.name, 'give', tag), part, part, dp=self.place.twin)

    def near_in(self, *whats):
        place = self.place
        for what in whats:
            for side, d in enumerate(DIRS):
                owner = place.at(-d, 0)
                part = self.part(owner, what)
                self.wires.recv((self.name, 'own', what, d), part)
                if what == 'give':
                    self.give(d, owner)
                if self.far_side[what] == side:
                    self.wires.send((self.name, 'far', what), part, part, wg=place.at(d, 0))
                self.wires.send((self.name, 'across', what, d), part, part, wg=place.at(0, 1))

    def far_in(self, *whats):
        place = self.place
        owner = place.at(2, 0)
        for what in whats:
            part = self.part(owner, what)
            self.wires.recv((self.name, 'far', what), part)
            if what == 'give':
                self.give(2, owner)
            self.wires.send((self.name, 'across', what, 2), part, part, wg=place.at(0, 1))

    def twin_in(self, *tags):
        for tag in tags:
            part = self.part(self.place.at(-tag, 0), 'take')
            self.wires.recv((self.name, 'give', tag), part)
            self.wires.send((self.name, 'across', 'take', tag), part, part, wg=self.place.at(0, 1))

    def sib_in(self):
        place = self.place
        self.wires.recv((self.name, 'sib'), self.dst.at[place.at(0, 1)])
        for tag in (1, -1, 2):
            for what in ('give', 'both', 'take'):
                self.wires.recv((self.name, 'across', what, tag), self.part(place.at(-tag, 1), what))


class Gather:
    def __init__(self, wires, name, region, half_region):
        self.wires, self.place, self.name = wires, wires.place, name
        self.region, self.half_region = region, half_region

    def start(self, src):
        place, dst = self.place, self.region(self.place.me)
        for d in DIRS:
            self.wires.send((self.name, 'own', d), src, dst, wg=place.at(d, 0))
        self.wires.send((self.name, 'own', 0), src, dst, wg=place.at(0, 1))

    def near_in(self, side):
        d, place = DIRS[side], self.place
        owner = place.at(-d, 0)
        block, part = self.region(owner), self.half_region(owner, side)
        self.wires.recv((self.name, 'own', d), block)
        self.wires.send((self.name, 'far', d), part, part, wg=place.at(d, 0))
        self.wires.send((self.name, 'across', d), block, block, wg=place.at(0, 1))

    def far_in(self):
        place = self.place
        owner = place.at(2, 0)
        for side, d in enumerate(DIRS):
            part = self.half_region(owner, side)
            self.wires.recv((self.name, 'far', d), part)
            self.wires.send((self.name, 'across2', d), part, part, wg=place.at(0, 1))

    def sib_own(self):
        self.wires.recv((self.name, 'own', 0), self.region(self.place.at(0, 1)))

    def sib_near(self, side):
        self.wires.recv((self.name, 'across', DIRS[side]), self.region(self.place.at(-DIRS[side], 1)))

    def sib_far(self):
        for side, d in enumerate(DIRS):
            self.wires.recv((self.name, 'across2', d), self.half_region(self.place.at(2, 1), side))


def attention_phase(n, place, small_all, mask, cos_t, sin_t, hidden_hbm, weights, gathered, gathers, moving, gain, norm, k_out, v_out,
                    xg, loc_sems, hidden, h, acc, ctx, wbuf, load_sems, x_sems):
    wq, wk, wv, wo = weights
    gq, gk, gv, go = gathered
    gather_q, gather_k, gather_v, gather_o = gathers
    me = place.me
    prompts, seq = mask.shape[0], mask.shape[1]
    rows, d_model = hidden.shape
    depth = wq.shape[0]
    q_dim, kv_dim = wq.shape[1], wk.shape[1]
    n_kv = kv_dim // HEAD_DIM
    group = q_dim // kv_dim
    tile = 512
    load = pltpu.make_async_copy(hidden_hbm, hidden, x_sems.at[prompts])
    load.start()
    load.wait()

    def norm_in(i, carry):
        r = pl.ds(pl.multiple_of(i * 16, 16), 16)
        h[r, :] = (norm(hidden[r, :].astype(jnp.float32)) * gain(0)).astype(jnp.bfloat16)
        return carry

    with jax.named_scope('norm_in'):
        lax.fori_loop(0, rows // 16, norm_in, 0)
        acc[...] = jnp.zeros_like(acc)

    with jax.named_scope('near'):
        gather_q.near_in('give', 'both')
        gather_k.near_in('give', 'both')
        gather_v.near_in('give', 'both')
        gather_o.start()
        moving.direct(0, 'gu')
        moving.first_leg(0, 'gu')
        moving.first_leg(1, 'gu')
        moving.near()
    with jax.named_scope('qkv_far'):
        gather_q.twin_in(1, -1)
        gather_k.twin_in(1, -1)
        gather_v.twin_in(1, -1)
        gather_q.far_in('give', 'both')
        gather_k.far_in('give', 'both')
        gather_v.far_in('give', 'both')
    with jax.named_scope('qkv_last'):
        gather_q.twin_in(2)
        gather_k.twin_in(2)
        gather_v.twin_in(2)
        gather_q.sib_in()
        gather_k.sib_in()
        gather_v.sib_in()
    with jax.named_scope('o_near_give'):
        gather_o.near_in('give')

    def owner_of(i):
        return (me + i) % n

    def product(lhs, weights, first_col):
        def loads(i, slot):
            owner = owner_of(i)

            def start(own):
                col = 0
                for w, (src, gathered) in enumerate(weights):
                    width = src.shape[1]
                    pltpu.make_async_copy(src if own else gathered.at[owner], wbuf.at[slot, :, pl.ds(col, width)],
                                          load_sems.at[slot, w]).start()
                    col += width

            @pl.when(i == 0)
            def _():
                start(True)

            @pl.when(i > 0)
            def _():
                start(False)

        def step(i, carry):
            slot = i % 2
            owner = owner_of(i)

            @pl.when(i + 1 < n)
            def _():
                loads(i + 1, 1 - slot)

            col = 0
            for w, (src, gathered) in enumerate(weights):
                width = src.shape[1]
                pltpu.make_async_copy(gathered.at[owner], wbuf.at[slot, :, pl.ds(col, width)], load_sems.at[slot, w]).wait()
                col += width

            def tiles(j, carry):
                c = pl.ds(pl.multiple_of(j * tile, tile), tile)
                acc[:, c] += dot_f32(lhs[:, pl.ds(pl.multiple_of(owner * depth, depth), depth)], wbuf[slot, :, c])
                return carry

            return lax.fori_loop(0, col // tile, tiles, carry)

        loads(0, 0)
        lax.fori_loop(0, n, step, 0)

    with jax.named_scope('qkv_mm'):
        product(h, ((wq, gq), (wk, gk), (wv, gv)), 0)

    def rope(values):
        values = values.astype(jnp.bfloat16).astype(jnp.float32)
        cos_v, sin_v = cos_t[...], sin_t[...]
        times = values.shape[0] // seq
        if times > 1:
            cos_v, sin_v = jnp.concatenate([cos_v] * times, axis=0), jnp.concatenate([sin_v] * times, axis=0)
        return (values * cos_v + pltpu.roll(values, HEAD_DIM // 2, 1) * sin_v).astype(jnp.bfloat16)

    def attend(i, carry):
        p, g = i // n_kv, i % n_kv
        r = pl.ds(pl.multiple_of(p * seq, seq), seq)
        kv_cols = pl.ds(pl.multiple_of(g * HEAD_DIM, HEAD_DIM), HEAD_DIM)
        q = jnp.concatenate([acc[r, pl.ds(pl.multiple_of((g * group + j) * HEAD_DIM, HEAD_DIM), HEAD_DIM)]
                             for j in range(group)], axis=0)
        q = rope(q)
        k = rope(acc[r, pl.ds(pl.multiple_of(q_dim + g * HEAD_DIM, HEAD_DIM), HEAD_DIM)])
        v = acc[r, pl.ds(pl.multiple_of(q_dim + kv_dim + g * HEAD_DIM, HEAD_DIM), HEAD_DIM)].astype(jnp.bfloat16)
        k_out[r, kv_cols] = k
        v_out[r, kv_cols] = v
        scores = lax.dot_general(q, k, LAST_DIMS, preferred_element_type=jnp.float32) * ATTN_SCALE
        scores = SOFT_CAP * jnp.tanh(scores / SOFT_CAP)
        allowed = jnp.concatenate([mask[p]] * group, axis=0) > 0.5
        scores = jnp.where(allowed, scores, -1e30)
        ex = jnp.exp(scores - jnp.max(scores, axis=-1, keepdims=True))
        probs = (ex / jnp.sum(ex, axis=-1, keepdims=True)).astype(jnp.bfloat16)
        out = dot_f32(probs, v).astype(jnp.bfloat16)
        for j in range(group):
            ctx[r, pl.ds(pl.multiple_of((g * group + j) * HEAD_DIM, HEAD_DIM), HEAD_DIM)] = out[j * seq:(j + 1) * seq]
        return carry

    with jax.named_scope('attend'):
        lax.fori_loop(0, prompts * n_kv, attend, 0)

    with jax.named_scope('o_near_both'):
        gather_o.near_in('both')
    with jax.named_scope('direct_in0'):
        moving.direct_in(0, ('gu',))
    with jax.named_scope('leg2'):
        moving.second_leg(0, ('gu',))
        moving.second_leg(1, ('gu',))
        moving.direct(1, 'gu')
        moving.direct(0, 'd')
        moving.direct(1, 'd')
    with jax.named_scope('o_far'):
        gather_o.twin_in(1, -1)
        gather_o.far_in('give', 'both')
    with jax.named_scope('mv_far'):
        moving.far_in(('gu',))
    with jax.named_scope('o_last'):
        gather_o.twin_in(2)
        gather_o.sib_in()
    with jax.named_scope('o_mm'):
        acc[...] = jnp.zeros_like(acc)
        product(ctx, ((wo, go),), 0)

    def finish_rows(i, carry):
        r = pl.ds(pl.multiple_of(i * 16, 16), 16)
        mid = (hidden[r, :].astype(jnp.float32) + norm(acc[r, pl.ds(0, d_model)]) * gain(1)).astype(jnp.bfloat16)
        ctx[r, :] = mid
        return carry

    with jax.named_scope('finish_rows'):
        lax.fori_loop(0, rows // 16, finish_rows, 0)
    stores = []
    for t in range(prompts):
        desc = pltpu.make_async_copy(ctx.at[pl.ds(t * seq, seq), :], xg.at[t, me], x_sems.at[t])
        desc.start()
        stores.append(desc)
    for desc in stores:
        desc.wait()


def moe_phase(n, experts, wires, moving, h_gathers, small, small_all, gain, norm, wgu, wd, xg, y_out, relay_y, u_all, vd, ss_all,
              vgu, hbuf, gates, us, mbuf, ybuf, xcols, route, router, gain_in, load_sems, w_sems, x_sems, out_sems):
    place = wires.place
    steps, seq, d_model = route.shape[0], route.shape[3], hbuf.shape[3]
    chips, me = place.chips, place.me
    rows = 2 * seq
    depth = small.shape[1]
    cols = vgu.shape[2] // 2
    dcols = vd.shape[2]
    offsets = (0, -1, 1, 2)

    with jax.named_scope('tables'):
        gain_in[...] = gain(2)
        for j in range(n):
            router[:, pl.ds(j * depth, depth)] = small_all[j]

        def route_of(j, carry):
            for t in range(steps):
                for i in range(2):
                    line = small_all[j, pl.ds(experts + 4 + i, 1), pl.ds(t * seq, seq)].astype(jnp.float32)
                    route[t, j, i] = jnp.transpose(jnp.broadcast_to(line, (LANES, seq))).astype(jnp.bfloat16)
            return carry

        lax.fori_loop(0, n, route_of, 0)

    own_cols = pl.ds(pl.multiple_of(me * dcols, LANES), dcols)
    half = experts // 2

    def u_owner_chip(owner, q):
        return (owner // 2 + offsets[q] + chips) % chips

    u_gathers = {t: [] for t in range(steps)}
    others = [(off, rel) for off in (0, 1, -1, 2) for rel in CORES][1:]

    pairs = ((0, 1), (2, 3))

    def begin(t, pair):
        loads = []
        for s, q in enumerate(pairs[pair]):
            chip = place.chip_at(offsets[q])
            desc = pltpu.make_async_copy(xg.at[t, pl.ds(2 * chip, 2)], hbuf.at[pair, pl.ds(2 * s, 2)], load_sems.at[pair, s])
            desc.start()
            loads.append(desc)
        return loads

    def routes(t, chips_of):
        def one(i):
            return jnp.concatenate([route[t, pl.ds(2 * chip, 2), i].reshape(rows, LANES) for chip in chips_of], axis=0)

        return one(0), one(1)

    def prepare(t, pair, loads):
        with jax.named_scope('load'):
            for desc in loads:
                desc.wait()
        h = hbuf.at[pair]

        def norm_rows(i, carry):
            r = pl.ds(pl.multiple_of(i % (seq // 32) * 32, 32), 32)
            x = h[i // (seq // 32), r, :].astype(jnp.float32)
            h[i // (seq // 32), r, :] = (norm(x) * gain_in[...]).astype(jnp.bfloat16)
            return carry

        with jax.named_scope('norm'):
            lax.fori_loop(0, 2 * rows // 32, norm_rows, 0)
        logits = lax.dot_general(h[...].reshape(2 * rows, d_model), router[...], LAST_DIMS,
                                 preferred_element_type=jnp.float32)
        lane = lax.broadcasted_iota(jnp.int32, logits.shape, 1)
        logits = jnp.where(lane < experts, logits, -1e30)
        peak = jnp.max(logits, axis=-1, keepdims=True)
        ex = jnp.where(lane < experts, jnp.exp(logits - peak), 0.0)
        probs = ex / jnp.sum(ex, axis=-1, keepdims=True)
        lane_f = lane.astype(jnp.float32)
        chips_of = [place.chip_at(offsets[q]) for q in pairs[pair]]
        g0, g1 = (jnp.sum(jnp.where(lane_f == r[:, :logits.shape[1]].astype(jnp.float32), probs, 0.0), axis=-1, keepdims=True)
                  for r in routes(t, chips_of))
        both = jnp.where(lax.broadcasted_iota(jnp.int32, (2 * rows, LANES), 1) == 0, g0, g1)
        for s, chip in enumerate(chips_of):
            gates[t % 2, chip] = both[s * rows:(s + 1) * rows]
        us[pair] = jnp.zeros(us.shape[1:], jnp.float32)

    def up_part(t, pair, e0, cnt):
        h = hbuf.at[pair]
        chips_of = [place.chip_at(offsets[q]) for q in pairs[pair]]

        def expert(i, carry):
            e = e0 + i
            act = dot_f32(h[...].reshape(2 * rows, d_model), vgu[e])
            inner = (jax.nn.gelu(act[:, :cols]) * act[:, cols:]).astype(jnp.bfloat16).astype(jnp.float32)
            e_f = e.astype(jnp.float32)
            r0, r1 = routes(t, chips_of)
            us[pair, 0] = jnp.where(r0.astype(jnp.float32) == e_f, inner, us[pair, 0])
            us[pair, 1] = jnp.where(r1.astype(jnp.float32) == e_f, inner, us[pair, 1])
            return carry

        with jax.named_scope('up'):
            lax.fori_loop(0, cnt, expert, 0)

    def emit(t, pair):
        for s, q in enumerate(pairs[pair]):
            chip = place.chip_at(offsets[q])
            for i in range(2):
                u_all[t, chip, me, :, pl.ds(i * cols, cols)] = us[pair, i, s * rows:(s + 1) * rows].astype(jnp.bfloat16)
            if t == steps - 1:
                gather = Gather(wires, ('u', t, q), lambda owner, q=q: u_all.at[t, u_owner_chip(owner, q), owner],
                                lambda owner, side, q=q: u_all.at[t, u_owner_chip(owner, q), owner, pl.ds(side * seq, seq), :])
                gather.start(u_all.at[t, chip, me])
                u_gathers[t].append(gather)
        if t < steps - 1 and pair == 1:
            gather = Gather(wires, ('u', t), lambda owner: u_all.at[t, :, owner],
                            lambda owner, side: u_all.at[t, pl.ds(side * (chips // 2), chips // 2), owner])
            gather.start(u_all.at[t, :, me])
            u_gathers[t].append(gather)

    def chunk_near(t):
        h_gathers[t].near_in(0)
        h_gathers[t].near_in(1)
        if t == 1:
            u_near(0, u_gathers[0])
        if t + 1 < steps:
            h_gathers[t + 1].start(xg.at[t + 1, me])

    def load_experts(e0):
        loads = []
        for i in range(half):
            desc = pltpu.make_async_copy(wgu.at[e0 + i], vgu.at[e0 + i], w_sems.at[i])
            desc.start()
            loads.append(desc)
        return loads

    first_loads = {}

    def enter_chunk(t):
        with jax.named_scope('near'):
            h_gathers[t].sib_own()
            chunk_near(t)
            h_gathers[t].sib_near(0)
            first_loads[t] = begin(t, 0)

    def phase_a(t):
        gather = h_gathers[t]
        mine_loads = []
        if t == 0:
            with jax.named_scope('mine_in'):
                moving.finish_near('gu')
                mine_loads = load_experts(moving.mine)
        if t < 2:
            enter_chunk(t)
        if t > 1:
            u_near(t - 1, u_gathers[t - 1])
        prepare(t, 0, first_loads.pop(t))
        if t == 0:
            for desc in mine_loads:
                desc.wait()
            up_part(t, 0, moving.mine, half)
        else:
            up_part(t, 0, 0, experts)
            emit(t, 0)
        with jax.named_scope('far'):
            if t == 1:
                moving.far_in(('d',))
            gather.sib_near(1)
            gather.far_in()
            gather.sib_far()
            loads = begin(t, 1)
        prepare(t, 1, loads)
        if t == steps - 1:
            u_near(t, u_gathers[t])
        if t == 0:
            with jax.named_scope('d_direct'):
                moving.direct_in(0, ('d',))
                moving.direct_in(1, ('d',))
                moving.second_leg(0, ('d',))
                moving.second_leg(1, ('d',))
            up_part(t, 1, moving.mine, half)
            with jax.named_scope('theirs_in'):
                moving.finish_twin('gu')
                theirs_loads = load_experts(moving.theirs)
                for desc in theirs_loads:
                    desc.wait()
            for pair in (0, 1):
                up_part(t, pair, moving.theirs, half)
                emit(t, pair)
        else:
            up_part(t, 1, 0, experts)
            emit(t, 1)

    def u_near(t, gathers):
        with jax.named_scope('u_near'):
            for gather in gathers:
                gather.near_in(0)
                gather.near_in(1)

    def phase_b(t, between):
        if t == 0:
            with jax.named_scope('d_in'):
                moving.finish_near('d')
                moving.finish_twin('d')
                d_load = pltpu.make_async_copy(wd, vd, w_sems.at[experts])
                d_load.start()
        with jax.named_scope('u_wait'):
            for gather in u_gathers[t]:
                gather.far_in()
                gather.sib_own()
                gather.sib_near(0)
                gather.sib_near(1)
                gather.sib_far()
        if t == 0:
            d_load.wait()
        for first in range(0, chips, 2):
            chips_of = (first, first + 1)
            acc = mbuf.at[pl.ds((chips * t + first) % mbuf.shape[0], 2)]
            acc[...] = jnp.zeros_like(acc)

            def expert(e, carry):
                e_b = e.astype(jnp.bfloat16)
                r0, r1 = routes(t, chips_of)
                m0, m1 = r0 == e_b, r1 == e_b
                zero = jnp.zeros((2 * rows, LANES), jnp.bfloat16)
                parts = []
                for j in range(n):
                    u0 = u_all[t, pl.ds(first, 2), j, :, pl.ds(0, cols)].reshape(2 * rows, cols)
                    u1 = u_all[t, pl.ds(first, 2), j, :, pl.ds(cols, cols)].reshape(2 * rows, cols)
                    parts.append(jnp.where(m0, u0, jnp.where(m1, u1, zero)))
                ue = jnp.concatenate(parts, axis=1)
                out = dot_f32(ue, vd[e])
                e_f = e.astype(jnp.float32)
                both = gates[t % 2, pl.ds(first, 2)].reshape(2 * rows, LANES)
                gate = jnp.where(r0.astype(jnp.float32) == e_f, both[:, :1], jnp.where(r1.astype(jnp.float32) == e_f, both[:, 1:2], 0.0))
                acc[...] += (jnp.concatenate([gate] * (dcols // LANES), axis=1) * out).reshape(2, rows, dcols)
                return carry

            with jax.named_scope('down'):
                lax.fori_loop(0, experts, expert, 0)
            for chip in chips_of:
                part = mbuf[(chips * t + chip) % mbuf.shape[0]]
                squares = jnp.sum(part * part, axis=-1, keepdims=True)
                ss_all[t, chip, me] = jnp.transpose(jnp.broadcast_to(squares, (rows, LANES)))[:ss_all.shape[3]]
            if first == 0:
                between()
        for off, rel in others:
            region = ss_all.at[t, :, me]
            wires.send(('ss', t, off, rel), region, region, wg=place.at(off, rel))

    y_open = []

    def phase_c(t):
        loads = []
        for q in range(4):
            chip = place.chip_at(offsets[q])
            desc = pltpu.make_async_copy(xg.at[t, pl.ds(2 * chip, 2), :, own_cols], xcols.at[q], x_sems.at[q])
            desc.start()
            loads.append(desc)
        gain_out = small[pl.ds(experts + 3, 1), :].astype(jnp.float32)
        with jax.named_scope('ss_wait'):
            for off, rel in others:
                wires.recv(('ss', t, off, rel), ss_all.at[t, :, place.at(-off, rel)])
        for q in (3, 1, 2, 0):
            chip = place.chip_at(offsets[q])
            loads[q].wait()
            with jax.named_scope('y'):
                total = ss_all[t, chip, 0]
                for j in range(1, n):
                    total += ss_all[t, chip, j]
                line = jnp.broadcast_to(total[:1], (LANES, rows))
                scale = lax.rsqrt(jnp.transpose(line) * (1.0 / d_model) + NORM_EPS)
                scale = jnp.concatenate([scale] * (dcols // LANES), axis=1)
                x1 = xcols[q].reshape(rows, dcols).astype(jnp.float32)
                ybuf[t, q] = (x1 + mbuf[(chips * t + chip) % mbuf.shape[0]] * scale * gain_out).astype(jnp.bfloat16).reshape(2, seq, dcols)
            dst = y_out.at[t, :, own_cols]
            for rel in CORES:
                part = ybuf.at[t, q, (place.core + rel) % 2]
                if q == 0 and rel == 0:
                    desc = pltpu.make_async_copy(part, dst, out_sems.at[t])
                    desc.start()
                    y_open.append(desc)
                elif q < 3:
                    wires.send(('y', t, q, rel), part, dst, wg=place.at(offsets[q], rel))
                else:
                    wires.send(('y1', t, rel), part, relay_y.at[t, rel], wg=place.at(DIRS[rel], 0))

    def y_cols(src):
        return pl.ds(pl.multiple_of(src * dcols, LANES), dcols)

    def y_relay(t):
        for rel, d in enumerate(DIRS):
            wires.recv(('y1', t, rel), relay_y.at[t, rel])
            wires.send(('y2', t, rel), relay_y.at[t, rel], y_out.at[t, :, y_cols(place.at(-d, 0))], wg=place.at(d, rel))

    def y_in(t):
        for q in range(4):
            for rel in CORES:
                if q == 0 and rel == 0:
                    continue
                wires.recv(('y', t, q, rel) if q < 3 else ('y2', t, rel), y_out.at[t, :, y_cols(place.at(-offsets[q], rel))])

    phase_a(0)
    for t in range(1, steps):
        phase_a(t)

        def between(t=t):
            if t + 1 < steps:
                enter_chunk(t + 1)
            else:
                u_near(t, u_gathers[t][2:])
            if t > 1:
                phase_c(t - 2)

        phase_b(t - 1, between)
    for t in range(steps - 2):
        y_relay(t)
    phase_b(steps - 1, functools.partial(phase_c, steps - 2))
    y_relay(steps - 2)
    phase_c(steps - 1)
    y_relay(steps - 1)
    with jax.named_scope('y_in'):
        for t in range(steps):
            y_in(t)
        for desc in y_open:
            desc.wait()
        wires.finish()


def layer_kernel(n, experts, small, mask, cos_t, sin_t, hidden, wq, wk, wv, wo, gate, up, down,
                 k_out, v_out, small_all, y_out, gq, gk, gv, go, wgu, wd, relay_gu, relay_d, xg, relay_y,
                 u_all, vd, ss_all, send_sems, recv_sems, loc_sems):
    place = Place(n)
    wires = Wires(place, send_sems, recv_sems)
    me = place.me
    prompts, seq = mask.shape[0], mask.shape[1]
    rows, d_model = hidden.shape
    cols, dcols = gate.shape[2] // n, down.shape[2] // n
    q_dim, kv_dim = wq.shape[1], wk.shape[1]
    bf16, f32 = jnp.bfloat16, jnp.float32

    enter(place)
    gather_q = PairGather(wires, 'q', wq, gq, 0)
    gather_k = PairGather(wires, 'k', wk, gk, 1)
    gather_v = PairGather(wires, 'v', wv, gv, 1)
    gather_o = PairGather(wires, 'o', wo, go, 1)
    moving = Reshard(wires, gate, up, down, wgu, wd, relay_gu, relay_d, loc_sems)
    others = [(off, rel) for off in (0, 1, -1, 2) for rel in CORES][1:]
    for off, rel in others:
        wires.send(('small', off, rel), small, small_all.at[me], wg=place.at(off, rel))
    gather_q.start()
    gather_k.start()
    gather_v.start()
    small_all[me] = small[...]
    for off, rel in others:
        wires.recv(('small', off, rel), small_all.at[place.at(-off, rel)])

    def gain(i):
        return jnp.concatenate([small_all[j, pl.ds(experts + i, 1), :] for j in range(n)], axis=1).astype(jnp.float32)

    def norm(values):
        return values * lax.rsqrt(jnp.mean(values * values, axis=-1, keepdims=True) + NORM_EPS)

    h_gathers = [Gather(wires, ('h', t), lambda owner, t=t: xg.at[t, owner],
                        lambda owner, side, t=t: xg.at[t, owner, pl.ds(side * (seq // 2), seq // 2), :]) for t in range(prompts)]
    pl.run_scoped(
        functools.partial(attention_phase, n, place, small_all, mask, cos_t, sin_t, hidden, (wq, wk, wv, wo), (gq, gk, gv, go),
                          (gather_q, gather_k, gather_v, gather_o), moving, gain, norm, k_out, v_out, xg, loc_sems),
        pltpu.VMEM((rows, d_model), bf16),
        pltpu.VMEM((rows, d_model), bf16),
        pltpu.VMEM((rows, q_dim + 2 * kv_dim), f32),
        pltpu.VMEM((rows, q_dim), bf16),
        pltpu.VMEM((2, wq.shape[0], q_dim + 2 * kv_dim), bf16),
        pltpu.SemaphoreType.DMA((2, 3)),
        pltpu.SemaphoreType.DMA((prompts + 1,)),
    )
    h_gathers[0].start(xg.at[0, me])
    with jax.named_scope('services'):
        moving.first_leg(0, 'd')
        moving.first_leg(1, 'd')
        moving.direct_in(1, ('gu',))
    pl.run_scoped(
        functools.partial(moe_phase, n, experts, wires, moving, h_gathers, small, small_all, gain, norm, wgu, wd, xg, y_out, relay_y,
                          u_all, vd, ss_all),
        pltpu.VMEM((experts, d_model, 2 * cols), bf16),
        pltpu.VMEM((2, 4, seq, d_model), bf16),
        pltpu.VMEM((2, n // 2, 2 * seq, LANES), f32),
        pltpu.VMEM((2, 2, 4 * seq, cols), f32),
        pltpu.VMEM((6, 2 * seq, dcols), f32),
        pltpu.VMEM((prompts, 4, 2, seq, dcols), bf16),
        pltpu.VMEM((4, 2, seq, dcols), bf16),
        pltpu.VMEM((prompts, n, 2, seq, LANES), bf16),
        pltpu.VMEM((small.shape[0], d_model), bf16),
        pltpu.VMEM((1, d_model), f32),
        pltpu.SemaphoreType.DMA((2, 2)),
        pltpu.SemaphoreType.DMA((experts + 1,)),
        pltpu.SemaphoreType.DMA((4,)),
        pltpu.SemaphoreType.DMA((prompts,)),
    )


def layer(n, experts, prompts, small, mask, cos_t, sin_t, hidden, wq, wk, wv, wo, gate, up, down):
    rows, d_model = hidden.shape
    seq = rows // prompts
    ff = gate.shape[2]
    drows = down.shape[1]
    cols, dcols = ff // n, d_model // n
    bf16, f32 = jnp.bfloat16, jnp.float32
    quarter = experts // 4

    def full(w):
        return jax.ShapeDtypeStruct((n,) + w.shape, bf16)

    outs = pl.pallas_call(
        functools.partial(layer_kernel, n, experts),
        name='layer',
        out_shape=(
            jax.ShapeDtypeStruct((rows, wk.shape[1]), bf16),
            jax.ShapeDtypeStruct((rows, wv.shape[1]), bf16),
            full(small),
            jax.ShapeDtypeStruct((prompts, seq, d_model), bf16),
            full(wq), full(wk), full(wv), full(wo),
            jax.ShapeDtypeStruct((experts, d_model, 2 * cols), bf16),
            jax.ShapeDtypeStruct((experts, ff, dcols), bf16),
            jax.ShapeDtypeStruct((2, 2, quarter, gate.shape[1], 2 * cols), bf16),
            jax.ShapeDtypeStruct((2, 2, quarter, drows, dcols), bf16),
            jax.ShapeDtypeStruct((prompts, n, seq, d_model), bf16),
            jax.ShapeDtypeStruct((prompts, 2, seq, dcols), bf16),
        ),
        in_specs=[VMEM_FULL] * 4 + [ANY] * 8,
        out_specs=(VMEM_FULL,) * 3 + (ANY,) * 11,
        scratch_shapes=[
            pltpu.VMEM((prompts, n // 2, n, 2 * seq, 2 * cols), bf16),
            pltpu.VMEM((experts, ff, dcols), bf16),
            pltpu.VMEM((prompts, n // 2, n, 8, 2 * seq), f32),
            pltpu.SemaphoreType.DMA((416,)),
            pltpu.SemaphoreType.DMA((416,)),
            pltpu.SemaphoreType.DMA((4,)),
        ],
        compiler_params=pltpu.CompilerParams(collective_id=0, has_side_effects=True, vmem_limit_bytes=67_000_000),
        cost_estimate=pl.CostEstimate(flops=110_000_000_000, bytes_accessed=400_000_000, transcendentals=0),
    )(small, mask, cos_t, sin_t, hidden, wq, wk, wv, wo, gate, up, down)
    return outs[3], outs[0], outs[1]


def solution(mesh):
    n = mesh.shape['wg']
    row_spec = P(('dp', 'wg'))
    dim0_spec = P('wg', None)
    dim1_spec = P(None, 'wg', None)

    def device_fn(hidden, seq_lens, route_idx, g_attn_in, w_query, w_key, w_value, w_attn_out, g_attn_out, g_moe_in, w_router, w_gate, w_up, w_down, g_moe_out):
        n_prompts, seq_len, d_model = hidden.shape
        experts = w_router.shape[1]
        rows = n_prompts * seq_len
        depth = w_query.shape[0]
        lines = -(-(experts + 4 + route_idx.shape[1]) // 16) * 16
        line = lax.broadcasted_iota(jnp.int32, (lines, depth), 0)
        small = jnp.pad(w_router.T, ((0, lines - experts), (0, 0)))
        for i, g in enumerate((g_attn_in, g_attn_out, g_moe_in, g_moe_out)):
            small = jnp.where(line == experts + i, g[None], small)
        first = experts + 4
        routes = jnp.pad(route_idx.T.astype(jnp.bfloat16), ((first, lines - first - route_idx.shape[1]), (0, depth - rows)))
        small = jnp.where(line >= first, routes, small)
        pos = jnp.arange(seq_len)
        mask = ((pos[None, None, :] <= pos[None, :, None]) & (pos[None, None, :] < seq_lens[:, None, None])).astype(jnp.float32)
        cos_t, sin_t = rope_tables(seq_len)
        tok_rows = hidden.reshape(rows, d_model)
        y_out, k_rope, v_rows = layer(
            n, experts, n_prompts, small, mask, cos_t, sin_t, tok_rows, w_query, w_key, w_value, w_attn_out, w_gate, w_up, w_down)
        cache = (n_prompts, seq_len, w_key.shape[1] // HEAD_DIM, HEAD_DIM)
        return y_out, k_rope.reshape(cache), v_rows.reshape(cache)

    return jax.shard_map(
        device_fn,
        mesh=mesh,
        in_specs=(row_spec, row_spec, row_spec, P('wg'), dim0_spec, dim0_spec, dim0_spec, dim0_spec, P('wg'), P('wg'), dim0_spec, dim1_spec, dim1_spec, dim1_spec, P('wg')),
        out_specs=(row_spec, row_spec, row_spec),
        check_vma=False,
    )
```
